32 devices in a mesh: gx: 4 (over x, core), gy: 8 (over z, y).
Axes of the slice: x: 2, y: 2, z: 4, core: 2. Of those that a mesh axis runs over, the one named last changes fastest.
Arguments:
- air_state: float32 [3, 16, 512, 1024], P(None, None, 'gx', 'gy'), may hold values from -6 to 6
- level_set: float32 [64, 256, 256], P(('gx', 'gy')), may hold values from -3 to 5
- fuel_left: float32 [64, 256, 256], P(('gx', 'gy')), may hold values from 0.2 to 1
- fuel_class: int32 [64, 256, 256], P(('gx', 'gy')), may hold values from 0 to 12
- fuel_props: float32 [5, 13], replicated, may hold values from 0.5 to 2
- blocks: int32 [64, 2], replicated, may hold values from 0 to 31, as said below
- adjacency: int32 [64, 4], replicated, may hold values from -1 to 63, as said below
Outputs:
- air_next: float32 [3, 16, 512, 1024], P(None, None, 'gx', 'gy')
- level_next: float32 [64, 256, 256], P(('gx', 'gy'))
- fuel_next: float32 [64, 256, 256], P(('gx', 'gy'))
- totals: float32 [2], replicated
The draws below stay inside these ranges and needn't reach their ends.
Inputs may be any that keep to these rules, and one draw needn't show every extreme that they name: Rows are distinct; entry [i, 0] is below 16 and entry [i, 1] below 32; block i's fire cells lie on device i // 2 of gx+gy; at most 4 blocks lie on the 128 x 128 atmosphere columns of one device, and in every draw some device's columns hold exactly that many. `adjacency`: entry [i, s] is the list index of the burning block one block row above (s = 0), below (1), one block column left (2) or right (3) of block i, and -1 where that block is not in the list.
All inputs are finite; a program needn't handle non-finite values.
Results may differ from the reference program's by a relative error of at most 0.00005.
Values sent between devices are 32-bit elements; how exact they have to be, the bound alone decides.
No kernel may reach another device: no remote copies, remote signals or barrier semaphores. Data moves between devices by JAX's collectives and lax.ppermute only.
A program may use at most 128 MiB of HBM per device.

```python
import math
from functools import partial
import jax
import jax.numpy as jnp
from jax import lax

CX = 128
CY = 128
LEV = 16
FB = 256
REF = 8
BA = 32
BLK_DEV = 2
SUB = 10
NCLASS = 13
NX = 512
NY = 1024
NBLK = 64


def block_layout(key):
    rows_total = NX // BA
    cols_total = NY // BA
    grand_total = rows_total * cols_total
    tile_rows = CX // BA
    tile_cols = CY // BA
    per_tile = tile_rows * tile_cols
    tiles_across = NY // CY
    tile_count = NX // CX * tiles_across
    capacity = 2 * BLK_DEV
    centre_rows = jax.random.randint(jax.random.fold_in(key, 101), (4,), 0, rows_total)
    centre_cols = jax.random.randint(jax.random.fold_in(key, 102), (4,), 0, cols_total)
    forced_choice = jax.random.randint(jax.random.fold_in(key, 105), (), 0, tile_count)
    tile_numbers = jnp.arange(tile_count, dtype=jnp.int32)[:, None]
    local_ids = jnp.arange(per_tile, dtype=jnp.int32)[None, :]
    cell_row = tile_numbers // tiles_across * tile_rows + local_ids // tile_cols
    cell_col = tile_numbers % tiles_across * tile_cols + local_ids % tile_cols
    grid_cell = cell_row * cols_total + cell_col
    separation = jnp.min(jnp.abs(cell_row[:, :, None] - centre_rows[None, None, :]) + jnp.abs(cell_col[:, :, None] - centre_cols[None, None, :]), axis=2)
    reach_radius = max(2, min(rows_total, cols_total) // 4)
    extra_reward = jnp.maximum(reach_radius - separation, 0)
    extra_reward = jnp.where(tile_numbers == forced_choice, reach_radius + 2, extra_reward)
    random_jitter = jax.random.randint(jax.random.fold_in(key, 103), (tile_count, per_tile), 0, 1024)
    block_score = (extra_reward * 1024 + random_jitter) * grand_total + grid_cell
    higher = block_score[:, None, :] > block_score[:, :, None]
    rank = jnp.sum(higher.astype(jnp.int32), axis=2)
    eligible = jnp.where(rank < capacity, block_score, -1 - grid_cell).reshape(grand_total)
    unused, picked = lax.top_k(eligible, NBLK)
    chosen = grid_cell.reshape(grand_total)[picked]
    order = jax.random.permutation(jax.random.fold_in(key, 104), NBLK).astype(jnp.int32)
    target = ((forced_choice + tile_count - tile_count // 2) % tile_count * BLK_DEV).astype(jnp.int32)
    where_first = jnp.argmax((order == 0).astype(jnp.int32)).astype(jnp.int32)
    target_value = order[target]
    order = order.at[where_first].set(target_value)
    order = order.at[target].set(0)
    chosen = chosen[order].astype(jnp.int32)
    coords = jnp.stack([chosen // cols_total, chosen % cols_total], axis=1).astype(jnp.int32)
    grid = jnp.full((grand_total,), -1, dtype=jnp.int32).at[chosen].set(jnp.arange(NBLK, dtype=jnp.int32))
    step_rows = jnp.array([-1, 1, 0, 0], dtype=jnp.int32)
    step_cols = jnp.array([0, 0, -1, 1], dtype=jnp.int32)
    near_rows = coords[:, 0:1] + step_rows[None, :]
    near_cols = coords[:, 1:2] + step_cols[None, :]
    inside = (near_rows >= 0) & (near_rows < rows_total) & (near_cols >= 0) & (near_cols < cols_total)
    position = jnp.clip(near_rows, 0, rows_total - 1) * cols_total + jnp.clip(near_cols, 0, cols_total - 1)
    adjacency = jnp.where(inside, grid[position], -1).astype(jnp.int32)
    return (coords, adjacency)


def draw_blocks(key, part):
    coords, adjacency = block_layout(key)
    return coords


def draw_adjacency(key, part):
    coords, adjacency = block_layout(key)
    return adjacency


def set_ends(values, own_key, smallest, largest):
    spot = [jax.random.randint(jax.random.fold_in(own_key, axis), (), 0, length) for axis, length in enumerate(values.shape)]
    main_axis = values.shape.index(max(values.shape))
    beside = spot[:main_axis] + [(spot[main_axis] + 1) % values.shape[main_axis]] + spot[main_axis + 1:]
    return values.at[tuple(spot)].set(smallest).at[tuple(beside)].set(largest)


def levels(stream_key, extent, pieces, least, largest):
    level = 1.0
    for dim, shards_of in pieces:
        steps = jax.random.uniform(jax.random.fold_in(jax.random.fold_in(stream_key, 6), dim), (shards_of,), jnp.float32, least / len(pieces), largest / len(pieces))
        level = level * jnp.repeat(jnp.exp(steps), extent[dim] // shards_of).reshape((-1,) + (1,) * (len(extent) - 1 - dim))
    return level


def gaussian(key, extent, width, bound, pieces=(), kind=jnp.bfloat16):
    drawn = width * jax.random.normal(key, extent, jnp.float32)
    if pieces:
        drawn = drawn * levels(key, extent, pieces, -0.22, 0.18)
    return jnp.clip(drawn, -bound, bound).astype(kind)


def setup_inputs(seed: int = 0) -> dict:
    streams_of = jax.random.split(jax.random.key(seed), 8)
    air_state = gaussian(streams_of[0], (3, LEV, NX, NY), 1.0, 6.0, ((2, 4), (3, 8)), jnp.float32)
    level_set = jnp.clip(-3.0 + 8.0 * jax.random.uniform(streams_of[1], (NBLK, FB, FB), jnp.float32) ** levels(streams_of[1], (NBLK, FB, FB), ((0, 32),), -0.2, 0.2), -3.0, 5.0)
    fuel_left = jnp.clip(0.2 + 0.8 * jax.random.uniform(streams_of[2], (NBLK, FB, FB), jnp.float32) ** levels(streams_of[2], (NBLK, FB, FB), ((0, 32),), -0.2, 0.2), 0.2, 1.0)
    fuel_class = set_ends(jax.random.randint(streams_of[3], (NBLK, FB, FB), 0, NCLASS), jax.random.fold_in(streams_of[3], 1), 0, NCLASS - 1).astype(jnp.int32)
    fuel_props = jnp.clip(jnp.exp(jax.random.uniform(streams_of[4], (5, NCLASS), jnp.float32, math.log(0.5), math.log(2.0))), 0.5, 2.0)
    blocks = draw_blocks(jax.random.fold_in(streams_of[7], 71), 0)
    adjacency = draw_adjacency(jax.random.fold_in(streams_of[7], 71), 0)
    return dict(air_state=air_state, level_set=level_set, fuel_left=fuel_left, fuel_class=fuel_class, fuel_props=fuel_props, blocks=blocks, adjacency=adjacency)


step_time = 0.25
smoothing = 0.15
floor_square = 0.25
viscosity = 0.1
courant = 0.25
mixing = 0.1
heating = 2.0

def edges_of(current):
    return jnp.stack([current[:, 0, :], current[:, -1, :], current[:, :, 0], current[:, :, -1]], axis=1)

def facing_ghosts(every_edge, own_edges, neighbours):
    edge_rows = every_edge.reshape(-1, every_edge.shape[2])
    facing = jnp.array([1, 0, 3, 2], dtype=jnp.int32)
    picked_rows = (jnp.maximum(neighbours, 0) * 4 + facing[None, :]).astype(jnp.int32)
    taken = jnp.take(edge_rows, picked_rows, axis=0)
    return jnp.where(neighbours[:, :, None] >= 0, taken, own_edges)

def cell_table(fuel_class, fuel_props):
    scales = (0.3, 0.3, 4.0, 1.0, 3.0)
    return tuple((scales[entry] * jnp.take(fuel_props[entry], fuel_class) for entry in range(5)))

def advance(current, remaining, released, emitted, ghosts, wind_rows, wind_cols, table):
    base_rate, wind_factor, burn_time, heat_content, emission = table
    north = jnp.concatenate([ghosts[:, 0, None, :], current[:, :-1, :]], axis=1)
    south = jnp.concatenate([current[:, 1:, :], ghosts[:, 1, None, :]], axis=1)
    west = jnp.concatenate([ghosts[:, 2, :, None], current[:, :, :-1]], axis=2)
    east = jnp.concatenate([current[:, :, 1:], ghosts[:, 3, :, None]], axis=2)
    grad_rows = 0.5 * (south - north)
    grad_cols = 0.5 * (east - west)
    laplace = north + south + west + east - 4.0 * current
    length = jnp.sqrt(grad_rows * grad_rows + grad_cols * grad_cols + floor_square)
    along = (wind_rows * grad_rows + wind_cols * grad_cols) / length
    soft = jax.nn.softplus(along)
    spread = base_rate * (1.0 + wind_factor * soft * jnp.sqrt(soft))
    updated = current - step_time * spread * length + smoothing * laplace
    burning = 0.5 * (1.0 - jnp.tanh(updated))
    new_fuel = remaining * jnp.exp(-step_time * burning / burn_time)
    spent = remaining - new_fuel
    return (updated, new_fuel, released + heat_content * spent, emitted + emission * spent)

def air_field(air_state, index):
    field = air_state[index]
    wind_rows = air_state[0]
    wind_cols = air_state[1]
    padded = jnp.pad(field, ((0, 0), (1, 1), (1, 1)))
    north = padded[:, :-2, 1:-1]
    south = padded[:, 2:, 1:-1]
    west = padded[:, 1:-1, :-2]
    east = padded[:, 1:-1, 2:]
    upper = jnp.concatenate([field[1:], jnp.zeros_like(field[:1])], axis=0)
    lower = jnp.concatenate([jnp.zeros_like(field[:1]), field[:-1]], axis=0)
    laplace = north + south + west + east - 4.0 * field
    advect = wind_rows * (0.5 * (south - north)) + wind_cols * (0.5 * (east - west))
    return field + viscosity * laplace - courant * advect + mixing * (upper + lower - 2.0 * field)

def reference(air_state, level_set, fuel_left, fuel_class, fuel_props, blocks, adjacency):
    count = blocks.shape[0]
    rows_total = NX // BA
    cols_total = NY // BA
    surface = air_state[0:2, 0].reshape(2, rows_total, BA, cols_total, BA).transpose(1, 3, 0, 2, 4)
    block_wind = surface[blocks[:, 0], blocks[:, 1]]
    fine_wind = jnp.broadcast_to(block_wind[:, :, :, None, :, None], (count, 2, BA, REF, BA, REF)).reshape(count, 2, FB, FB)
    table = cell_table(fuel_class, fuel_props)
    current = level_set
    remaining = fuel_left
    released = jnp.zeros(level_set.shape, jnp.float32)
    emitted = jnp.zeros(level_set.shape, jnp.float32)
    for index in range(SUB):
        own_edges = edges_of(current)
        ghosts = facing_ghosts(own_edges, own_edges, adjacency)
        current, remaining, released, emitted = advance(current, remaining, released, emitted, ghosts, fine_wind[:, 0], fine_wind[:, 1], table)
    burning = 0.5 * (1.0 - jnp.tanh(current))
    column_heat = heating * released.reshape(count, BA, REF, BA, REF).mean(axis=(2, 4))
    grid = jnp.zeros((rows_total, cols_total, BA, BA), jnp.float32).at[blocks[:, 0], blocks[:, 1]].add(column_heat)
    heat_field = grid.transpose(0, 2, 1, 3).reshape(NX, NY)
    air_next = lax.map(partial(air_field, air_state), jnp.arange(3, dtype=jnp.int32))
    air_next = air_next.at[2, 0].add(heat_field)
    cells = count * FB * FB
    totals = jnp.stack([jnp.sum(burning) / cells, jnp.sum(emitted) / cells])
    return (air_next, current, remaining, totals)
```

```python
import math

import jax
import jax.numpy as jnp
from jax import lax
from jax.experimental import pallas as pl
from jax.experimental.pallas import tpu as pltpu
from jax.sharding import PartitionSpec as P


REF = 8
BA = 32
SUB = 10
PIECES = 32
LANES = 128

step_time = 0.25
smoothing = 0.15
floor_square = 0.25
viscosity = 0.1
courant = 0.25
mixing = 0.1
heating = 2.0

SIDE = 0
CORNER = 10
WIND = 12
COLS = 16
ROWS = 20
REC1 = 24
CORNER2 = 10
WINDA = 11
WINDB = 13
COLS2 = 15
ROWS2 = 19
REC2 = 24
HEAT_ROWS = 17

TOP = 8
EXT = 304
FIRST = 24

f32 = jnp.float32
i32 = jnp.int32


def lanes(shape=(8, LANES)):
    return lax.broadcasted_iota(i32, shape, len(shape) - 1)


def rolled(x, shift):
    return pltpu.roll(x, shift % LANES, x.ndim - 1)


def opposite(side):
    return (1, 0, 3, 2)[side]


def pick(table, index):
    return jnp.take_along_axis(table, index, axis=1, mode="promise_in_bounds")


def pack_kernel(pos, blocks, level, fuel_class, air_hbm, out, air, strip, edge, sem):
    load = pltpu.make_async_copy(air_hbm, air, sem)
    load.start()
    lane256 = lanes((256, LANES))
    lane16 = lanes((16, LANES))

    def place(row, first, values):
        out[pl.ds(first * REC1 + row, values.shape[0], stride=REC1), :] = values

    for q in range(2):
        fields = (level[q], fuel_class[q].astype(f32))
        turned = [
            jnp.where(lane256 < 64, field[:, :LANES], field[:, LANES:]).T for field in fields
        ]
        for side in range(4):
            for number, (field, turn) in enumerate(zip(fields, turned)):
                if side == 0:
                    rows = field[0:SUB, :]
                elif side == 1:
                    rows = field[256 - SUB : 256, :]
                elif side == 2:
                    rows = turn[0:SUB, :]
                else:
                    rows = turn[LANES - SUB : LANES, :]
                strip[side, 2 * SUB * number : 2 * SUB * number + SUB, :] = rows[:, :LANES]
                strip[side, 2 * SUB * number + SUB : 2 * SUB * (number + 1), :] = rows[:, LANES:]
            place(SIDE + q * 5 + side, 0, strip[side, 0:32, :])
            place(SIDE + q * 5 + 4, 8 * side, strip[side, 32:40, :])
        for number, field in enumerate(fields):
            half = jnp.where(
                lane16 < 16,
                field[240:256, :LANES],
                jnp.where(
                    lane16 < 32,
                    rolled(field[0:16, :LANES], 16),
                    jnp.where(
                        lane16 < 48,
                        rolled(field[0:16, LANES:], 48),
                        rolled(field[240:256, LANES:], 64),
                    ),
                ),
            )
            place(CORNER + q, 16 * number, jnp.where(lane16 < 64, half, rolled(half, 64)))

    load.wait()
    blank = jnp.zeros((PIECES, LANES), f32)
    for slot in range(4):
        place(WIND + slot, 0, blank)
    lane32 = lanes((32, LANES))
    tile_rows = 128 // BA

    def find(j, count):
        row = blocks[j, 0] - pos[0] * tile_rows
        col = blocks[j, 1] - pos[1] * tile_rows
        inside = (row >= 0) & (row < tile_rows) & (col >= 0) & (col < tile_rows)

        @pl.when(inside)
        def _():
            start = pl.multiple_of(row * BA, BA)
            u = air[pl.ds(start, BA), :]
            v = air[pl.ds(16 * 128 + start, BA), :]
            shift = LANES - col * BA
            u = pltpu.roll(u, shift, 1)
            v = pltpu.roll(v, shift, 1)
            half = jnp.where(lane32 < 32, u, rolled(v, 32))
            both = jnp.where(lane32 < 64, half, rolled(half, 64))
            out[pl.ds(WIND + count, PIECES, stride=REC1), :] = both

        return count + inside.astype(i32)

    lax.fori_loop(0, blocks.shape[0], find, jnp.int32(0))

    edge[0:48, :] = air[pl.ds(127, 48, stride=128), :]
    edge[48:96, :] = air[pl.ds(0, 48, stride=128), :]
    for group in range(3):
        place(ROWS + group, 0, edge[32 * group : 32 * group + 32, :])

    lane8 = lanes()

    def columns(chunk, carry):
        base = pl.multiple_of(chunk * 8, 8)
        total = jnp.zeros((8, LANES), f32)
        for plane in range(48):
            x = air[pl.ds(plane * 128 + base, 8), :]
            total = jnp.where(lane8 // 2 == plane, rolled(x, 1 + 2 * plane), total)
        edge[pl.ds(base, 8), :] = total
        return carry

    lax.fori_loop(0, 16, columns, 0)
    for group in range(4):
        place(COLS + group, 0, edge[32 * group : 32 * group + 32, :])
    if out.shape[0] > PIECES * REC1:
        out[PIECES * REC1 :, :] = jnp.zeros((out.shape[0] - PIECES * REC1, LANES), f32)


def select_kernel(across, down, pos, blocks, adjacency, received, out, wind_row, count):
    total = blocks.shape[0]
    devices = across * down
    relay = jnp.minimum(pos[0] * across + pos[1], PIECES - 1)
    lane1 = lanes((1, LANES))
    tile_rows = 128 // BA

    def clear(d, carry):
        count[d] = 0
        return carry

    lax.fori_loop(0, devices, clear, 0)

    def number(j, carry):
        tile = (blocks[j, 0] // tile_rows) * across + blocks[j, 1] // tile_rows
        slot = count[tile]
        count[tile] = slot + 1
        wind_row[j] = tile * REC1 + WIND + slot
        return carry

    lax.fori_loop(0, total, number, 0)

    def take(index):
        return received[pl.ds(index, 1), :]

    spare_side = relay // 8
    upper = relay >= 16
    lane_col = lane1 % 32 < 16
    first_half = lane1 < 64
    quarter = lane1 // 16

    def serve(d, carry):
        base = d * REC2

        def put(row, value):
            out[pl.ds(base + row, 1), :] = value

        corner_rows = []
        for q in range(2):
            i = 2 * d + q
            near = [adjacency[i, s] for s in range(4)]
            safe = [jnp.maximum(near[s], 0) for s in range(4)]

            def diagonal(s, t):
                by_row = adjacency[safe[s], t]
                by_col = adjacency[safe[t], s]
                return jnp.maximum(jnp.where(near[s] >= 0, by_row, jnp.where(near[t] >= 0, by_col, 0)), 0)

            nw, ne, sw, se = diagonal(0, 2), diagonal(0, 3), diagonal(1, 2), diagonal(1, 3)

            def side_row(j, s):
                return (j // 2) * REC1 + SIDE + (j % 2) * 5 + s

            def corner_row(j):
                return (j // 2) * REC1 + CORNER + j % 2

            for s in range(4):
                put(SIDE + q * 5 + s, take(side_row(safe[s], opposite(s))))
            spare = jnp.where(
                spare_side == 0,
                safe[1],
                jnp.where(spare_side == 1, safe[0], jnp.where(spare_side == 2, safe[3], safe[2])),
            )
            put(SIDE + q * 5 + 4, take(side_row(spare, 4)))
            corner_rows += [take(corner_row(j)) for j in (ne, se, sw, nw)]
            put(
                WINDA + q,
                jnp.where(
                    first_half,
                    take(wind_row[i]),
                    take(wind_row[jnp.where(upper, safe[0], safe[1])]),
                ),
            )
            east = take(wind_row[safe[3]])
            west = take(wind_row[safe[2]])
            corner_east = take(wind_row[jnp.where(upper, ne, se)])
            corner_west = take(wind_row[jnp.where(upper, nw, sw)])
            put(
                WINDB + q,
                jnp.where(
                    lane_col,
                    jnp.where(first_half, east, corner_east),
                    jnp.where(first_half, west, corner_west),
                ),
            )
        merged = corner_rows[7]
        for k in range(7):
            merged = jnp.where(quarter == k, corner_rows[k], merged)
        put(CORNER2, merged)
        a = d // across
        b = d % across
        north = jnp.where(a > 0, d - across, d)
        south = jnp.where(a < down - 1, d + across, d)
        west_tile = jnp.where(b > 0, d - 1, d)
        east_tile = jnp.where(b < across - 1, d + 1, d)
        odd = lane1 % 2 == 1
        for group in range(4):
            put(
                COLS2 + group,
                jnp.where(
                    odd,
                    take(east_tile * REC1 + COLS + group),
                    take(west_tile * REC1 + COLS + group),
                ),
            )
        put(ROWS2, take(north * REC1 + ROWS))
        put(ROWS2 + 1, take(jnp.where(relay < 16, north, south) * REC1 + ROWS + 1))
        put(ROWS2 + 2, take(south * REC1 + ROWS + 2))
        for row in range(ROWS2 + 3, REC2):
            put(row, jnp.zeros((1, LANES), f32))
        return carry

    lax.fori_loop(0, devices, serve, 0)


MAIN = (0, 1, 3, 4)


def fire_kernel(
    across,
    down,
    pos,
    adjacency,
    props,
    received,
    level,
    fuel_left,
    fuel_class,
    air_hbm,
    level_out,
    fuel_out,
    heat_out,
    air_out,
    cur,
    base_rate,
    wind_rate,
    wind,
    strips,
    turned,
    tanh_sum,
    links,
    row_heat,
    air,
    air_new,
    sem_in,
    sem_out,
):
    load = pltpu.make_async_copy(air_hbm, air.at[:, 1:17, 8:136, :], sem_in)
    load.start()
    lane = lanes()
    sub = lax.broadcasted_iota(i32, (8, LANES), 0)
    lane32 = lanes((32, LANES))
    own = 2 * (pos[0] * across + pos[1])

    def got(row, first=0, size=PIECES):
        return received[pl.ds(first * REC2 + row, size, stride=REC2), :]

    table_base = jnp.broadcast_to(0.125 * 0.3 * props[0:1, :], (8, LANES))
    table_wind = table_base * jnp.broadcast_to(0.3 * props[1:2, :], (8, LANES))
    log2e = math.log2(math.e)
    table_burn = jnp.broadcast_to((-0.5 * step_time * log2e / 4.0) / props[2:3, :], (8, LANES))
    table_heat = jnp.broadcast_to(props[3:4, :], (8, LANES))
    table_emit = jnp.broadcast_to(3.0 * props[4:5, :], (8, LANES))

    turned[...] = jnp.zeros(turned.shape, f32)
    for q in range(2):
        for s in range(4):
            strips[0:32, :] = got(SIDE + q * 5 + s)
            strips[32:40, :] = got(SIDE + q * 5 + 4, 8 * opposite(s), 8)
            for number in range(2):
                low = strips[2 * SUB * number : 2 * SUB * number + SUB, :]
                high = strips[2 * SUB * number + SUB : 2 * SUB * (number + 1), :]
                if s < 2:
                    at = FIRST - SUB if s == 0 else FIRST + 256
                    target = cur.at[0] if number == 0 else cur.at[1]
                    target[3 * q, at : at + SUB, :] = low
                    target[3 * q + 1, at : at + SUB, :] = high
                else:
                    at = (54, 118)[q] if s == 2 else (0, 64)[q]
                    turned[number, at : at + SUB, :LANES] = low
                    turned[number, at : at + SUB, LANES:] = high
    for number in range(2):
        cur[number, 2, FIRST : FIRST + 256, :] = turned[number].T
        corner = got(CORNER2, 16 * number, 16)
        cur[number, 2, TOP : TOP + 16, :] = corner
        cur[number, 2, FIRST + 256 : FIRST + 272, :] = jnp.where(
            lanes((16, LANES)) % 64 < 32, rolled(corner, -16), rolled(corner, 16)
        )
    for q in range(2):
        for half in range(2):
            cur[0, 3 * q + half, FIRST : FIRST + 256, :] = level[q, :, LANES * half : LANES * (half + 1)]
            cur[1, 3 * q + half, FIRST : FIRST + 256, :] = fuel_class[
                q, :, LANES * half : LANES * (half + 1)
            ].astype(f32)

    def rates(chunk, carry):
        at = pl.multiple_of(chunk * 8, 8)
        for t in range(5):
            kind = cur[1, t, pl.ds(at, 8), :].astype(i32) & 127
            base_rate[t, pl.ds(at, 8), :] = pick(table_base, kind)
            wind_rate[t, pl.ds(at, 8), :] = pick(table_wind, kind)
        return carry

    lax.fori_loop(1, 37, rates, 0)

    inner = lane % 64
    side_col = jnp.where(inner < 16, inner // 8, jnp.where(inner >= 48, 30 + (inner - 48) // 8, 0))
    for k in range(2):
        for t in range(5):
            for quarter in range(4):
                for outer in (0, 64):
                    if outer and quarter in (1, 2):
                        continue
                    at = outer + k * 32
                    if t == 2:
                        west = got(WINDB, 8 * quarter, 8)
                        east = got(WINDB + 1, 8 * quarter, 8)
                        index = side_col + at
                        value = jnp.where(lane < 64, pick(west, index), pick(east, index))
                    else:
                        source = got(WINDA + t // 3, 8 * quarter, 8)
                        value = pick(source, lane // 8 + (at + 16 * (t % 3)))
                    value = value * log2e
                    if not outer:
                        wind[k, t, 3 + 8 * quarter : 11 + 8 * quarter, :] = value
                    elif quarter == 3:
                        wind[k, t, 1:3, :] = value[6:8, :]
                    else:
                        wind[k, t, 35:37, :] = value[0:2, :]

    def there(j):
        return j >= 0

    across_links = []
    groups = []
    for q in range(2):
        i = own + q
        near = [adjacency[i, s] for s in range(4)]
        safe = [jnp.maximum(near[s], 0) for s in range(4)]

        def joined(s, t):
            return there(near[s]) & there(adjacency[safe[s], t])

        groups.append([(there(near[s]), joined(2, s), joined(3, s)) for s in range(2)])
        across_links.append([[joined(0, t), there(near[t]), joined(1, t)] for t in (2, 3)])

    def as_int(flag):
        return jnp.where(flag, 1, 0)

    for line in range(2):
        for q in range(2):
            mid, west, east = groups[q][line]
            row = jnp.broadcast_to(as_int(mid), (8, LANES))
            links[line, 3 * q] = row
            links[line, 3 * q + 1] = row
        w0, e0 = groups[0][line][1:]
        w1, e1 = groups[1][line][1:]
        links[line, 2] = jnp.where(
            lane < 32,
            as_int(e0),
            jnp.where(lane < 64, as_int(w0), jnp.where(lane < 96, as_int(e1), as_int(w1))),
        )

    is0 = lane == 0
    is63 = lane == 63
    is64 = lane == 64
    is127 = lane == 127
    tanh_sum[...] = jnp.zeros(tanh_sum.shape, f32)

    def make_masks(region):
        (w0, e0), (w1, e1) = [
            [as_int(across_links[q][t][region]) for t in range(2)] for q in range(2)
        ]
        on = [jnp.broadcast_to(flag, (8, LANES)) > 0 for flag in (w0, e0, w1, e1)]
        return on

    def update(source, target, chunk, masks, rows_edge, main):
        lw0, le0, lw1, le1 = masks
        at = chunk * 8
        x = [cur[source, t, pl.ds(at, 8), :] for t in range(5)]
        up = [cur[source, t, pl.ds(at - 1, 8), :] for t in range(5)]
        dn = [cur[source, t, pl.ds(at + 1, 8), :] for t in range(5)]
        if rows_edge is not None:
            kind, line, row = rows_edge
            for t in range(5):
                broken = (sub == row) & (links[line, t] == 0)
                if kind == "up":
                    up[t] = jnp.where(broken, x[t], up[t])
                else:
                    dn[t] = jnp.where(broken, x[t], dn[t])
        right = [rolled(v, 1) for v in x]
        left = [rolled(v, -1) for v in x]
        h = x[2]
        west = [
            jnp.where(is0, jnp.where(lw0, rolled(h, 65), x[0]), right[0]),
            jnp.where(is0, right[0], right[1]),
            jnp.where(
                is0,
                jnp.where(le0, right[1], h),
                jnp.where(is64, jnp.where(le1, rolled(x[4], 65), h), right[2]),
            ),
            jnp.where(is0, jnp.where(lw1, right[2], x[3]), right[3]),
            jnp.where(is0, right[3], right[4]),
        ]
        east = [
            jnp.where(is127, left[1], left[0]),
            jnp.where(is127, jnp.where(le0, left[2], x[1]), left[1]),
            jnp.where(
                is127,
                jnp.where(lw1, left[3], h),
                jnp.where(is63, jnp.where(lw0, rolled(x[0], 63), h), left[2]),
            ),
            jnp.where(is127, left[4], left[3]),
            jnp.where(is127, jnp.where(le1, rolled(h, -65), x[4]), left[4]),
        ]
        for t in range(5):
            diff_rows = dn[t] - up[t]
            diff_cols = east[t] - west[t]
            around = (dn[t] + up[t]) + (east[t] + west[t])
            square = diff_rows * diff_rows + (diff_cols * diff_cols + 4.0 * floor_square)
            inverse = lax.rsqrt(square)
            wind_r = wind[0, t, pl.ds(chunk, 1), :]
            wind_c = wind[1, t, pl.ds(chunk, 1), :]
            along = (wind_r * diff_rows + wind_c * diff_cols) * inverse
            soft = jnp.log(1.0 + jnp.exp2(along))
            power = soft * soft * lax.rsqrt(soft)
            b = base_rate[t, pl.ds(at, 8), :]
            w = wind_rate[t, pl.ds(at, 8), :]
            new = ((1.0 - 4.0 * smoothing) * x[t] + smoothing * around) - (b + w * power) * (
                square * inverse
            )
            cur[target, t, pl.ds(at, 8), :] = new
            if main and t != 2:
                m = t - t // 3
                tanh_sum[m, pl.ds(at - FIRST, 8), :] += jnp.tanh(new)

    above = make_masks(0)
    within = make_masks(1)
    below = make_masks(2)

    def substep(step, carry):
        source = step & 1
        target = 1 - source
        update(source, target, 1, above, None, False)
        update(source, target, 2, above, ("down", 0, 7), False)
        update(source, target, 3, within, ("up", 0, 0), True)

        def middle(chunk, inner_carry):
            update(source, target, chunk, within, None, True)
            return inner_carry

        lax.fori_loop(4, 34, middle, 0)
        update(source, target, 34, within, ("down", 1, 7), True)
        update(source, target, 35, below, ("up", 1, 0), False)
        update(source, target, 36, below, None, False)
        return carry

    lax.fori_loop(0, SUB, substep, 0)

    last = SUB % 2

    def finish(chunk, sums):
        burn, emit = sums
        at = pl.multiple_of(chunk * 8, 8)
        for q in range(2):
            for half in range(2):
                t = 3 * q + half
                cols = slice(LANES * half, LANES * (half + 1))
                final = cur[last, t, pl.ds(FIRST + at, 8), :]
                level_out[q, pl.ds(at, 8), cols] = final
                burn = burn + (0.5 - 0.5 * jnp.tanh(final))
                kind = fuel_class[q, pl.ds(at, 8), cols]
                fuel = fuel_left[q, pl.ds(at, 8), cols]
                power = pick(table_burn, kind) * (float(SUB) - tanh_sum[2 * q + half, pl.ds(at, 8), :])
                new_fuel = fuel * jnp.exp2(power)
                fuel_out[q, pl.ds(at, 8), cols] = new_fuel
                spent = fuel - new_fuel
                emit = emit + pick(table_emit, kind) * spent
                released = pick(table_heat, kind) * spent
                row_heat[2 * q + half, pl.ds(chunk, 1), :] = jnp.sum(released, axis=0, keepdims=True)
        return burn, emit

    blank = jnp.zeros((8, LANES), f32)
    burn, emit = lax.fori_loop(0, 32, finish, (blank, blank))
    source_lane = lax.broadcasted_iota(i32, (LANES, LANES), 0) // REF
    target_lane = lanes((LANES, LANES))
    for q in range(2):
        packed = blank
        for g in range(4):
            for half in range(2):
                gather = jnp.where(
                    target_lane == 32 * g + 16 * half + source_lane, heating / (REF * REF), 0.0
                ).astype(f32)
                packed = packed + jnp.dot(
                    row_heat[2 * q + half, 8 * g : 8 * g + 8, :],
                    gather,
                    precision=lax.Precision.HIGHEST,
                    preferred_element_type=f32,
                )
        heat_out[8 * q : 8 * q + 8, :] = packed
    burn_sum = jnp.sum(jnp.sum(burn, axis=0, keepdims=True), axis=1, keepdims=True)
    emit_sum = jnp.sum(jnp.sum(emit, axis=0, keepdims=True), axis=1, keepdims=True)
    lane1 = lanes((1, LANES))
    heat_out[16:17, :] = jnp.where(lane1 == 0, burn_sum, jnp.where(lane1 == 1, emit_sum, 0.0))

    load.wait()
    zero = jnp.zeros((128, LANES), f32)
    for f in range(3):
        air[f, 0, 8:136, :] = zero
        air[f, 17, 8:136, :] = zero
    keep_north = jnp.where(pos[0] > 0, 1.0, 0.0).astype(f32)
    keep_south = jnp.where(pos[0] < down - 1, 1.0, 0.0).astype(f32)
    keep_west = jnp.where(pos[1] > 0, 1.0, 0.0).astype(f32)
    keep_east = jnp.where(pos[1] < across - 1, 1.0, 0.0).astype(f32)
    for group in range(3):
        strips[...] = jnp.zeros(strips.shape, f32)
        rows = got(ROWS2 + group)
        for p in range(32):
            number = 32 * group + p
            plane = number % 48
            at = 7 if number < 48 else 136
            keep = keep_north if number < 48 else keep_south
            air[plane // 16, plane % 16 + 1, at : at + 1, :] = rows[p : p + 1, :] * keep
    sides = []
    for group in range(4):
        sides.append(got(COLS2 + group) * jnp.where(lane32 % 2 == 1, keep_east, keep_west))
    for group in range(4):
        turned[0, 32 * group : 32 * group + 32, :LANES] = sides[group]

    def air_level(number, carry):
        def air_rows(chunk, inner_carry):
            at = 8 + chunk * 8
            halo = turned[0, pl.ds(chunk * 8, 8), :LANES]
            u = air[0, number + 1, pl.ds(at, 8), :]
            v = air[1, number + 1, pl.ds(at, 8), :]
            for f in range(3):
                x = u if f == 0 else v if f == 1 else air[2, number + 1, pl.ds(at, 8), :]
                up = air[f, number + 1, pl.ds(at - 1, 8), :]
                dn = air[f, number + 1, pl.ds(at + 1, 8), :]
                over = air[f, number + 2, pl.ds(at, 8), :]
                under = air[f, number, pl.ds(at, 8), :]
                mine = pltpu.roll(halo, LANES - 1 - 2 * (f * 16 + number), 1)
                west = rolled(jnp.where(is127, mine, x), 1)
                east = rolled(jnp.where(is0, mine, x), -1)
                around = (up + dn) + (west + east)
                advect = u * (dn - up) + v * (east - west)
                air_new[f, number, pl.ds(chunk * 8, 8), :] = (
                    (1.0 - 4.0 * viscosity - 2.0 * mixing) * x
                    + viscosity * around
                    - (0.5 * courant) * advect
                    + mixing * (over + under)
                )
            return inner_carry

        lax.fori_loop(0, 16, air_rows, 0)
        return carry

    lax.fori_loop(0, 16, air_level, 0)
    store = pltpu.make_async_copy(air_new, air_out, sem_out)
    store.start()
    store.wait()


def heat_kernel(cells, pos, blocks, gathered, air_in, air_out, totals, plane, sem):
    load = pltpu.make_async_copy(air_in.at[2, 0], plane, sem)
    load.start()
    devices = gathered.shape[0] // HEAT_ROWS
    sums = jnp.sum(
        gathered[pl.ds(16, devices, stride=HEAT_ROWS), :], axis=0, keepdims=True
    )
    totals[...] = sums * (1.0 / cells)
    load.wait()
    lane = lanes()
    tile_rows = 128 // BA

    def place(j, carry):
        row = blocks[j, 0] - pos[0] * tile_rows
        col = blocks[j, 1] - pos[1] * tile_rows
        inside = (row >= 0) & (row < tile_rows) & (col >= 0) & (col < tile_rows)

        @pl.when(inside)
        def _():
            heat = gathered[pl.ds((j // 2) * HEAT_ROWS + 8 * (j % 2), 8), :]
            for g in range(4):
                moved = pltpu.roll(heat, (col - g + 4) * BA % LANES, 1)
                at = pl.multiple_of(row * BA + 8 * g, 8)
                plane[pl.ds(at, 8), :] += jnp.where(lane // BA == col, moved, 0.0)

        return carry

    lax.fori_loop(0, blocks.shape[0], place, 0)
    store = pltpu.make_async_copy(plane, air_out.at[2, 0], sem)
    store.start()
    store.wait()


def local(air_state, level_set, fuel_left, fuel_class, fuel_props, blocks, adjacency):
    down = lax.axis_size("gx")
    across = lax.axis_size("gy")
    devices = down * across
    both = ("gx", "gy")
    pos = jnp.stack([lax.axis_index("gx"), lax.axis_index("gy")]).astype(i32)
    smem = pl.BlockSpec(memory_space=pltpu.SMEM)
    vmem = pl.BlockSpec(memory_space=pltpu.VMEM)
    anywhere = pl.BlockSpec(memory_space=pl.ANY)
    packed = pl.pallas_call(
        pack_kernel,
        out_shape=jax.ShapeDtypeStruct((devices * REC1, LANES), f32),
        in_specs=[smem, smem, vmem, vmem, anywhere],
        out_specs=vmem,
        scratch_shapes=[
            pltpu.VMEM((48 * 128, LANES), f32),
            pltpu.VMEM((4, 40, LANES), f32),
            pltpu.VMEM((128, LANES), f32),
            pltpu.SemaphoreType.DMA(()),
        ],
        name="pack",
    )(pos, blocks, level_set, fuel_class, air_state.reshape(48 * 128, LANES))
    relayed = lax.all_to_all(packed.reshape(devices, REC1, LANES), both, 0, 0)
    chosen = pl.pallas_call(
        lambda *refs: select_kernel(across, down, *refs),
        out_shape=jax.ShapeDtypeStruct((devices * REC2, LANES), f32),
        in_specs=[smem, smem, smem, vmem],
        out_specs=vmem,
        scratch_shapes=[pltpu.SMEM((blocks.shape[0],), i32), pltpu.SMEM((devices,), i32)],
        name="select",
    )(pos, blocks, adjacency, relayed.reshape(devices * REC1, LANES))
    received = lax.all_to_all(chosen.reshape(devices, REC2, LANES), both, 0, 0)
    props = jnp.pad(fuel_props, ((0, 3), (0, LANES - fuel_props.shape[1])), constant_values=1.0)
    level_next, fuel_next, heat, air_next = pl.pallas_call(
        lambda *refs: fire_kernel(across, down, *refs),
        out_shape=(
            jax.ShapeDtypeStruct(level_set.shape, f32),
            jax.ShapeDtypeStruct(level_set.shape, f32),
            jax.ShapeDtypeStruct((HEAT_ROWS, LANES), f32),
            jax.ShapeDtypeStruct(air_state.shape, f32),
        ),
        in_specs=[smem, smem, vmem, vmem, vmem, vmem, vmem, anywhere],
        out_specs=(vmem, vmem, vmem, anywhere),
        scratch_shapes=[
            pltpu.VMEM((2, 5, EXT, LANES), f32),
            pltpu.VMEM((5, EXT, LANES), f32),
            pltpu.VMEM((5, EXT, LANES), f32),
            pltpu.VMEM((2, 5, 40, LANES), f32),
            pltpu.VMEM((40, LANES), f32),
            pltpu.VMEM((2, LANES, 256), f32),
            pltpu.VMEM((4, 256, LANES), f32),
            pltpu.VMEM((2, 5, 8, LANES), i32),
            pltpu.VMEM((4, 32, LANES), f32),
            pltpu.VMEM((3, 18, 144, LANES), f32),
            pltpu.VMEM((3, 16, 128, LANES), f32),
            pltpu.SemaphoreType.DMA(()),
            pltpu.SemaphoreType.DMA(()),
        ],
        name="fire",
    )(
        pos,
        adjacency,
        props,
        received.reshape(devices * REC2, LANES)[: PIECES * REC2],
        level_set,
        fuel_left,
        fuel_class,
        air_state,
    )
    spread = jnp.broadcast_to(
        heat.reshape(1, 1, HEAT_ROWS * LANES), (devices, 1, HEAT_ROWS * LANES)
    )
    gathered = lax.all_to_all(spread, both, 0, 0).reshape(devices * HEAT_ROWS, LANES)
    cells = blocks.shape[0] * level_set.shape[1] * level_set.shape[2]
    air_next, totals = pl.pallas_call(
        lambda *refs: heat_kernel(cells, *refs),
        out_shape=(
            jax.ShapeDtypeStruct(air_state.shape, f32),
            jax.ShapeDtypeStruct((1, LANES), f32),
        ),
        in_specs=[smem, smem, vmem, anywhere],
        out_specs=(anywhere, vmem),
        scratch_shapes=[pltpu.VMEM((128, LANES), f32), pltpu.SemaphoreType.DMA(())],
        input_output_aliases={3: 0},
        name="heat",
    )(pos, blocks, gathered, air_next)
    return (air_next, level_next, fuel_next, totals[0, 0:2])


def solution(mesh):
    in_specs = (
        P(None, None, "gx", "gy"),
        P(("gx", "gy"), None, None),
        P(("gx", "gy"), None, None),
        P(("gx", "gy"), None, None),
        P(),
        P(),
        P(),
    )
    out_specs = (
        P(None, None, "gx", "gy"),
        P(("gx", "gy"), None, None),
        P(("gx", "gy"), None, None),
        P(),
    )
    return jax.shard_map(local, mesh=mesh, in_specs=in_specs, out_specs=out_specs, check_vma=False)
```

```python
import math

import jax
import jax.numpy as jnp
from jax import lax
from jax.experimental import pallas as pl
from jax.experimental.pallas import tpu as pltpu
from jax.sharding import PartitionSpec as P


REF = 8
BA = 32
SUB = 10
PIECES = 32
LANES = 128
UNROLL = 30
RATE_UNROLL = 12
FINISH_UNROLL = 16
AIR_UNROLL = 16

step_time = 0.25
smoothing = 0.15
floor_square = 0.25
viscosity = 0.1
courant = 0.25
mixing = 0.1
heating = 2.0

SIDE = 0
CORNER = 10
WIND = 12
COLS = 16
ROWS = 20
REC1 = 24
CORNER2 = 10
WINDA = 11
WINDB = 13
COLS2 = 15
ROWS2 = 19
REC2 = 24
HEAT_ROWS = 17

TOP = 8
EXT = 304
FIRST = 24

f32 = jnp.float32
i32 = jnp.int32


def lanes(shape=(8, LANES)):
    return lax.broadcasted_iota(i32, shape, len(shape) - 1)


def rolled(x, shift):
    return pltpu.roll(x, shift % LANES, x.ndim - 1)


def opposite(side):
    return (1, 0, 3, 2)[side]


def pick(table, index):
    return jnp.take_along_axis(table, index, axis=1, mode="promise_in_bounds")


def pack_kernel(pos, blocks, level, fuel_class, air_hbm, out, air, strip, edge, sem):
    load = pltpu.make_async_copy(air_hbm, air, sem)
    load.start()
    lane256 = lanes((256, LANES))
    lane16 = lanes((16, LANES))

    def place(row, first, values):
        out[pl.ds(first * REC1 + row, values.shape[0], stride=REC1), :] = values

    for q in range(2):
        fields = (level[q], fuel_class[q].astype(f32))
        turned = [
            jnp.where(lane256 < 64, field[:, :LANES], field[:, LANES:]).T for field in fields
        ]
        for side in range(4):
            for number, (field, turn) in enumerate(zip(fields, turned)):
                if side == 0:
                    rows = field[0:SUB, :]
                elif side == 1:
                    rows = field[256 - SUB : 256, :]
                elif side == 2:
                    rows = turn[0:SUB, :]
                else:
                    rows = turn[LANES - SUB : LANES, :]
                strip[side, 2 * SUB * number : 2 * SUB * number + SUB, :] = rows[:, :LANES]
                strip[side, 2 * SUB * number + SUB : 2 * SUB * (number + 1), :] = rows[:, LANES:]
            place(SIDE + q * 5 + side, 0, strip[side, 0:32, :])
            place(SIDE + q * 5 + 4, 8 * side, strip[side, 32:40, :])
        for number, field in enumerate(fields):
            half = jnp.where(
                lane16 < 16,
                field[240:256, :LANES],
                jnp.where(
                    lane16 < 32,
                    rolled(field[0:16, :LANES], 16),
                    jnp.where(
                        lane16 < 48,
                        rolled(field[0:16, LANES:], 48),
                        rolled(field[240:256, LANES:], 64),
                    ),
                ),
            )
            place(CORNER + q, 16 * number, jnp.where(lane16 < 64, half, rolled(half, 64)))

    load.wait()
    blank = jnp.zeros((PIECES, LANES), f32)
    for slot in range(4):
        place(WIND + slot, 0, blank)
    lane32 = lanes((32, LANES))
    tile_rows = 128 // BA

    def find(j, count):
        row = blocks[0, j] - pos[0] * tile_rows
        col = blocks[1, j] - pos[1] * tile_rows
        inside = (row >= 0) & (row < tile_rows) & (col >= 0) & (col < tile_rows)

        @pl.when(inside)
        def _():
            start = pl.multiple_of(row * BA, BA)
            u = air[pl.ds(start, BA), :]
            v = air[pl.ds(16 * 128 + start, BA), :]
            shift = LANES - col * BA
            u = pltpu.roll(u, shift, 1)
            v = pltpu.roll(v, shift, 1)
            half = jnp.where(lane32 < 32, u, rolled(v, 32))
            both = jnp.where(lane32 < 64, half, rolled(half, 64))
            out[pl.ds(WIND + count, PIECES, stride=REC1), :] = both

        return count + inside.astype(i32)

    lax.fori_loop(0, blocks.shape[1], find, jnp.int32(0))

    edge[0:48, :] = air[pl.ds(127, 48, stride=128), :]
    edge[48:96, :] = air[pl.ds(0, 48, stride=128), :]
    for group in range(3):
        place(ROWS + group, 0, edge[32 * group : 32 * group + 32, :])

    lane8 = lanes()

    def columns(chunk, carry):
        base = pl.multiple_of(chunk * 8, 8)
        total = jnp.zeros((8, LANES), f32)
        for plane in range(48):
            x = air[pl.ds(plane * 128 + base, 8), :]
            total = jnp.where(lane8 // 2 == plane, rolled(x, 1 + 2 * plane), total)
        edge[pl.ds(base, 8), :] = total
        return carry

    lax.fori_loop(0, 16, columns, 0)
    for group in range(4):
        place(COLS + group, 0, edge[32 * group : 32 * group + 32, :])
    if out.shape[0] > PIECES * REC1:
        out[PIECES * REC1 :, :] = jnp.zeros((out.shape[0] - PIECES * REC1, LANES), f32)


WORDS = 40


def index_kernel(across, down, pos, blocks, adjacency, out, wind_row, count):
    total = blocks.shape[1]
    devices = across * down
    relay = jnp.minimum(pos[0] * across + pos[1], PIECES - 1)
    tile_rows = 128 // BA

    def clear(d, carry):
        count[d] = 0
        return carry

    lax.fori_loop(0, devices, clear, 0)

    def number(j, carry):
        tile = (blocks[0, j] // tile_rows) * across + blocks[1, j] // tile_rows
        slot = count[tile]
        count[tile] = slot + 1
        wind_row[j] = tile * REC1 + WIND + slot
        return carry

    lax.fori_loop(0, total, number, 0)
    spare_side = relay // 8
    upper = relay >= 16

    def serve(d, carry):
        base = d * WORDS
        for q in range(2):
            i = 2 * d + q
            near = [adjacency[s, i] for s in range(4)]
            safe = [jnp.maximum(near[s], 0) for s in range(4)]

            def diagonal(s, t):
                by_row = adjacency[t, safe[s]]
                by_col = adjacency[s, safe[t]]
                return jnp.maximum(jnp.where(near[s] >= 0, by_row, jnp.where(near[t] >= 0, by_col, 0)), 0)

            nw, ne, sw, se = diagonal(0, 2), diagonal(0, 3), diagonal(1, 2), diagonal(1, 3)

            def side_row(j, s):
                return (j // 2) * REC1 + SIDE + (j % 2) * 5 + s

            for s in range(4):
                out[base + 5 * q + s] = side_row(safe[s], opposite(s))
            spare = jnp.where(
                spare_side == 0,
                safe[1],
                jnp.where(spare_side == 1, safe[0], jnp.where(spare_side == 2, safe[3], safe[2])),
            )
            out[base + 5 * q + 4] = side_row(spare, 4)
            for k, j in enumerate((ne, se, sw, nw)):
                out[base + 10 + 4 * q + k] = (j // 2) * REC1 + CORNER + j % 2
            winds = (
                i,
                jnp.where(upper, safe[0], safe[1]),
                safe[3],
                safe[2],
                jnp.where(upper, ne, se),
                jnp.where(upper, nw, sw),
            )
            for k, j in enumerate(winds):
                out[base + 18 + 6 * q + k] = wind_row[j]
        a = d // across
        b = d % across
        north = jnp.where(a > 0, d - across, d)
        south = jnp.where(a < down - 1, d + across, d)
        out[base + 30] = jnp.where(b < across - 1, d + 1, d) * REC1 + COLS
        out[base + 31] = jnp.where(b > 0, d - 1, d) * REC1 + COLS
        out[base + 32] = north * REC1 + ROWS
        out[base + 33] = jnp.where(relay < 16, north, south) * REC1 + ROWS + 1
        out[base + 34] = south * REC1 + ROWS + 2
        return carry

    lax.fori_loop(0, devices, serve, 0)


def select_kernel(index, received, out):
    lane1 = lanes((1, LANES))
    lane_col = lane1 % 32 < 16
    first_half = lane1 < 64
    quarter = lane1 // 16
    odd = lane1 % 2 == 1

    def one(d):
        def take(word, more=0):
            return received[pl.ds(index[d * WORDS + word] + more, 1), :]

        def put(row, value):
            out[pl.ds(d * REC2 + row, 1), :] = value

        for row in range(10):
            put(SIDE + row, take(row))
        merged = take(17)
        for k in range(7):
            merged = jnp.where(quarter == k, take(10 + k), merged)
        put(CORNER2, merged)
        for q in range(2):
            own, beyond, east, west, corner_east, corner_west = [take(18 + 6 * q + k) for k in range(6)]
            put(WINDA + q, jnp.where(first_half, own, beyond))
            put(
                WINDB + q,
                jnp.where(
                    lane_col,
                    jnp.where(first_half, east, corner_east),
                    jnp.where(first_half, west, corner_west),
                ),
            )
        for group in range(4):
            put(COLS2 + group, jnp.where(odd, take(30, group), take(31, group)))
        for group in range(3):
            put(ROWS2 + group, take(32 + group))
        for row in range(ROWS2 + 3, REC2):
            put(row, jnp.zeros((1, LANES), f32))

    def serve(pair, carry):
        one(2 * pair)
        one(2 * pair + 1)
        return carry

    lax.fori_loop(0, out.shape[0] // REC2 // 2, serve, 0)


def fire_kernel(
    across,
    down,
    pos,
    adjacency,
    props,
    received,
    level,
    fuel_left,
    fuel_class,
    level_out,
    fuel_out,
    heat_out,
    cur_a,
    cur_b,
    base_rate,
    wind_rate,
    wind,
    strips,
    turned,
    tanh_sum,
    links,
    row_heat,
):
    cur = (cur_a, cur_b)
    lane = lanes()
    sub = lax.broadcasted_iota(i32, (8, LANES), 0)
    lane32 = lanes((32, LANES))
    own = 2 * (pos[0] * across + pos[1])

    def got(row, first=0, size=PIECES):
        return received[pl.ds(first * REC2 + row, size, stride=REC2), :]

    def table(value):
        row = jnp.zeros((8, LANES), f32)
        for kind in range(props.shape[1]):
            row = jnp.where(lane == kind, value(kind), row)
        return row

    log2e = math.log2(math.e)
    table_base = table(lambda c: 0.125 * 0.3 * props[0, c])
    table_wind = table_base * table(lambda c: 0.3 * props[1, c])
    table_burn = (-0.5 * step_time * log2e / 4.0) / jnp.where(
        lane < props.shape[1], table(lambda c: props[2, c]), 1.0
    )
    table_heat = table(lambda c: props[3, c])
    table_emit = table(lambda c: 3.0 * props[4, c])

    turned[...] = jnp.zeros(turned.shape, f32)
    for q in range(2):
        for s in range(4):
            strips[0:32, :] = got(SIDE + q * 5 + s)
            strips[32:40, :] = got(SIDE + q * 5 + 4, 8 * opposite(s), 8)
            for number in range(2):
                low = strips[2 * SUB * number : 2 * SUB * number + SUB, :]
                high = strips[2 * SUB * number + SUB : 2 * SUB * (number + 1), :]
                if s < 2:
                    at = FIRST - SUB if s == 0 else FIRST + 256
                    target = cur[number]
                    target[3 * q, at : at + SUB, :] = low
                    target[3 * q + 1, at : at + SUB, :] = high
                else:
                    at = (54, 118)[q] if s == 2 else (0, 64)[q]
                    turned[number, at : at + SUB, :LANES] = low
                    turned[number, at : at + SUB, LANES:] = high
    for number in range(2):
        cur[number][2, FIRST : FIRST + 256, :] = turned[number].T
        corner = got(CORNER2, 16 * number, 16)
        cur[number][2, TOP : TOP + 16, :] = corner
        cur[number][2, FIRST + 256 : FIRST + 272, :] = jnp.where(
            lanes((16, LANES)) % 64 < 32, rolled(corner, -16), rolled(corner, 16)
        )
    for q in range(2):
        for half in range(2):
            cur_a[3 * q + half, FIRST : FIRST + 256, :] = level[q, :, LANES * half : LANES * (half + 1)]
            cur_b[3 * q + half, FIRST : FIRST + 256, :] = fuel_class[
                q, :, LANES * half : LANES * (half + 1)
            ].astype(f32)

    def rates(group, carry):
        for k in range(RATE_UNROLL):
            at = pl.multiple_of((1 + group * RATE_UNROLL + k) * 8, 8)
            for t in range(5):
                kind = cur_b[t, pl.ds(at, 8), :].astype(i32) & 127
                base_rate[t, pl.ds(at, 8), :] = pick(table_base, kind)
                wind_rate[t, pl.ds(at, 8), :] = pick(table_wind, kind)
        return carry

    lax.fori_loop(0, 36 // RATE_UNROLL, rates, 0)

    inner = lane % 64
    side_col = jnp.where(inner < 16, inner // 8, jnp.where(inner >= 48, 30 + (inner - 48) // 8, 0))
    for k in range(2):
        for t in range(5):
            for quarter in range(4):
                for outer in (0, 64):
                    if outer and quarter in (1, 2):
                        continue
                    at = outer + k * 32
                    if t == 2:
                        west = got(WINDB, 8 * quarter, 8)
                        east = got(WINDB + 1, 8 * quarter, 8)
                        index = side_col + at
                        value = jnp.where(lane < 64, pick(west, index), pick(east, index))
                    else:
                        source = got(WINDA + t // 3, 8 * quarter, 8)
                        value = pick(source, lane // 8 + (at + 16 * (t % 3)))
                    value = value * log2e
                    if not outer:
                        wind[k, t, 3 + 8 * quarter : 11 + 8 * quarter, :] = value
                    elif quarter == 3:
                        wind[k, t, 1:3, :] = value[6:8, :]
                    else:
                        wind[k, t, 35:37, :] = value[0:2, :]

    def there(j):
        return j >= 0

    across_links = []
    groups = []
    for q in range(2):
        i = own + q
        near = [adjacency[s, i] for s in range(4)]
        safe = [jnp.maximum(near[s], 0) for s in range(4)]

        def joined(s, t):
            return there(near[s]) & there(adjacency[t, safe[s]])

        groups.append([(there(near[s]), joined(2, s), joined(3, s)) for s in range(2)])
        across_links.append([[joined(0, t), there(near[t]), joined(1, t)] for t in (2, 3)])

    def as_int(flag):
        return jnp.where(flag, 1, 0)

    for line in range(2):
        for q in range(2):
            mid, west, east = groups[q][line]
            row = jnp.broadcast_to(as_int(mid), (8, LANES))
            links[line, 3 * q] = row
            links[line, 3 * q + 1] = row
        w0, e0 = groups[0][line][1:]
        w1, e1 = groups[1][line][1:]
        links[line, 2] = jnp.where(
            lane < 32,
            as_int(e0),
            jnp.where(lane < 64, as_int(w0), jnp.where(lane < 96, as_int(e1), as_int(w1))),
        )

    is0 = lane == 0
    is63 = lane == 63
    is64 = lane == 64
    is127 = lane == 127
    tanh_sum[...] = jnp.zeros(tanh_sum.shape, f32)

    def make_masks(region):
        (w0, e0), (w1, e1) = [
            [as_int(across_links[q][t][region]) for t in range(2)] for q in range(2)
        ]
        on = [jnp.broadcast_to(flag, (8, LANES)) > 0 for flag in (w0, e0, w1, e1)]
        return on

    def update(source, target, chunk, masks, rows_edge, main):
        lw0, le0, lw1, le1 = masks
        at = chunk * 8
        x = [source[t, pl.ds(at, 8), :] for t in range(5)]
        up = [source[t, pl.ds(at - 1, 8), :] for t in range(5)]
        dn = [source[t, pl.ds(at + 1, 8), :] for t in range(5)]
        if rows_edge is not None:
            kind, line, row = rows_edge
            for t in range(5):
                broken = (sub == row) & (links[line, t] == 0)
                if kind == "up":
                    up[t] = jnp.where(broken, x[t], up[t])
                else:
                    dn[t] = jnp.where(broken, x[t], dn[t])
        right = [rolled(v, 1) for v in x]
        left = [rolled(v, -1) for v in x]
        h = x[2]
        west = [
            jnp.where(is0, jnp.where(lw0, rolled(h, 65), x[0]), right[0]),
            jnp.where(is0, right[0], right[1]),
            jnp.where(
                is0,
                jnp.where(le0, right[1], h),
                jnp.where(is64, jnp.where(le1, rolled(x[4], 65), h), right[2]),
            ),
            jnp.where(is0, jnp.where(lw1, right[2], x[3]), right[3]),
            jnp.where(is0, right[3], right[4]),
        ]
        east = [
            jnp.where(is127, left[1], left[0]),
            jnp.where(is127, jnp.where(le0, left[2], x[1]), left[1]),
            jnp.where(
                is127,
                jnp.where(lw1, left[3], h),
                jnp.where(is63, jnp.where(lw0, rolled(x[0], 63), h), left[2]),
            ),
            jnp.where(is127, left[4], left[3]),
            jnp.where(is127, jnp.where(le1, rolled(h, -65), x[4]), left[4]),
        ]
        for t in range(5):
            diff_rows = dn[t] - up[t]
            diff_cols = east[t] - west[t]
            around = (dn[t] + up[t]) + (east[t] + west[t])
            square = diff_rows * diff_rows + (diff_cols * diff_cols + 4.0 * floor_square)
            inverse = lax.rsqrt(square)
            wind_r = wind[0, t, pl.ds(chunk, 1), :]
            wind_c = wind[1, t, pl.ds(chunk, 1), :]
            along = (wind_r * diff_rows + wind_c * diff_cols) * inverse
            soft = jnp.log(1.0 + jnp.exp2(along))
            power = soft * soft * lax.rsqrt(soft)
            b = base_rate[t, pl.ds(at, 8), :]
            w = wind_rate[t, pl.ds(at, 8), :]
            new = ((1.0 - 4.0 * smoothing) * x[t] + smoothing * around) - (b + w * power) * (
                square * inverse
            )
            target[t, pl.ds(at, 8), :] = new
            if main and t != 2:
                m = t - t // 3
                tanh_sum[m, pl.ds(at - FIRST, 8), :] += jnp.tanh(new)

    above = make_masks(0)
    within = make_masks(1)
    below = make_masks(2)

    def substep(source, target):
        update(source, target, 1, above, None, False)
        update(source, target, 2, above, ("down", 0, 7), False)
        update(source, target, 3, within, ("up", 0, 0), True)

        def middle(group, carry):
            for k in range(UNROLL):
                update(source, target, 4 + group * UNROLL + k, within, None, True)
            return carry

        lax.fori_loop(0, 30 // UNROLL, middle, 0)
        update(source, target, 34, within, ("down", 1, 7), True)
        update(source, target, 35, below, ("up", 1, 0), False)
        update(source, target, 36, below, None, False)

    def two_substeps(pair, carry):
        substep(cur_a, cur_b)
        substep(cur_b, cur_a)
        return carry

    lax.fori_loop(0, SUB // 2, two_substeps, 0)

    last = SUB % 2

    def finish(chunk, burn, emit):
        at = pl.multiple_of(chunk * 8, 8)
        for q in range(2):
            for half in range(2):
                t = 3 * q + half
                cols = slice(LANES * half, LANES * (half + 1))
                final = cur[last][t, pl.ds(FIRST + at, 8), :]
                level_out[q, pl.ds(at, 8), cols] = final
                burn = burn + (0.5 - 0.5 * jnp.tanh(final))
                kind = fuel_class[q, pl.ds(at, 8), cols]
                fuel = fuel_left[q, pl.ds(at, 8), cols]
                power = pick(table_burn, kind) * (float(SUB) - tanh_sum[2 * q + half, pl.ds(at, 8), :])
                new_fuel = fuel * jnp.exp2(power)
                fuel_out[q, pl.ds(at, 8), cols] = new_fuel
                spent = fuel - new_fuel
                emit = emit + pick(table_emit, kind) * spent
                released = pick(table_heat, kind) * spent
                row_heat[2 * q + half, pl.ds(chunk, 1), :] = jnp.sum(released, axis=0, keepdims=True)
        return burn, emit

    blank = jnp.zeros((8, LANES), f32)
    sums = [blank] * 4

    def finish_group(group, totals):
        totals = list(totals)
        for k in range(FINISH_UNROLL):
            pair = 2 * (k % 2)
            totals[pair], totals[pair + 1] = finish(
                group * FINISH_UNROLL + k, totals[pair], totals[pair + 1]
            )
        return tuple(totals)

    sums = lax.fori_loop(0, 32 // FINISH_UNROLL, finish_group, tuple(sums))
    burn = sums[0] + sums[2]
    emit = sums[1] + sums[3]
    devices = across * down

    def spread(row, value):
        heat_out[pl.ds(row, devices, stride=HEAT_ROWS), :] = jnp.broadcast_to(value, (devices, LANES))

    source_lane = lax.broadcasted_iota(i32, (LANES, LANES), 0) // REF
    target_lane = lanes((LANES, LANES))
    for q in range(2):
        packed = blank
        for g in range(4):
            for half in range(2):
                gather = jnp.where(
                    target_lane == 32 * g + 16 * half + source_lane, heating / (REF * REF), 0.0
                ).astype(f32)
                packed = packed + jnp.dot(
                    row_heat[2 * q + half, 8 * g : 8 * g + 8, :],
                    gather,
                    precision=lax.Precision.HIGHEST,
                    preferred_element_type=f32,
                )
        for row in range(8):
            spread(8 * q + row, packed[row : row + 1, :])
    burn_sum = jnp.sum(jnp.sum(burn, axis=0, keepdims=True), axis=1, keepdims=True)
    emit_sum = jnp.sum(jnp.sum(emit, axis=0, keepdims=True), axis=1, keepdims=True)
    lane1 = lanes((1, LANES))
    spread(16, jnp.where(lane1 == 0, burn_sum, jnp.where(lane1 == 1, emit_sum, 0.0)))


def air_kernel(across, down, pos, received, air_hbm, air_out, air, fresh, sides, sem_in, sem_out):
    def load(number):
        return pltpu.make_async_copy(
            air_hbm.at[:, number], air.at[:, number + 1, 8:136, :], sem_in.at[number]
        )

    def store(number):
        return pltpu.make_async_copy(fresh.at[:, number], air_out.at[:, number], sem_out.at[number])

    levels = 16
    for number in range(levels):
        load(number).start()
    lane = lanes()
    is0 = lane == 0
    is127 = lane == 127
    zero = jnp.zeros((128, LANES), f32)
    for f in range(3):
        air[f, 0, 8:136, :] = zero
        air[f, levels + 1, 8:136, :] = zero
    keep_north = jnp.where(pos[0] > 0, 1.0, 0.0).astype(f32)
    keep_south = jnp.where(pos[0] < down - 1, 1.0, 0.0).astype(f32)
    keep_west = jnp.where(pos[1] > 0, 1.0, 0.0).astype(f32)
    keep_east = jnp.where(pos[1] < across - 1, 1.0, 0.0).astype(f32)

    def got(row):
        return received[pl.ds(row, PIECES, stride=REC2), :]

    for group in range(3):
        rows = got(ROWS2 + group)
        for p in range(32):
            number = 32 * group + p
            plane = number % 48
            at = 7 if number < 48 else 136
            keep = keep_north if number < 48 else keep_south
            air[plane // 16, plane % 16 + 1, at : at + 1, :] = rows[p : p + 1, :] * keep
    lane32 = lanes((32, LANES))
    for group in range(4):
        sides[32 * group : 32 * group + 32, :] = got(COLS2 + group) * jnp.where(
            lane32 % 2 == 1, keep_east, keep_west
        )

    load(0).wait()

    def air_level(number, carry):
        @pl.when(number < levels - 1)
        def _():
            load(number + 1).wait()

        def air_rows(group, inner_carry):
            for k in range(AIR_UNROLL):
                row = group * (8 * AIR_UNROLL) + k * 8
                at = 8 + row
                halo = sides[pl.ds(row, 8), :]
                x = [air[f, number + 1, pl.ds(at, 8), :] for f in range(3)]
                for f in range(3):
                    up = air[f, number + 1, pl.ds(at - 1, 8), :]
                    dn = air[f, number + 1, pl.ds(at + 1, 8), :]
                    over = air[f, number + 2, pl.ds(at, 8), :]
                    under = air[f, number, pl.ds(at, 8), :]
                    mine = pltpu.roll(halo, LANES - 1 - 2 * (f * 16 + number), 1)
                    west = rolled(jnp.where(is127, mine, x[f]), 1)
                    east = rolled(jnp.where(is0, mine, x[f]), -1)
                    around = (up + dn) + (west + east)
                    advect = x[0] * (dn - up) + x[1] * (east - west)
                    fresh[f, number, pl.ds(row, 8), :] = (
                        (1.0 - 4.0 * viscosity - 2.0 * mixing) * x[f]
                        + viscosity * around
                        - (0.5 * courant) * advect
                        + mixing * (over + under)
                    )
            return inner_carry

        lax.fori_loop(0, 16 // AIR_UNROLL, air_rows, 0)
        store(number).start()
        return carry

    lax.fori_loop(0, levels, air_level, 0)

    def drain(number, carry):
        store(number).wait()
        return carry

    lax.fori_loop(0, levels, drain, 0)


def heat_kernel(cells, pos, blocks, gathered, air_in, air_out, totals, plane, sem):
    load = pltpu.make_async_copy(air_in.at[2, 0], plane, sem)
    load.start()
    devices = gathered.shape[0] // HEAT_ROWS
    sums = jnp.sum(
        gathered[pl.ds(16, devices, stride=HEAT_ROWS), :], axis=0, keepdims=True
    )
    lane1 = lanes((1, LANES))
    for k in range(2):
        totals[k] = jnp.sum(jnp.where(lane1 == k, sums, 0.0)) * (1.0 / cells)
    load.wait()
    lane = lanes()
    tile_rows = 128 // BA

    def place(j, carry):
        row = blocks[0, j] - pos[0] * tile_rows
        col = blocks[1, j] - pos[1] * tile_rows
        inside = (row >= 0) & (row < tile_rows) & (col >= 0) & (col < tile_rows)

        @pl.when(inside)
        def _():
            heat = gathered[pl.ds((j // 2) * HEAT_ROWS + 8 * (j % 2), 8), :]
            for g in range(4):
                moved = pltpu.roll(heat, (col - g + 4) * BA % LANES, 1)
                at = pl.multiple_of(row * BA + 8 * g, 8)
                plane[pl.ds(at, 8), :] += jnp.where(lane // BA == col, moved, 0.0)

        return carry

    lax.fori_loop(0, blocks.shape[1], place, 0)
    store = pltpu.make_async_copy(plane, air_out.at[2, 0], sem)
    store.start()
    store.wait()


def local(air_state, level_set, fuel_left, fuel_class, fuel_props, blocks, adjacency):
    down = lax.axis_size("gx")
    across = lax.axis_size("gy")
    devices = down * across
    both = ("gx", "gy")
    pos = jnp.stack([lax.axis_index("gx"), lax.axis_index("gy")]).astype(i32)
    smem = pl.BlockSpec(memory_space=pltpu.SMEM)
    vmem = pl.BlockSpec(memory_space=pltpu.VMEM)
    anywhere = pl.BlockSpec(memory_space=pl.ANY)
    blocks = blocks.T
    adjacency = adjacency.T
    packed = pl.pallas_call(
        pack_kernel,
        out_shape=jax.ShapeDtypeStruct((devices * REC1, LANES), f32),
        in_specs=[smem, smem, vmem, vmem, anywhere],
        out_specs=vmem,
        scratch_shapes=[
            pltpu.VMEM((48 * 128, LANES), f32),
            pltpu.VMEM((4, 40, LANES), f32),
            pltpu.VMEM((128, LANES), f32),
            pltpu.SemaphoreType.DMA(()),
        ],
        name="pack",
    )(pos, blocks, level_set, fuel_class, air_state.reshape(48 * 128, LANES))
    relayed = lax.all_to_all(packed.reshape(devices, REC1, LANES), both, 0, 0)
    index = pl.pallas_call(
        lambda *refs: index_kernel(across, down, *refs),
        out_shape=jax.ShapeDtypeStruct((devices * WORDS,), i32),
        in_specs=[smem, smem, smem],
        out_specs=smem,
        scratch_shapes=[pltpu.SMEM((blocks.shape[1],), i32), pltpu.SMEM((devices,), i32)],
        cost_estimate=pl.CostEstimate(flops=40_000_000, transcendentals=0, bytes_accessed=10_000),
        name="index",
    )(pos, blocks, adjacency)
    chosen = pl.pallas_call(
        select_kernel,
        out_shape=jax.ShapeDtypeStruct((devices * REC2, LANES), f32),
        in_specs=[smem, vmem],
        out_specs=vmem,
        name="select",
    )(index, relayed.reshape(devices * REC1, LANES))
    received = lax.all_to_all(chosen.reshape(devices, REC2, LANES), both, 0, 0)
    received = received.reshape(devices * REC2, LANES)[: PIECES * REC2]
    level_next, fuel_next, heat = pl.pallas_call(
        lambda *refs: fire_kernel(across, down, *refs),
        out_shape=(
            jax.ShapeDtypeStruct(level_set.shape, f32),
            jax.ShapeDtypeStruct(level_set.shape, f32),
            jax.ShapeDtypeStruct((devices * HEAT_ROWS, LANES), f32),
        ),
        in_specs=[smem, smem, smem, vmem, vmem, vmem, vmem],
        out_specs=(vmem, vmem, vmem),
        scratch_shapes=[
            pltpu.VMEM((5, EXT, LANES), f32),
            pltpu.VMEM((5, EXT, LANES), f32),
            pltpu.VMEM((5, EXT, LANES), f32),
            pltpu.VMEM((5, EXT, LANES), f32),
            pltpu.VMEM((2, 5, 40, LANES), f32),
            pltpu.VMEM((40, LANES), f32),
            pltpu.VMEM((2, LANES, 256), f32),
            pltpu.VMEM((4, 256, LANES), f32),
            pltpu.VMEM((2, 5, 8, LANES), i32),
            pltpu.VMEM((4, 32, LANES), f32),
        ],
        name="fire",
    )(pos, adjacency, fuel_props, received, level_set, fuel_left, fuel_class)
    gathered = lax.all_to_all(heat.reshape(devices, 1, HEAT_ROWS * LANES), both, 0, 0)
    gathered = gathered.reshape(devices * HEAT_ROWS, LANES)
    air_next = pl.pallas_call(
        lambda *refs: air_kernel(across, down, *refs),
        out_shape=jax.ShapeDtypeStruct(air_state.shape, f32),
        in_specs=[smem, vmem, anywhere],
        out_specs=anywhere,
        scratch_shapes=[
            pltpu.VMEM((3, 18, 144, LANES), f32),
            pltpu.VMEM((3, 16, 128, LANES), f32),
            pltpu.VMEM((128, LANES), f32),
            pltpu.SemaphoreType.DMA((16,)),
            pltpu.SemaphoreType.DMA((16,)),
        ],
        cost_estimate=pl.CostEstimate(flops=80_000_000, transcendentals=0, bytes_accessed=6_300_000),
        name="air",
    )(pos, received, air_state)
    cells = blocks.shape[1] * level_set.shape[1] * level_set.shape[2]
    air_next, totals = pl.pallas_call(
        lambda *refs: heat_kernel(cells, *refs),
        out_shape=(jax.ShapeDtypeStruct(air_state.shape, f32), jax.ShapeDtypeStruct((2,), f32)),
        in_specs=[smem, smem, vmem, anywhere],
        out_specs=(anywhere, smem),
        scratch_shapes=[pltpu.VMEM((128, LANES), f32), pltpu.SemaphoreType.DMA(())],
        input_output_aliases={3: 0},
        name="heat",
    )(pos, blocks, gathered, air_next)
    return (air_next, level_next, fuel_next, totals)


def solution(mesh):
    in_specs = (
        P(None, None, "gx", "gy"),
        P(("gx", "gy"), None, None),
        P(("gx", "gy"), None, None),
        P(("gx", "gy"), None, None),
        P(),
        P(),
        P(),
    )
    out_specs = (
        P(None, None, "gx", "gy"),
        P(("gx", "gy"), None, None),
        P(("gx", "gy"), None, None),
        P(),
    )
    return jax.shard_map(local, mesh=mesh, in_specs=in_specs, out_specs=out_specs, check_vma=False)
```

```python
import math

import jax
import jax.numpy as jnp
from jax import lax
from jax.experimental import pallas as pl
from jax.experimental.pallas import tpu as pltpu
from jax.sharding import PartitionSpec as P


REF = 8
BA = 32
SUB = 10
PIECES = 32
LANES = 128
UNROLL = 30
RATE_UNROLL = 12
FINISH_UNROLL = 16
AIR_UNROLL = 16
EDGE_UNROLL = 2

step_time = 0.25
smoothing = 0.15
floor_square = 0.25
viscosity = 0.1
courant = 0.25
mixing = 0.1
heating = 2.0

SIDE = 0
CORNER = 10
WIND = 12
REC1 = 16
CORNER2 = 10
WINDA = 11
WINDB = 13
REC2 = 16
HEAT_ROWS = 17

TOP = 8
EXT = 304
FIRST = 24

f32 = jnp.float32
i32 = jnp.int32


def lanes(shape=(8, LANES)):
    return lax.broadcasted_iota(i32, shape, len(shape) - 1)


def rolled(x, shift):
    return pltpu.roll(x, shift % LANES, x.ndim - 1)


def opposite(side):
    return (1, 0, 3, 2)[side]


def pick(table, index):
    return jnp.take_along_axis(table, index, axis=1, mode="promise_in_bounds")


def pack_kernel(pos, blocks, level, fuel_class, air_hbm, out, air, strip, sem):
    load = pltpu.make_async_copy(air_hbm.at[0:2, 0], air, sem)
    load.start()
    lane256 = lanes((256, LANES))
    lane16 = lanes((16, LANES))

    def place(row, first, values):
        out[pl.ds(first * REC1 + row, values.shape[0], stride=REC1), :] = values

    for q in range(2):
        fields = (level[q], fuel_class[q].astype(f32))
        turned = [
            jnp.where(lane256 < 64, field[:, :LANES], field[:, LANES:]).T for field in fields
        ]
        for side in range(4):
            for number, (field, turn) in enumerate(zip(fields, turned)):
                if side == 0:
                    rows = field[0:SUB, :]
                elif side == 1:
                    rows = field[256 - SUB : 256, :]
                elif side == 2:
                    rows = turn[0:SUB, :]
                else:
                    rows = turn[LANES - SUB : LANES, :]
                strip[side, 2 * SUB * number : 2 * SUB * number + SUB, :] = rows[:, :LANES]
                strip[side, 2 * SUB * number + SUB : 2 * SUB * (number + 1), :] = rows[:, LANES:]
            place(SIDE + q * 5 + side, 0, strip[side, 0:32, :])
            place(SIDE + q * 5 + 4, 8 * side, strip[side, 32:40, :])
        for number, field in enumerate(fields):
            half = jnp.where(
                lane16 < 16,
                field[240:256, :LANES],
                jnp.where(
                    lane16 < 32,
                    rolled(field[0:16, :LANES], 16),
                    jnp.where(
                        lane16 < 48,
                        rolled(field[0:16, LANES:], 48),
                        rolled(field[240:256, LANES:], 64),
                    ),
                ),
            )
            place(CORNER + q, 16 * number, jnp.where(lane16 < 64, half, rolled(half, 64)))

    load.wait()
    blank = jnp.zeros((PIECES, LANES), f32)
    for slot in range(4):
        place(WIND + slot, 0, blank)
    lane32 = lanes((32, LANES))
    tile_rows = 128 // BA

    def find(j, count):
        row = blocks[0, j] - pos[0] * tile_rows
        col = blocks[1, j] - pos[1] * tile_rows
        inside = (row >= 0) & (row < tile_rows) & (col >= 0) & (col < tile_rows)

        @pl.when(inside)
        def _():
            start = pl.multiple_of(row * BA, BA)
            u = air[0, pl.ds(start, BA), :]
            v = air[1, pl.ds(start, BA), :]
            shift = LANES - col * BA
            u = pltpu.roll(u, shift, 1)
            v = pltpu.roll(v, shift, 1)
            half = jnp.where(lane32 < 32, u, rolled(v, 32))
            both = jnp.where(lane32 < 64, half, rolled(half, 64))
            out[pl.ds(WIND + count, PIECES, stride=REC1), :] = both

        return count + inside.astype(i32)

    lax.fori_loop(0, blocks.shape[1], find, jnp.int32(0))

    if out.shape[0] > PIECES * REC1:
        out[PIECES * REC1 :, :] = jnp.zeros((out.shape[0] - PIECES * REC1, LANES), f32)


WORDS = 15


def edge_kernel(air_hbm, ready, first_rows, last_rows, columns, air, sem):
    load = pltpu.make_async_copy(air_hbm, air, sem)
    load.start()
    load.wait()
    first_rows[...] = air[pl.ds(0, 48, stride=128), :]
    last_rows[...] = air[pl.ds(127, 48, stride=128), :]
    lane = lanes()

    def gather(group, carry):
        for k in range(EDGE_UNROLL):
            base = pl.multiple_of((group * EDGE_UNROLL + k) * 8, 8)
            total = jnp.zeros((8, LANES), f32)
            for plane in range(48):
                x = air[pl.ds(plane * 128 + base, 8), :]
                total = jnp.where(lane // 2 == plane, rolled(x, 1 + 2 * plane), total)
            columns[pl.ds(base, 8), :] = total
        return carry

    lax.fori_loop(0, 16 // EDGE_UNROLL, gather, 0)


def index_kernel(across, pos, blocks, adjacency, out, padded):
    total = blocks.shape[1]
    tiles = out.shape[1] // LANES
    relay = jnp.minimum(pos[0] * across + pos[1], PIECES - 1)
    padded[...] = jnp.zeros(padded.shape, i32)
    padded[0:2, 0:total] = blocks[...]
    padded[8:12, 0:total] = adjacency[...]

    def row(number):
        return [
            jnp.broadcast_to(padded[number : number + 1, LANES * u : LANES * (u + 1)], (8, LANES))
            for u in range(tiles)
        ]

    def lookup(table, index):
        found = []
        for u in range(tiles):
            value = pick(table[0], index[u] & (LANES - 1))
            for v in range(1, tiles):
                value = jnp.where(index[u] >> 7 == v, pick(table[v], index[u] & (LANES - 1)), value)
            found.append(value)
        return found

    def each(f, *rows):
        return [f(*values) for values in zip(*rows)]

    lane = lanes()
    tile_of = each(lambda r, c: (r >> 2) * across + (c >> 2), row(0), row(1))
    before = lax.broadcasted_iota(i32, (LANES, LANES), 0)
    here = lanes((LANES, LANES))
    as_rows = [jnp.broadcast_to(t[0:1, :].astype(f32), (LANES, LANES)) for t in tile_of]
    as_cols = [t.T for t in as_rows]
    wind_row = []
    for u in range(tiles):
        slot = jnp.zeros((1, LANES), f32)
        for v in range(u + 1):
            same = (as_cols[v] == as_rows[u]) & (before + LANES * v < here + LANES * u)
            slot = slot + jnp.sum(jnp.where(same, 1.0, 0.0), axis=0, keepdims=True)
        wind_row.append(tile_of[u] * REC1 + WIND + jnp.broadcast_to(slot.astype(i32), (8, LANES)))
    near = [row(8 + s) for s in range(4)]
    safe = [each(lambda n: jnp.maximum(n, 0), near[s]) for s in range(4)]

    def diagonal(s, t):
        by_row = lookup(near[t], safe[s])
        by_col = lookup(near[s], safe[t])
        return each(
            lambda n, m, r, c: jnp.maximum(jnp.where(n >= 0, r, jnp.where(m >= 0, c, 0)), 0),
            near[s],
            near[t],
            by_row,
            by_col,
        )

    nw, ne, sw, se = diagonal(0, 2), diagonal(0, 3), diagonal(1, 2), diagonal(1, 3)
    spare_side = relay >> 3
    upper = relay >= 16

    def side_row(j, s):
        return each(lambda b: (b >> 1) * REC1 + SIDE + (b & 1) * 5 + s, j)

    def choose(flag, yes, no):
        return each(lambda a, b: jnp.where(flag, a, b), yes, no)

    words = [side_row(safe[s], opposite(s)) for s in range(4)]
    spare = choose(
        spare_side == 0,
        safe[1],
        choose(spare_side == 1, safe[0], choose(spare_side == 2, safe[3], safe[2])),
    )
    words.append(side_row(spare, 4))
    for j in (ne, se, sw, nw):
        words.append(each(lambda b: (b >> 1) * REC1 + CORNER + (b & 1), j))
    words.append(wind_row)
    for j in (
        choose(upper, safe[0], safe[1]),
        safe[3],
        safe[2],
        choose(upper, ne, se),
        choose(upper, nw, sw),
    ):
        words.append(lookup(wind_row, j))
    for number, word in enumerate(words):
        for u in range(tiles):
            out[number : number + 1, LANES * u : LANES * (u + 1)] = word[u][0:1, :]
    out[WORDS : WORDS + 1, :] = jnp.zeros((1, out.shape[1]), i32)


def select_kernel(index, received, north, south, out):
    lane1 = lanes((1, LANES))
    lane_col = lane1 % 32 < 16
    first_half = lane1 < 64
    quarter = lane1 // 16

    def one(d):
        def take(word, q):
            return received[pl.ds(index[word, 2 * d + q], 1), :]

        def put(row, value):
            out[pl.ds(d * REC2 + row, 1), :] = value

        for row in range(10):
            put(SIDE + row, take(row % 5, row // 5))
        merged = take(8, 1)
        for k in range(7):
            merged = jnp.where(quarter == k, take(5 + k % 4, k // 4), merged)
        put(CORNER2, merged)
        for q in range(2):
            own, beyond, east, west, corner_east, corner_west = [take(9 + k, q) for k in range(6)]
            put(WINDA + q, jnp.where(first_half, own, beyond))
            put(
                WINDB + q,
                jnp.where(
                    lane_col,
                    jnp.where(first_half, east, corner_east),
                    jnp.where(first_half, west, corner_west),
                ),
            )
        put(REC2 - 1, jnp.zeros((1, LANES), f32))

    def serve(pair, carry):
        one(2 * pair)
        one(2 * pair + 1)
        return carry

    lax.fori_loop(0, out.shape[0] // REC2 // 2, serve, 0)


def fire_kernel(
    across,
    down,
    pos,
    adjacency,
    props,
    received,
    level,
    fuel_left,
    fuel_class,
    west_side,
    east_side,
    level_out,
    fuel_out,
    heat_out,
    cur_a,
    cur_b,
    base_rate,
    wind_rate,
    wind,
    strips,
    turned,
    tanh_sum,
    links,
    row_heat,
):
    cur = (cur_a, cur_b)
    lane = lanes()
    sub = lax.broadcasted_iota(i32, (8, LANES), 0)
    lane32 = lanes((32, LANES))
    own = 2 * (pos[0] * across + pos[1])

    def got(row, first=0, size=PIECES):
        return received[pl.ds(first * REC2 + row, size, stride=REC2), :]

    def table(value):
        row = jnp.zeros((8, LANES), f32)
        for kind in range(props.shape[1]):
            row = jnp.where(lane == kind, value(kind), row)
        return row

    log2e = math.log2(math.e)
    table_base = table(lambda c: 0.125 * 0.3 * props[0, c])
    table_wind = table_base * table(lambda c: 0.3 * props[1, c])
    table_burn = (-0.5 * step_time * log2e / 4.0) / jnp.where(
        lane < props.shape[1], table(lambda c: props[2, c]), 1.0
    )
    table_heat = table(lambda c: props[3, c])
    table_emit = table(lambda c: 3.0 * props[4, c])

    turned[...] = jnp.zeros(turned.shape, f32)
    for q in range(2):
        for s in range(4):
            strips[0:32, :] = got(SIDE + q * 5 + s)
            strips[32:40, :] = got(SIDE + q * 5 + 4, 8 * opposite(s), 8)
            for number in range(2):
                low = strips[2 * SUB * number : 2 * SUB * number + SUB, :]
                high = strips[2 * SUB * number + SUB : 2 * SUB * (number + 1), :]
                if s < 2:
                    at = FIRST - SUB if s == 0 else FIRST + 256
                    target = cur[number]
                    target[3 * q, at : at + SUB, :] = low
                    target[3 * q + 1, at : at + SUB, :] = high
                else:
                    at = (54, 118)[q] if s == 2 else (0, 64)[q]
                    turned[number, at : at + SUB, :LANES] = low
                    turned[number, at : at + SUB, LANES:] = high
    for number in range(2):
        cur[number][2, FIRST : FIRST + 256, :] = turned[number].T
        corner = got(CORNER2, 16 * number, 16)
        cur[number][2, TOP : TOP + 16, :] = corner
        cur[number][2, FIRST + 256 : FIRST + 272, :] = jnp.where(
            lanes((16, LANES)) % 64 < 32, rolled(corner, -16), rolled(corner, 16)
        )
    for q in range(2):
        for half in range(2):
            cur_a[3 * q + half, FIRST : FIRST + 256, :] = level[q, :, LANES * half : LANES * (half + 1)]
            cur_b[3 * q + half, FIRST : FIRST + 256, :] = fuel_class[
                q, :, LANES * half : LANES * (half + 1)
            ].astype(f32)

    def rates(group, carry):
        for k in range(RATE_UNROLL):
            at = pl.multiple_of((1 + group * RATE_UNROLL + k) * 8, 8)
            for t in range(5):
                kind = cur_b[t, pl.ds(at, 8), :].astype(i32) & 127
                base_rate[t, pl.ds(at, 8), :] = pick(table_base, kind)
                wind_rate[t, pl.ds(at, 8), :] = pick(table_wind, kind)
        return carry

    lax.fori_loop(0, 36 // RATE_UNROLL, rates, 0)

    inner = lane % 64
    side_col = jnp.where(inner < 16, inner // 8, jnp.where(inner >= 48, 30 + (inner - 48) // 8, 0))
    for k in range(2):
        for t in range(5):
            for quarter in range(4):
                for outer in (0, 64):
                    if outer and quarter in (1, 2):
                        continue
                    at = outer + k * 32
                    if t == 2:
                        west = got(WINDB, 8 * quarter, 8)
                        east = got(WINDB + 1, 8 * quarter, 8)
                        index = side_col + at
                        value = jnp.where(lane < 64, pick(west, index), pick(east, index))
                    else:
                        source = got(WINDA + t // 3, 8 * quarter, 8)
                        value = pick(source, lane // 8 + (at + 16 * (t % 3)))
                    value = value * log2e
                    if not outer:
                        wind[k, t, 3 + 8 * quarter : 11 + 8 * quarter, :] = value
                    elif quarter == 3:
                        wind[k, t, 1:3, :] = value[6:8, :]
                    else:
                        wind[k, t, 35:37, :] = value[0:2, :]

    def there(j):
        return j >= 0

    across_links = []
    groups = []
    for q in range(2):
        i = own + q
        near = [adjacency[s, i] for s in range(4)]
        safe = [jnp.maximum(near[s], 0) for s in range(4)]

        def joined(s, t):
            return there(near[s]) & there(adjacency[t, safe[s]])

        groups.append([(there(near[s]), joined(2, s), joined(3, s)) for s in range(2)])
        across_links.append([[joined(0, t), there(near[t]), joined(1, t)] for t in (2, 3)])

    def as_int(flag):
        return jnp.where(flag, 1, 0)

    for line in range(2):
        for q in range(2):
            mid, west, east = groups[q][line]
            row = jnp.broadcast_to(as_int(mid), (8, LANES))
            links[line, 3 * q] = row
            links[line, 3 * q + 1] = row
        w0, e0 = groups[0][line][1:]
        w1, e1 = groups[1][line][1:]
        links[line, 2] = jnp.where(
            lane < 32,
            as_int(e0),
            jnp.where(lane < 64, as_int(w0), jnp.where(lane < 96, as_int(e1), as_int(w1))),
        )

    is0 = lane == 0
    is63 = lane == 63
    is64 = lane == 64
    is127 = lane == 127
    tanh_sum[...] = jnp.zeros(tanh_sum.shape, f32)

    def make_masks(region):
        (w0, e0), (w1, e1) = [
            [as_int(across_links[q][t][region]) for t in range(2)] for q in range(2)
        ]
        on = [jnp.broadcast_to(flag, (8, LANES)) > 0 for flag in (w0, e0, w1, e1)]
        return on

    def update(source, target, chunk, masks, rows_edge, main):
        lw0, le0, lw1, le1 = masks
        at = chunk * 8
        x = [source[t, pl.ds(at, 8), :] for t in range(5)]
        up = [source[t, pl.ds(at - 1, 8), :] for t in range(5)]
        dn = [source[t, pl.ds(at + 1, 8), :] for t in range(5)]
        if rows_edge is not None:
            kind, line, row = rows_edge
            for t in range(5):
                broken = (sub == row) & (links[line, t] == 0)
                if kind == "up":
                    up[t] = jnp.where(broken, x[t], up[t])
                else:
                    dn[t] = jnp.where(broken, x[t], dn[t])
        right = [rolled(v, 1) for v in x]
        left = [rolled(v, -1) for v in x]
        h = x[2]
        west = [
            jnp.where(is0, jnp.where(lw0, rolled(h, 65), x[0]), right[0]),
            jnp.where(is0, right[0], right[1]),
            jnp.where(
                is0,
                jnp.where(le0, right[1], h),
                jnp.where(is64, jnp.where(le1, rolled(x[4], 65), h), right[2]),
            ),
            jnp.where(is0, jnp.where(lw1, right[2], x[3]), right[3]),
            jnp.where(is0, right[3], right[4]),
        ]
        east = [
            jnp.where(is127, left[1], left[0]),
            jnp.where(is127, jnp.where(le0, left[2], x[1]), left[1]),
            jnp.where(
                is127,
                jnp.where(lw1, left[3], h),
                jnp.where(is63, jnp.where(lw0, rolled(x[0], 63), h), left[2]),
            ),
            jnp.where(is127, left[4], left[3]),
            jnp.where(is127, jnp.where(le1, rolled(h, -65), x[4]), left[4]),
        ]
        for t in range(5):
            diff_rows = dn[t] - up[t]
            diff_cols = east[t] - west[t]
            around = (dn[t] + up[t]) + (east[t] + west[t])
            square = diff_rows * diff_rows + (diff_cols * diff_cols + 4.0 * floor_square)
            inverse = lax.rsqrt(square)
            wind_r = wind[0, t, pl.ds(chunk, 1), :]
            wind_c = wind[1, t, pl.ds(chunk, 1), :]
            along = (wind_r * diff_rows + wind_c * diff_cols) * inverse
            soft = jnp.log(1.0 + jnp.exp2(along))
            power = soft * soft * lax.rsqrt(soft)
            b = base_rate[t, pl.ds(at, 8), :]
            w = wind_rate[t, pl.ds(at, 8), :]
            new = ((1.0 - 4.0 * smoothing) * x[t] + smoothing * around) - (b + w * power) * (
                square * inverse
            )
            target[t, pl.ds(at, 8), :] = new
            if main and t != 2:
                m = t - t // 3
                tanh_sum[m, pl.ds(at - FIRST, 8), :] += jnp.tanh(new)

    above = make_masks(0)
    within = make_masks(1)
    below = make_masks(2)

    def substep(source, target):
        update(source, target, 1, above, None, False)
        update(source, target, 2, above, ("down", 0, 7), False)
        update(source, target, 3, within, ("up", 0, 0), True)

        def middle(group, carry):
            for k in range(UNROLL):
                update(source, target, 4 + group * UNROLL + k, within, None, True)
            return carry

        lax.fori_loop(0, 30 // UNROLL, middle, 0)
        update(source, target, 34, within, ("down", 1, 7), True)
        update(source, target, 35, below, ("up", 1, 0), False)
        update(source, target, 36, below, None, False)

    def two_substeps(pair, carry):
        substep(cur_a, cur_b)
        substep(cur_b, cur_a)
        return carry

    lax.fori_loop(0, SUB // 2, two_substeps, 0)

    last = SUB % 2

    def finish(chunk, burn, emit):
        at = pl.multiple_of(chunk * 8, 8)
        for q in range(2):
            for half in range(2):
                t = 3 * q + half
                cols = slice(LANES * half, LANES * (half + 1))
                final = cur[last][t, pl.ds(FIRST + at, 8), :]
                level_out[q, pl.ds(at, 8), cols] = final
                burn = burn + (0.5 - 0.5 * jnp.tanh(final))
                kind = fuel_class[q, pl.ds(at, 8), cols]
                fuel = fuel_left[q, pl.ds(at, 8), cols]
                power = pick(table_burn, kind) * (float(SUB) - tanh_sum[2 * q + half, pl.ds(at, 8), :])
                new_fuel = fuel * jnp.exp2(power)
                fuel_out[q, pl.ds(at, 8), cols] = new_fuel
                spent = fuel - new_fuel
                emit = emit + pick(table_emit, kind) * spent
                released = pick(table_heat, kind) * spent
                row_heat[2 * q + half, pl.ds(chunk, 1), :] = jnp.sum(released, axis=0, keepdims=True)
        return burn, emit

    blank = jnp.zeros((8, LANES), f32)
    sums = [blank] * 4

    def finish_group(group, totals):
        totals = list(totals)
        for k in range(FINISH_UNROLL):
            pair = 2 * (k % 2)
            totals[pair], totals[pair + 1] = finish(
                group * FINISH_UNROLL + k, totals[pair], totals[pair + 1]
            )
        return tuple(totals)

    sums = lax.fori_loop(0, 32 // FINISH_UNROLL, finish_group, tuple(sums))
    burn = sums[0] + sums[2]
    emit = sums[1] + sums[3]
    devices = across * down

    def spread(row, value):
        heat_out[pl.ds(row, devices, stride=HEAT_ROWS), :] = jnp.broadcast_to(value, (devices, LANES))

    source_lane = lax.broadcasted_iota(i32, (LANES, LANES), 0) // REF
    target_lane = lanes((LANES, LANES))
    for q in range(2):
        packed = blank
        for g in range(4):
            for half in range(2):
                gather = jnp.where(
                    target_lane == 32 * g + 16 * half + source_lane, heating / (REF * REF), 0.0
                ).astype(f32)
                packed = packed + jnp.dot(
                    row_heat[2 * q + half, 8 * g : 8 * g + 8, :],
                    gather,
                    precision=lax.Precision.HIGHEST,
                    preferred_element_type=f32,
                )
        for row in range(8):
            spread(8 * q + row, packed[row : row + 1, :])
    burn_sum = jnp.sum(jnp.sum(burn, axis=0, keepdims=True), axis=1, keepdims=True)
    emit_sum = jnp.sum(jnp.sum(emit, axis=0, keepdims=True), axis=1, keepdims=True)
    lane1 = lanes((1, LANES))
    spread(16, jnp.where(lane1 == 0, burn_sum, jnp.where(lane1 == 1, emit_sum, 0.0)))


def air_kernel(north, south, west_side, east_side, air_hbm, air_out, air, fresh, sides, sem_in, sem_out):
    def load(number):
        return pltpu.make_async_copy(
            air_hbm.at[:, number], air.at[:, number + 1, 8:136, :], sem_in.at[number]
        )

    def store(number):
        return pltpu.make_async_copy(fresh.at[:, number], air_out.at[:, number], sem_out.at[number])

    levels = 16
    for number in range(levels):
        load(number).start()
    lane = lanes()
    is0 = lane == 0
    is127 = lane == 127
    zero = jnp.zeros((128, LANES), f32)
    for f in range(3):
        air[f, 0, 8:136, :] = zero
        air[f, levels + 1, 8:136, :] = zero
    for plane in range(48):
        at = (plane // 16, plane % 16 + 1)
        air[at[0], at[1], 7:8, :] = north[plane : plane + 1, :]
        air[at[0], at[1], 136:137, :] = south[plane : plane + 1, :]
    sides[...] = jnp.where(lanes((128, LANES)) % 2 == 1, east_side[...], west_side[...])

    load(0).wait()

    def air_level(number, carry):
        @pl.when(number < levels - 1)
        def _():
            load(number + 1).wait()

        def air_rows(group, inner_carry):
            for k in range(AIR_UNROLL):
                row = group * (8 * AIR_UNROLL) + k * 8
                at = 8 + row
                halo = sides[pl.ds(row, 8), :]
                x = [air[f, number + 1, pl.ds(at, 8), :] for f in range(3)]
                for f in range(3):
                    up = air[f, number + 1, pl.ds(at - 1, 8), :]
                    dn = air[f, number + 1, pl.ds(at + 1, 8), :]
                    over = air[f, number + 2, pl.ds(at, 8), :]
                    under = air[f, number, pl.ds(at, 8), :]
                    mine = pltpu.roll(halo, LANES - 1 - 2 * (f * 16 + number), 1)
                    west = rolled(jnp.where(is127, mine, x[f]), 1)
                    east = rolled(jnp.where(is0, mine, x[f]), -1)
                    around = (up + dn) + (west + east)
                    advect = x[0] * (dn - up) + x[1] * (east - west)
                    fresh[f, number, pl.ds(row, 8), :] = (
                        (1.0 - 4.0 * viscosity - 2.0 * mixing) * x[f]
                        + viscosity * around
                        - (0.5 * courant) * advect
                        + mixing * (over + under)
                    )
            return inner_carry

        lax.fori_loop(0, 16 // AIR_UNROLL, air_rows, 0)
        store(number).start()
        return carry

    lax.fori_loop(0, levels, air_level, 0)

    def drain(number, carry):
        store(number).wait()
        return carry

    lax.fori_loop(0, levels, drain, 0)


def heat_kernel(cells, pos, blocks, gathered, air_in, air_out, totals, plane, sem):
    load = pltpu.make_async_copy(air_in.at[2, 0], plane, sem)
    load.start()
    devices = gathered.shape[0] // HEAT_ROWS
    sums = jnp.sum(
        gathered[pl.ds(16, devices, stride=HEAT_ROWS), :], axis=0, keepdims=True
    )
    lane1 = lanes((1, LANES))
    for k in range(2):
        totals[k] = jnp.sum(jnp.where(lane1 == k, sums, 0.0)) * (1.0 / cells)
    load.wait()
    lane = lanes()
    tile_rows = 128 // BA

    def place(j, carry):
        row = blocks[0, j] - pos[0] * tile_rows
        col = blocks[1, j] - pos[1] * tile_rows
        inside = (row >= 0) & (row < tile_rows) & (col >= 0) & (col < tile_rows)

        @pl.when(inside)
        def _():
            heat = gathered[pl.ds((j // 2) * HEAT_ROWS + 8 * (j % 2), 8), :]
            for g in range(4):
                moved = pltpu.roll(heat, (col - g + 4) * BA % LANES, 1)
                at = pl.multiple_of(row * BA + 8 * g, 8)
                plane[pl.ds(at, 8), :] += jnp.where(lane // BA == col, moved, 0.0)

        return carry

    lax.fori_loop(0, blocks.shape[1], place, 0)
    store = pltpu.make_async_copy(plane, air_out.at[2, 0], sem)
    store.start()
    store.wait()


def local(air_state, level_set, fuel_left, fuel_class, fuel_props, blocks, adjacency):
    down = lax.axis_size("gx")
    across = lax.axis_size("gy")
    devices = down * across
    both = ("gx", "gy")
    pos = jnp.stack([lax.axis_index("gx"), lax.axis_index("gy")]).astype(i32)
    smem = pl.BlockSpec(memory_space=pltpu.SMEM)
    vmem = pl.BlockSpec(memory_space=pltpu.VMEM)
    anywhere = pl.BlockSpec(memory_space=pl.ANY)
    blocks = blocks.T
    adjacency = adjacency.T
    packed = pl.pallas_call(
        pack_kernel,
        out_shape=pltpu.VMEM((devices * REC1, LANES), f32),
        in_specs=[smem, smem, vmem, vmem, anywhere],
        out_specs=vmem,
        scratch_shapes=[
            pltpu.VMEM((2, 128, LANES), f32),
            pltpu.VMEM((4, 40, LANES), f32),
            pltpu.SemaphoreType.DMA(()),
        ],
        name="pack",
    )(pos, blocks, level_set, fuel_class, air_state)
    relayed = lax.all_to_all(packed.reshape(devices, REC1, LANES), both, 0, 0)
    lanes_used = -(-blocks.shape[1] // LANES) * LANES
    index = pl.pallas_call(
        lambda *refs: index_kernel(across, *refs),
        out_shape=jax.ShapeDtypeStruct((WORDS + 1, lanes_used), i32),
        in_specs=[smem, vmem, vmem],
        out_specs=vmem,
        scratch_shapes=[pltpu.VMEM((16, lanes_used), i32)],
        cost_estimate=pl.CostEstimate(flops=20_000_000, transcendentals=0, bytes_accessed=10_000),
        name="index",
    )(pos, blocks, adjacency)
    first_rows, last_rows, columns = pl.pallas_call(
        edge_kernel,
        out_shape=(
            pltpu.VMEM((48, LANES), f32),
            pltpu.VMEM((48, LANES), f32),
            pltpu.VMEM((128, LANES), f32),
        ),
        in_specs=[anywhere, anywhere],
        out_specs=(vmem, vmem, vmem),
        scratch_shapes=[pltpu.VMEM((48 * 128, LANES), f32), pltpu.SemaphoreType.DMA(())],
        cost_estimate=pl.CostEstimate(flops=30_000_000, transcendentals=0, bytes_accessed=3_200_000),
        name="edge",
    )(air_state.reshape(48 * 128, LANES), index)
    north = near(lax.ppermute(last_rows, "gx", [(k, k + 1) for k in range(down - 1)]))
    south = near(lax.ppermute(first_rows, "gx", [(k + 1, k) for k in range(down - 1)]))
    chosen = pl.pallas_call(
        select_kernel,
        out_shape=pltpu.VMEM((devices * REC2, LANES), f32),
        in_specs=[smem, vmem, vmem, vmem],
        out_specs=vmem,
        name="select",
    )(index, near(relayed.reshape(devices * REC1, LANES)), north, south)
    columns, chosen = lax.optimization_barrier((columns, chosen))
    west_side = near(lax.ppermute(columns, "gy", [(k, k + 1) for k in range(across - 1)]))
    east_side = near(lax.ppermute(columns, "gy", [(k + 1, k) for k in range(across - 1)]))
    received = lax.all_to_all(chosen.reshape(devices, REC2, LANES), both, 0, 0)
    received = received.reshape(devices * REC2, LANES)[: PIECES * REC2]
    received = near(received)
    level_next, fuel_next, heat = pl.pallas_call(
        lambda *refs: fire_kernel(across, down, *refs),
        out_shape=(
            jax.ShapeDtypeStruct(level_set.shape, f32),
            jax.ShapeDtypeStruct(level_set.shape, f32),
            pltpu.VMEM((devices * HEAT_ROWS, LANES), f32),
        ),
        in_specs=[smem, smem, smem, vmem, vmem, vmem, vmem] + [vmem] * 2,
        out_specs=(vmem, vmem, vmem),
        scratch_shapes=[
            pltpu.VMEM((5, EXT, LANES), f32),
            pltpu.VMEM((5, EXT, LANES), f32),
            pltpu.VMEM((5, EXT, LANES), f32),
            pltpu.VMEM((5, EXT, LANES), f32),
            pltpu.VMEM((2, 5, 40, LANES), f32),
            pltpu.VMEM((40, LANES), f32),
            pltpu.VMEM((2, LANES, 256), f32),
            pltpu.VMEM((4, 256, LANES), f32),
            pltpu.VMEM((2, 5, 8, LANES), i32),
            pltpu.VMEM((4, 32, LANES), f32),
        ],
        name="fire",
    )(
        pos,
        adjacency,
        fuel_props,
        received,
        near(level_set),
        near(fuel_left),
        near(fuel_class),
        west_side,
        east_side,
    )
    gathered = lax.all_to_all(heat.reshape(devices, 1, HEAT_ROWS * LANES), both, 0, 0)
    gathered = near(gathered.reshape(devices * HEAT_ROWS, LANES))
    air_next = pl.pallas_call(
        air_kernel,
        out_shape=jax.ShapeDtypeStruct(air_state.shape, f32),
        in_specs=[vmem, vmem, vmem, vmem, anywhere],
        out_specs=anywhere,
        scratch_shapes=[
            pltpu.VMEM((3, 18, 144, LANES), f32),
            pltpu.VMEM((3, 16, 128, LANES), f32),
            pltpu.VMEM((128, LANES), f32),
            pltpu.SemaphoreType.DMA((16,)),
            pltpu.SemaphoreType.DMA((16,)),
        ],
        cost_estimate=pl.CostEstimate(flops=80_000_000, transcendentals=0, bytes_accessed=6_300_000),
        name="air",
    )(north, south, west_side, east_side, air_state)
    cells = blocks.shape[1] * level_set.shape[1] * level_set.shape[2]
    air_next, totals = pl.pallas_call(
        lambda *refs: heat_kernel(cells, *refs),
        out_shape=(jax.ShapeDtypeStruct(air_state.shape, f32), jax.ShapeDtypeStruct((2,), f32)),
        in_specs=[smem, smem, vmem, anywhere],
        out_specs=(anywhere, smem),
        scratch_shapes=[pltpu.VMEM((128, LANES), f32), pltpu.SemaphoreType.DMA(())],
        input_output_aliases={3: 0},
        name="heat",
    )(pos, blocks, gathered, air_next)
    return (air_next, level_next, fuel_next, totals)


def near(x):
    return pltpu.with_memory_space_constraint(x, pltpu.VMEM)


def solution(mesh):
    in_specs = (
        P(None, None, "gx", "gy"),
        P(("gx", "gy"), None, None),
        P(("gx", "gy"), None, None),
        P(("gx", "gy"), None, None),
        P(),
        P(),
        P(),
    )
    out_specs = (
        P(None, None, "gx", "gy"),
        P(("gx", "gy"), None, None),
        P(("gx", "gy"), None, None),
        P(),
    )
    return jax.shard_map(local, mesh=mesh, in_specs=in_specs, out_specs=out_specs, check_vma=False)
```

```python
import math

import jax
import jax.numpy as jnp
from jax import lax
from jax.experimental import pallas as pl
from jax.experimental.pallas import tpu as pltpu
from jax.sharding import PartitionSpec as P


REF = 8
BA = 32
SUB = 10
PIECES = 32
LANES = 128
UNROLL = 30
RATE_UNROLL = 12
FINISH_UNROLL = 16
AIR_UNROLL = 16
EDGE_UNROLL = 2

step_time = 0.25
smoothing = 0.15
floor_square = 0.25
viscosity = 0.1
courant = 0.25
mixing = 0.1
heating = 2.0

SIDE = 0
CORNER = 10
WIND = 12
REC1 = 16
CORNER2 = 10
WINDA = 11
WINDB = 13
REC2 = 16
HEAT_ROWS = 17

TOP = 8
EXT = 304
FIRST = 24

f32 = jnp.float32
i32 = jnp.int32


def lanes(shape=(8, LANES)):
    return lax.broadcasted_iota(i32, shape, len(shape) - 1)


def rolled(x, shift):
    return pltpu.roll(x, shift % LANES, x.ndim - 1)


def opposite(side):
    return (1, 0, 3, 2)[side]


def pick(table, index):
    return jnp.take_along_axis(table, index, axis=1, mode="promise_in_bounds")


def position():
    return lax.axis_index("gx"), lax.axis_index("gy")


def pack_kernel(blocks, level_hbm, class_hbm, air_hbm, out, level, fuel_class, air, strip, mine, sem):
    loads = [
        pltpu.make_async_copy(level_hbm, level, sem.at[0]),
        pltpu.make_async_copy(class_hbm, fuel_class, sem.at[1]),
        pltpu.make_async_copy(air_hbm.at[0:2, 0], air, sem.at[2]),
    ]
    for load in loads:
        load.start()
    pos = position()
    tile_rows = 128 // BA
    for slot in range(4):
        mine[slot] = -1

    def find(j, count):
        row = blocks[0, j] - pos[0] * tile_rows
        col = blocks[1, j] - pos[1] * tile_rows
        inside = (row >= 0) & (row < tile_rows) & (col >= 0) & (col < tile_rows)

        @pl.when(inside)
        def _():
            mine[count] = row * tile_rows + col

        return count + inside.astype(i32)

    lax.fori_loop(0, blocks.shape[1], find, jnp.int32(0))
    loads[0].wait()
    loads[1].wait()
    lane256 = lanes((256, LANES))
    lane16 = lanes((16, LANES))

    def place(row, first, values):
        out[pl.ds(first * REC1 + row, values.shape[0], stride=REC1), :] = values

    for q in range(2):
        fields = (level[q], fuel_class[q].astype(f32))
        turned = [
            jnp.where(lane256 < 64, field[:, :LANES], field[:, LANES:]).T for field in fields
        ]
        for side in range(4):
            for number, (field, turn) in enumerate(zip(fields, turned)):
                if side == 0:
                    rows = field[0:SUB, :]
                elif side == 1:
                    rows = field[256 - SUB : 256, :]
                elif side == 2:
                    rows = turn[0:SUB, :]
                else:
                    rows = turn[LANES - SUB : LANES, :]
                strip[side, 2 * SUB * number : 2 * SUB * number + SUB, :] = rows[:, :LANES]
                strip[side, 2 * SUB * number + SUB : 2 * SUB * (number + 1), :] = rows[:, LANES:]
            place(SIDE + q * 5 + side, 0, strip[side, 0:32, :])
            place(SIDE + q * 5 + 4, 8 * side, strip[side, 32:40, :])
        for number, field in enumerate(fields):
            half = jnp.where(
                lane16 < 16,
                field[240:256, :LANES],
                jnp.where(
                    lane16 < 32,
                    rolled(field[0:16, :LANES], 16),
                    jnp.where(
                        lane16 < 48,
                        rolled(field[0:16, LANES:], 48),
                        rolled(field[240:256, LANES:], 64),
                    ),
                ),
            )
            place(CORNER + q, 16 * number, jnp.where(lane16 < 64, half, rolled(half, 64)))

    loads[2].wait()
    lane32 = lanes((32, LANES))
    for slot in range(4):
        at = jnp.maximum(mine[slot], 0)
        start = pl.multiple_of((at // tile_rows) * BA, BA)
        shift = LANES - (at % tile_rows) * BA
        u = pltpu.roll(air[0, pl.ds(start, BA), :], shift, 1)
        v = pltpu.roll(air[1, pl.ds(start, BA), :], shift, 1)
        half = jnp.where(lane32 < 32, u, rolled(v, 32))
        place(WIND + slot, 0, jnp.where(lane32 < 64, half, rolled(half, 64)))
    if out.shape[0] > PIECES * REC1:
        out[PIECES * REC1 :, :] = jnp.zeros((out.shape[0] - PIECES * REC1, LANES), f32)


WORDS = 15


def edge_kernel(air_hbm, ready, first_rows, last_rows, columns, air, sem):
    load = pltpu.make_async_copy(air_hbm, air, sem)
    load.start()
    load.wait()
    first_rows[...] = air[pl.ds(0, 48, stride=128), :]
    last_rows[...] = air[pl.ds(127, 48, stride=128), :]
    lane = lanes()

    def gather(group, carry):
        for k in range(EDGE_UNROLL):
            base = pl.multiple_of((group * EDGE_UNROLL + k) * 8, 8)
            total = jnp.zeros((8, LANES), f32)
            for plane in range(48):
                x = air[pl.ds(plane * 128 + base, 8), :]
                total = jnp.where(lane // 2 == plane, rolled(x, 1 + 2 * plane), total)
            columns[pl.ds(base, 8), :] = total
        return carry

    lax.fori_loop(0, 16 // EDGE_UNROLL, gather, 0)


def index_kernel(across, blocks, adjacency, out, padded):
    pos = position()
    total = blocks.shape[1]
    tiles = out.shape[1] // LANES
    relay = jnp.minimum(pos[0] * across + pos[1], PIECES - 1)
    padded[...] = jnp.zeros(padded.shape, i32)
    padded[0:2, 0:total] = blocks[...]
    padded[8:12, 0:total] = adjacency[...]

    def row(number):
        return [
            jnp.broadcast_to(padded[number : number + 1, LANES * u : LANES * (u + 1)], (8, LANES))
            for u in range(tiles)
        ]

    def lookup(table, index):
        found = []
        for u in range(tiles):
            value = pick(table[0], index[u] & (LANES - 1))
            for v in range(1, tiles):
                value = jnp.where(index[u] >> 7 == v, pick(table[v], index[u] & (LANES - 1)), value)
            found.append(value)
        return found

    def each(f, *rows):
        return [f(*values) for values in zip(*rows)]

    lane = lanes()
    tile_of = each(lambda r, c: (r >> 2) * across + (c >> 2), row(0), row(1))
    before = lax.broadcasted_iota(i32, (LANES, LANES), 0)
    here = lanes((LANES, LANES))
    as_rows = [jnp.broadcast_to(t[0:1, :].astype(f32), (LANES, LANES)) for t in tile_of]
    as_cols = [t.T for t in as_rows]
    wind_row = []
    placed = [jnp.zeros((8, 1), f32)] * 4
    own = (pos[0] * across + pos[1]).astype(f32)
    lane = lanes()
    for u in range(tiles):
        slot = jnp.zeros((1, LANES), f32)
        for v in range(u + 1):
            same = (as_cols[v] == as_rows[u]) & (before + LANES * v < here + LANES * u)
            slot = slot + jnp.sum(jnp.where(same, 1.0, 0.0), axis=0, keepdims=True)
        number = (lane + (LANES * u + 1)).astype(f32)
        own_tile = (jnp.broadcast_to(as_rows[u][0:1, :], (8, LANES)) == own) & (number <= total)
        for c in range(4):
            at_slot = own_tile & (jnp.broadcast_to(slot, (8, LANES)) == c)
            placed[c] = placed[c] + jnp.sum(jnp.where(at_slot, number, 0.0), axis=1, keepdims=True)
        wind_row.append(tile_of[u] * REC1 + WIND + jnp.broadcast_to(slot.astype(i32), (8, LANES)))
    near = [row(8 + s) for s in range(4)]
    safe = [each(lambda n: jnp.maximum(n, 0), near[s]) for s in range(4)]

    def diagonal(s, t):
        by_row = lookup(near[t], safe[s])
        by_col = lookup(near[s], safe[t])
        return each(
            lambda n, m, r, c: jnp.maximum(jnp.where(n >= 0, r, jnp.where(m >= 0, c, 0)), 0),
            near[s],
            near[t],
            by_row,
            by_col,
        )

    nw, ne, sw, se = diagonal(0, 2), diagonal(0, 3), diagonal(1, 2), diagonal(1, 3)
    spare_side = relay >> 3
    upper = relay >= 16

    def side_row(j, s):
        return each(lambda b: (b >> 1) * REC1 + SIDE + (b & 1) * 5 + s, j)

    def choose(flag, yes, no):
        return each(lambda a, b: jnp.where(flag, a, b), yes, no)

    words = [side_row(safe[s], opposite(s)) for s in range(4)]
    spare = choose(
        spare_side == 0,
        safe[1],
        choose(spare_side == 1, safe[0], choose(spare_side == 2, safe[3], safe[2])),
    )
    words.append(side_row(spare, 4))
    for j in (ne, se, sw, nw):
        words.append(each(lambda b: (b >> 1) * REC1 + CORNER + (b & 1), j))
    words.append(wind_row)
    for j in (
        choose(upper, safe[0], safe[1]),
        safe[3],
        safe[2],
        choose(upper, ne, se),
        choose(upper, nw, sw),
    ):
        words.append(lookup(wind_row, j))
    for number, word in enumerate(words):
        for u in range(tiles):
            out[number : number + 1, LANES * u : LANES * (u + 1)] = word[u][0:1, :]
    listed = jnp.zeros((8, LANES), f32)
    for c in range(4):
        listed = jnp.where(lane == c, placed[c], listed)
    out[WORDS : WORDS + 1, 0:LANES] = listed[0:1, :].astype(i32)
    if tiles > 1:
        out[WORDS : WORDS + 1, LANES:] = jnp.zeros((1, out.shape[1] - LANES), i32)


def select_kernel(index, received, north, south, out):
    lane1 = lanes((1, LANES))
    lane_col = lane1 % 32 < 16
    first_half = lane1 < 64
    quarter = lane1 // 16

    def one(d):
        def take(word, q):
            return received[pl.ds(index[word, 2 * d + q], 1), :]

        def put(row, value):
            out[pl.ds(d * REC2 + row, 1), :] = value

        for row in range(10):
            put(SIDE + row, take(row % 5, row // 5))
        merged = take(8, 1)
        for k in range(7):
            merged = jnp.where(quarter == k, take(5 + k % 4, k // 4), merged)
        put(CORNER2, merged)
        for q in range(2):
            own, beyond, east, west, corner_east, corner_west = [take(9 + k, q) for k in range(6)]
            put(WINDA + q, jnp.where(first_half, own, beyond))
            put(
                WINDB + q,
                jnp.where(
                    lane_col,
                    jnp.where(first_half, east, corner_east),
                    jnp.where(first_half, west, corner_west),
                ),
            )
        put(REC2 - 1, jnp.zeros((1, LANES), f32))

    def serve(pair, carry):
        one(2 * pair)
        one(2 * pair + 1)
        return carry

    lax.fori_loop(0, out.shape[0] // REC2 // 2, serve, 0)


def fire_kernel(
    across,
    down,
    adjacency,
    props,
    received,
    level,
    fuel_left,
    fuel_class,
    west_side,
    east_side,
    level_hbm,
    fuel_hbm,
    heat_out,
    level_out,
    fuel_out,
    cur_a,
    cur_b,
    base_rate,
    wind_rate,
    wind,
    strips,
    turned,
    tanh_sum,
    links,
    row_heat,
    sem,
):
    cur = (cur_a, cur_b)
    pos = position()
    lane = lanes()
    sub = lax.broadcasted_iota(i32, (8, LANES), 0)
    lane32 = lanes((32, LANES))
    own = 2 * (pos[0] * across + pos[1])

    def got(row, first=0, size=PIECES):
        return received[pl.ds(first * REC2 + row, size, stride=REC2), :]

    def table(value):
        row = jnp.zeros((8, LANES), f32)
        for kind in range(props.shape[1]):
            row = jnp.where(lane == kind, value(kind), row)
        return row

    log2e = math.log2(math.e)
    table_base = table(lambda c: 0.125 * 0.3 * props[0, c])
    table_wind = table_base * table(lambda c: 0.3 * props[1, c])
    table_burn = (-0.5 * step_time * log2e / 4.0) / jnp.where(
        lane < props.shape[1], table(lambda c: props[2, c]), 1.0
    )
    table_heat = table(lambda c: props[3, c])
    table_emit = table(lambda c: 3.0 * props[4, c])

    turned[...] = jnp.zeros(turned.shape, f32)
    for q in range(2):
        for s in range(4):
            strips[0:32, :] = got(SIDE + q * 5 + s)
            strips[32:40, :] = got(SIDE + q * 5 + 4, 8 * opposite(s), 8)
            for number in range(2):
                low = strips[2 * SUB * number : 2 * SUB * number + SUB, :]
                high = strips[2 * SUB * number + SUB : 2 * SUB * (number + 1), :]
                if s < 2:
                    at = FIRST - SUB if s == 0 else FIRST + 256
                    target = cur[number]
                    target[3 * q, at : at + SUB, :] = low
                    target[3 * q + 1, at : at + SUB, :] = high
                else:
                    at = (54, 118)[q] if s == 2 else (0, 64)[q]
                    turned[number, at : at + SUB, :LANES] = low
                    turned[number, at : at + SUB, LANES:] = high
    for number in range(2):
        cur[number][2, FIRST : FIRST + 256, :] = turned[number].T
        corner = got(CORNER2, 16 * number, 16)
        cur[number][2, TOP : TOP + 16, :] = corner
        cur[number][2, FIRST + 256 : FIRST + 272, :] = jnp.where(
            lanes((16, LANES)) % 64 < 32, rolled(corner, -16), rolled(corner, 16)
        )
    for q in range(2):
        for half in range(2):
            cur_a[3 * q + half, FIRST : FIRST + 256, :] = level[q, :, LANES * half : LANES * (half + 1)]
            cur_b[3 * q + half, FIRST : FIRST + 256, :] = fuel_class[
                q, :, LANES * half : LANES * (half + 1)
            ].astype(f32)

    def rates(group, carry):
        for k in range(RATE_UNROLL):
            at = pl.multiple_of((1 + group * RATE_UNROLL + k) * 8, 8)
            for t in range(5):
                kind = cur_b[t, pl.ds(at, 8), :].astype(i32) & 127
                base_rate[t, pl.ds(at, 8), :] = pick(table_base, kind)
                wind_rate[t, pl.ds(at, 8), :] = pick(table_wind, kind)
        return carry

    lax.fori_loop(0, 36 // RATE_UNROLL, rates, 0)

    inner = lane % 64
    side_col = jnp.where(inner < 16, inner // 8, jnp.where(inner >= 48, 30 + (inner - 48) // 8, 0))
    for k in range(2):
        for t in range(5):
            for quarter in range(4):
                for outer in (0, 64):
                    if outer and quarter in (1, 2):
                        continue
                    at = outer + k * 32
                    if t == 2:
                        west = got(WINDB, 8 * quarter, 8)
                        east = got(WINDB + 1, 8 * quarter, 8)
                        index = side_col + at
                        value = jnp.where(lane < 64, pick(west, index), pick(east, index))
                    else:
                        source = got(WINDA + t // 3, 8 * quarter, 8)
                        value = pick(source, lane // 8 + (at + 16 * (t % 3)))
                    value = value * log2e
                    if not outer:
                        wind[k, t, 3 + 8 * quarter : 11 + 8 * quarter, :] = value
                    elif quarter == 3:
                        wind[k, t, 1:3, :] = value[6:8, :]
                    else:
                        wind[k, t, 35:37, :] = value[0:2, :]

    def there(j):
        return j >= 0

    across_links = []
    groups = []
    for q in range(2):
        i = own + q
        near = [adjacency[s, i] for s in range(4)]
        safe = [jnp.maximum(near[s], 0) for s in range(4)]

        def joined(s, t):
            return there(near[s]) & there(adjacency[t, safe[s]])

        groups.append([(there(near[s]), joined(2, s), joined(3, s)) for s in range(2)])
        across_links.append([[joined(0, t), there(near[t]), joined(1, t)] for t in (2, 3)])

    def as_int(flag):
        return jnp.where(flag, 1, 0)

    for line in range(2):
        for q in range(2):
            mid, west, east = groups[q][line]
            row = jnp.broadcast_to(as_int(mid), (8, LANES))
            links[line, 3 * q] = row
            links[line, 3 * q + 1] = row
        w0, e0 = groups[0][line][1:]
        w1, e1 = groups[1][line][1:]
        links[line, 2] = jnp.where(
            lane < 32,
            as_int(e0),
            jnp.where(lane < 64, as_int(w0), jnp.where(lane < 96, as_int(e1), as_int(w1))),
        )

    is0 = lane == 0
    is63 = lane == 63
    is64 = lane == 64
    is127 = lane == 127
    tanh_sum[...] = jnp.zeros(tanh_sum.shape, f32)

    def make_masks(region):
        (w0, e0), (w1, e1) = [
            [as_int(across_links[q][t][region]) for t in range(2)] for q in range(2)
        ]
        on = [jnp.broadcast_to(flag, (8, LANES)) > 0 for flag in (w0, e0, w1, e1)]
        return on

    def update(source, target, chunk, masks, rows_edge, main):
        lw0, le0, lw1, le1 = masks
        at = chunk * 8
        x = [source[t, pl.ds(at, 8), :] for t in range(5)]
        up = [source[t, pl.ds(at - 1, 8), :] for t in range(5)]
        dn = [source[t, pl.ds(at + 1, 8), :] for t in range(5)]
        if rows_edge is not None:
            kind, line, row = rows_edge
            for t in range(5):
                broken = (sub == row) & (links[line, t] == 0)
                if kind == "up":
                    up[t] = jnp.where(broken, x[t], up[t])
                else:
                    dn[t] = jnp.where(broken, x[t], dn[t])
        right = [rolled(v, 1) for v in x]
        left = [rolled(v, -1) for v in x]
        h = x[2]
        west = [
            jnp.where(is0, jnp.where(lw0, rolled(h, 65), x[0]), right[0]),
            jnp.where(is0, right[0], right[1]),
            jnp.where(
                is0,
                jnp.where(le0, right[1], h),
                jnp.where(is64, jnp.where(le1, rolled(x[4], 65), h), right[2]),
            ),
            jnp.where(is0, jnp.where(lw1, right[2], x[3]), right[3]),
            jnp.where(is0, right[3], right[4]),
        ]
        east = [
            jnp.where(is127, left[1], left[0]),
            jnp.where(is127, jnp.where(le0, left[2], x[1]), left[1]),
            jnp.where(
                is127,
                jnp.where(lw1, left[3], h),
                jnp.where(is63, jnp.where(lw0, rolled(x[0], 63), h), left[2]),
            ),
            jnp.where(is127, left[4], left[3]),
            jnp.where(is127, jnp.where(le1, rolled(h, -65), x[4]), left[4]),
        ]
        for t in range(5):
            diff_rows = dn[t] - up[t]
            diff_cols = east[t] - west[t]
            around = (dn[t] + up[t]) + (east[t] + west[t])
            square = diff_rows * diff_rows + (diff_cols * diff_cols + 4.0 * floor_square)
            inverse = lax.rsqrt(square)
            wind_r = wind[0, t, pl.ds(chunk, 1), :]
            wind_c = wind[1, t, pl.ds(chunk, 1), :]
            along = (wind_r * diff_rows + wind_c * diff_cols) * inverse
            soft = jnp.log(1.0 + jnp.exp2(along))
            power = soft * soft * lax.rsqrt(soft)
            b = base_rate[t, pl.ds(at, 8), :]
            w = wind_rate[t, pl.ds(at, 8), :]
            new = ((1.0 - 4.0 * smoothing) * x[t] + smoothing * around) - (b + w * power) * (
                square * inverse
            )
            target[t, pl.ds(at, 8), :] = new
            if main and t != 2:
                m = t - t // 3
                tanh_sum[m, pl.ds(at - FIRST, 8), :] += jnp.tanh(new)

    above = make_masks(0)
    within = make_masks(1)
    below = make_masks(2)

    def outer(source, target):
        update(source, target, 1, above, None, False)
        update(source, target, 36, below, None, False)

    def substep(source, target):
        update(source, target, 2, above, ("down", 0, 7), False)
        update(source, target, 3, within, ("up", 0, 0), True)

        def middle(group, carry):
            for k in range(UNROLL):
                update(source, target, 4 + group * UNROLL + k, within, None, True)
            return carry

        lax.fori_loop(0, 30 // UNROLL, middle, 0)
        update(source, target, 34, within, ("down", 1, 7), True)
        update(source, target, 35, below, ("up", 1, 0), False)

    def two_substeps(pair, carry):
        substep(cur_a, cur_b)
        substep(cur_b, cur_a)
        return carry

    outer(cur_a, cur_b)
    lax.fori_loop(0, SUB // 2, two_substeps, 0)

    last = SUB % 2

    def finish(chunk, burn, emit):
        at = pl.multiple_of(chunk * 8, 8)
        for q in range(2):
            for half in range(2):
                t = 3 * q + half
                cols = slice(LANES * half, LANES * (half + 1))
                final = cur[last][t, pl.ds(FIRST + at, 8), :]
                level_out[q, pl.ds(at, 8), cols] = final
                burn = burn + (0.5 - 0.5 * jnp.tanh(final))
                kind = fuel_class[q, pl.ds(at, 8), cols]
                fuel = fuel_left[q, pl.ds(at, 8), cols]
                power = pick(table_burn, kind) * (float(SUB) - tanh_sum[2 * q + half, pl.ds(at, 8), :])
                new_fuel = fuel * jnp.exp2(power)
                fuel_out[q, pl.ds(at, 8), cols] = new_fuel
                spent = fuel - new_fuel
                emit = emit + pick(table_emit, kind) * spent
                released = pick(table_heat, kind) * spent
                row_heat[2 * q + half, pl.ds(chunk, 1), :] = jnp.sum(released, axis=0, keepdims=True)
        return burn, emit

    blank = jnp.zeros((8, LANES), f32)
    sums = [blank] * 4

    def stores(group):
        rows = pl.ds(group * (8 * FINISH_UNROLL), 8 * FINISH_UNROLL)
        return [
            pltpu.make_async_copy(level_out.at[:, rows, :], level_hbm.at[:, rows, :], sem.at[0, group]),
            pltpu.make_async_copy(fuel_out.at[:, rows, :], fuel_hbm.at[:, rows, :], sem.at[1, group]),
        ]

    def finish_group(group, totals):
        totals = list(totals)
        for k in range(FINISH_UNROLL):
            pair = 2 * (k % 2)
            totals[pair], totals[pair + 1] = finish(
                group * FINISH_UNROLL + k, totals[pair], totals[pair + 1]
            )
        for copy in stores(group):
            copy.start()
        return tuple(totals)

    sums = lax.fori_loop(0, 32 // FINISH_UNROLL, finish_group, tuple(sums))
    burn = sums[0] + sums[2]
    emit = sums[1] + sums[3]
    devices = across * down

    def spread(row, value):
        heat_out[pl.ds(row, devices, stride=HEAT_ROWS), :] = jnp.broadcast_to(value, (devices, LANES))

    source_lane = lax.broadcasted_iota(i32, (LANES, LANES), 0) // REF
    target_lane = lanes((LANES, LANES))
    for q in range(2):
        packed = blank
        for g in range(4):
            for half in range(2):
                gather = jnp.where(
                    target_lane == 32 * g + 16 * half + source_lane, heating / (REF * REF), 0.0
                ).astype(f32)
                packed = packed + jnp.dot(
                    row_heat[2 * q + half, 8 * g : 8 * g + 8, :],
                    gather,
                    precision=lax.Precision.HIGHEST,
                    preferred_element_type=f32,
                )
        for row in range(8):
            spread(8 * q + row, packed[row : row + 1, :])
    burn_sum = jnp.sum(jnp.sum(burn, axis=0, keepdims=True), axis=1, keepdims=True)
    emit_sum = jnp.sum(jnp.sum(emit, axis=0, keepdims=True), axis=1, keepdims=True)
    lane1 = lanes((1, LANES))
    spread(16, jnp.where(lane1 == 0, burn_sum, jnp.where(lane1 == 1, emit_sum, 0.0)))
    for group in range(32 // FINISH_UNROLL):
        for copy in stores(group):
            copy.wait()


def air_kernel(north, south, west_side, east_side, air_hbm, air_out, surface, air, fresh, sides, sem_in, sem_out):
    def load(number):
        return pltpu.make_async_copy(
            air_hbm.at[:, number], air.at[:, number + 1, 8:136, :], sem_in.at[number]
        )

    def store(number):
        return pltpu.make_async_copy(fresh.at[:, number], air_out.at[:, number], sem_out.at[number])

    levels = 16
    for number in range(levels):
        load(number).start()
    lane = lanes()
    is0 = lane == 0
    is127 = lane == 127
    zero = jnp.zeros((128, LANES), f32)
    for f in range(3):
        air[f, 0, 8:136, :] = zero
        air[f, levels + 1, 8:136, :] = zero
    for plane in range(48):
        at = (plane // 16, plane % 16 + 1)
        air[at[0], at[1], 7:8, :] = north[plane : plane + 1, :]
        air[at[0], at[1], 136:137, :] = south[plane : plane + 1, :]
    sides[...] = jnp.where(lanes((128, LANES)) % 2 == 1, east_side[...], west_side[...])

    load(0).wait()

    def air_level(number, carry):
        @pl.when(number < levels - 1)
        def _():
            load(number + 1).wait()

        def air_rows(group, inner_carry):
            for k in range(AIR_UNROLL):
                row = group * (8 * AIR_UNROLL) + k * 8
                at = 8 + row
                halo = sides[pl.ds(row, 8), :]
                x = [air[f, number + 1, pl.ds(at, 8), :] for f in range(3)]
                for f in range(3):
                    up = air[f, number + 1, pl.ds(at - 1, 8), :]
                    dn = air[f, number + 1, pl.ds(at + 1, 8), :]
                    over = air[f, number + 2, pl.ds(at, 8), :]
                    under = air[f, number, pl.ds(at, 8), :]
                    mine = pltpu.roll(halo, LANES - 1 - 2 * (f * 16 + number), 1)
                    west = rolled(jnp.where(is127, mine, x[f]), 1)
                    east = rolled(jnp.where(is0, mine, x[f]), -1)
                    around = (up + dn) + (west + east)
                    advect = x[0] * (dn - up) + x[1] * (east - west)
                    fresh[f, number, pl.ds(row, 8), :] = (
                        (1.0 - 4.0 * viscosity - 2.0 * mixing) * x[f]
                        + viscosity * around
                        - (0.5 * courant) * advect
                        + mixing * (over + under)
                    )
            return inner_carry

        lax.fori_loop(0, 16 // AIR_UNROLL, air_rows, 0)
        store(number).start()
        return carry

    lax.fori_loop(0, levels, air_level, 0)

    surface[...] = fresh[2, 0]

    def drain(number, carry):
        store(number).wait()
        return carry

    lax.fori_loop(0, levels, drain, 0)


def heat_kernel(cells, blocks, index, gathered, plane, air_in, air_out, totals, warm, sem):
    pos = position()
    tile_rows = 128 // BA
    lane = lanes()
    warm[...] = plane[...]
    for slot in range(4):
        j = index[WORDS, slot] - 1

        @pl.when(j >= 0)
        def _():
            row = blocks[0, j] - pos[0] * tile_rows
            col = blocks[1, j] - pos[1] * tile_rows
            heat = gathered[pl.ds((j // 2) * HEAT_ROWS + 8 * (j % 2), 8), :]
            for g in range(4):
                moved = pltpu.roll(heat, (col - g + 4) * BA % LANES, 1)
                at = pl.multiple_of(row * BA + 8 * g, 8)
                warm[pl.ds(at, 8), :] += jnp.where(lane // BA == col, moved, 0.0)

    store = pltpu.make_async_copy(warm, air_out.at[2, 0], sem)
    store.start()
    devices = gathered.shape[0] // HEAT_ROWS
    sums = jnp.sum(gathered[pl.ds(16, devices, stride=HEAT_ROWS), :], axis=0, keepdims=True)
    lane1 = lanes((1, LANES))
    for k in range(2):
        totals[k] = jnp.sum(jnp.where(lane1 == k, sums, 0.0)) * (1.0 / cells)
    store.wait()


def local(air_state, level_set, fuel_left, fuel_class, fuel_props, blocks, adjacency):
    down = lax.axis_size("gx")
    across = lax.axis_size("gy")
    devices = down * across
    both = ("gx", "gy")
    smem = pl.BlockSpec(memory_space=pltpu.SMEM)
    vmem = pl.BlockSpec(memory_space=pltpu.VMEM)
    anywhere = pl.BlockSpec(memory_space=pl.ANY)
    blocks = blocks.T
    adjacency = adjacency.T
    packed = pl.pallas_call(
        pack_kernel,
        out_shape=pltpu.VMEM((devices * REC1, LANES), f32),
        in_specs=[smem, anywhere, anywhere, anywhere],
        out_specs=vmem,
        scratch_shapes=[
            pltpu.VMEM(level_set.shape, f32),
            pltpu.VMEM(level_set.shape, i32),
            pltpu.VMEM((2, 128, LANES), f32),
            pltpu.VMEM((4, 40, LANES), f32),
            pltpu.SMEM((8,), i32),
            pltpu.SemaphoreType.DMA((3,)),
        ],
        name="pack",
    )(blocks, level_set, fuel_class, air_state)
    relayed = lax.all_to_all(packed.reshape(devices, REC1, LANES), both, 0, 0)
    lanes_used = -(-blocks.shape[1] // LANES) * LANES
    index = pl.pallas_call(
        lambda *refs: index_kernel(across, *refs),
        out_shape=jax.ShapeDtypeStruct((WORDS + 1, lanes_used), i32),
        in_specs=[vmem, vmem],
        out_specs=vmem,
        scratch_shapes=[pltpu.VMEM((16, lanes_used), i32)],
        cost_estimate=pl.CostEstimate(flops=20_000_000, transcendentals=0, bytes_accessed=10_000),
        name="index",
    )(blocks, adjacency)
    first_rows, last_rows, columns = pl.pallas_call(
        edge_kernel,
        out_shape=(
            pltpu.VMEM((48, LANES), f32),
            pltpu.VMEM((48, LANES), f32),
            pltpu.VMEM((128, LANES), f32),
        ),
        in_specs=[anywhere, anywhere],
        out_specs=(vmem, vmem, vmem),
        scratch_shapes=[pltpu.VMEM((48 * 128, LANES), f32), pltpu.SemaphoreType.DMA(())],
        cost_estimate=pl.CostEstimate(flops=30_000_000, transcendentals=0, bytes_accessed=3_200_000),
        name="edge",
    )(air_state.reshape(48 * 128, LANES), index)
    north = near(lax.ppermute(last_rows, "gx", [(k, k + 1) for k in range(down - 1)]))
    south = near(lax.ppermute(first_rows, "gx", [(k + 1, k) for k in range(down - 1)]))
    chosen = pl.pallas_call(
        select_kernel,
        out_shape=pltpu.VMEM((devices * REC2, LANES), f32),
        in_specs=[smem, vmem, vmem, vmem],
        out_specs=vmem,
        name="select",
    )(index, near(relayed.reshape(devices * REC1, LANES)), north, south)
    columns, chosen = lax.optimization_barrier((columns, chosen))
    west_side = near(lax.ppermute(columns, "gy", [(k, k + 1) for k in range(across - 1)]))
    east_side = near(lax.ppermute(columns, "gy", [(k + 1, k) for k in range(across - 1)]))
    received = lax.all_to_all(chosen.reshape(devices, REC2, LANES), both, 0, 0)
    received = received.reshape(devices * REC2, LANES)[: PIECES * REC2]
    received = near(received)
    level_next, fuel_next, heat = pl.pallas_call(
        lambda *refs: fire_kernel(across, down, *refs),
        out_shape=(
            jax.ShapeDtypeStruct(level_set.shape, f32),
            jax.ShapeDtypeStruct(level_set.shape, f32),
            pltpu.VMEM((devices * HEAT_ROWS, LANES), f32),
        ),
        in_specs=[smem, smem, vmem, vmem, vmem, vmem] + [vmem] * 2,
        out_specs=(anywhere, anywhere, vmem),
        scratch_shapes=[
            pltpu.VMEM(level_set.shape, f32),
            pltpu.VMEM(level_set.shape, f32),
            pltpu.VMEM((5, EXT, LANES), f32),
            pltpu.VMEM((5, EXT, LANES), f32),
            pltpu.VMEM((5, EXT, LANES), f32),
            pltpu.VMEM((5, EXT, LANES), f32),
            pltpu.VMEM((2, 5, 40, LANES), f32),
            pltpu.VMEM((40, LANES), f32),
            pltpu.VMEM((2, LANES, 256), f32),
            pltpu.VMEM((4, 256, LANES), f32),
            pltpu.VMEM((2, 5, 8, LANES), i32),
            pltpu.VMEM((4, 32, LANES), f32),
            pltpu.SemaphoreType.DMA((2, 32 // FINISH_UNROLL)),
        ],
        name="fire",
    )(
        adjacency,
        fuel_props,
        received,
        near(level_set),
        near(fuel_left),
        near(fuel_class),
        west_side,
        east_side,
    )
    gathered = lax.all_to_all(heat.reshape(devices, 1, HEAT_ROWS * LANES), both, 0, 0)
    gathered = near(gathered.reshape(devices * HEAT_ROWS, LANES))
    air_next, plane = pl.pallas_call(
        air_kernel,
        out_shape=(jax.ShapeDtypeStruct(air_state.shape, f32), pltpu.VMEM((128, LANES), f32)),
        in_specs=[vmem, vmem, vmem, vmem, anywhere],
        out_specs=(anywhere, vmem),
        scratch_shapes=[
            pltpu.VMEM((3, 18, 144, LANES), f32),
            pltpu.VMEM((3, 16, 128, LANES), f32),
            pltpu.VMEM((128, LANES), f32),
            pltpu.SemaphoreType.DMA((16,)),
            pltpu.SemaphoreType.DMA((16,)),
        ],
        cost_estimate=pl.CostEstimate(flops=80_000_000, transcendentals=0, bytes_accessed=6_300_000),
        name="air",
    )(north, south, west_side, east_side, air_state)
    cells = blocks.shape[1] * level_set.shape[1] * level_set.shape[2]
    air_next, totals = pl.pallas_call(
        lambda *refs: heat_kernel(cells, *refs),
        out_shape=(jax.ShapeDtypeStruct(air_state.shape, f32), jax.ShapeDtypeStruct((2,), f32)),
        in_specs=[smem, smem, vmem, vmem, anywhere],
        out_specs=(anywhere, smem),
        scratch_shapes=[pltpu.VMEM((128, LANES), f32), pltpu.SemaphoreType.DMA(())],
        input_output_aliases={4: 0},
        name="heat",
    )(blocks, index, gathered, plane, air_next)
    return (air_next, level_next, fuel_next, totals)


def near(x):
    return pltpu.with_memory_space_constraint(x, pltpu.VMEM)


def solution(mesh):
    in_specs = (
        P(None, None, "gx", "gy"),
        P(("gx", "gy"), None, None),
        P(("gx", "gy"), None, None),
        P(("gx", "gy"), None, None),
        P(),
        P(),
        P(),
    )
    out_specs = (
        P(None, None, "gx", "gy"),
        P(("gx", "gy"), None, None),
        P(("gx", "gy"), None, None),
        P(),
    )
    return jax.shard_map(local, mesh=mesh, in_specs=in_specs, out_specs=out_specs, check_vma=False)
```

```python
import math

import jax
import jax.numpy as jnp
from jax import lax
from jax.experimental import pallas as pl
from jax.experimental.pallas import tpu as pltpu
from jax.sharding import PartitionSpec as P


REF = 8
BA = 32
SUB = 10
PIECES = 32
LANES = 128
UNROLL = 30
RATE_UNROLL = 12
FINISH_UNROLL = 16
AIR_UNROLL = 16
EDGE_UNROLL = 2

step_time = 0.25
smoothing = 0.15
floor_square = 0.25
viscosity = 0.1
courant = 0.25
mixing = 0.1
heating = 2.0

SIDE = 0
CORNER = 10
WIND = 12
REC1 = 16
CORNER2 = 10
WINDA = 11
WINDB = 13
REC2 = 16
HEAT_ROWS = 17

TOP = 8
EXT = 304
FIRST = 24

f32 = jnp.float32
i32 = jnp.int32


def lanes(shape=(8, LANES)):
    return lax.broadcasted_iota(i32, shape, len(shape) - 1)


def rolled(x, shift):
    return pltpu.roll(x, shift % LANES, x.ndim - 1)


def opposite(side):
    return (1, 0, 3, 2)[side]


def pick(table, index):
    return jnp.take_along_axis(table, index, axis=1, mode="promise_in_bounds")


def position():
    return lax.axis_index("gx"), lax.axis_index("gy")


def pack_kernel(blocks, level_hbm, class_hbm, air_hbm, out, level, fuel_class, air, strip, mine, sem):
    loads = [
        pltpu.make_async_copy(level_hbm, level, sem.at[0]),
        pltpu.make_async_copy(class_hbm, fuel_class, sem.at[1]),
        pltpu.make_async_copy(air_hbm.at[0:2, 0], air, sem.at[2]),
    ]
    for load in loads:
        load.start()
    pos = position()
    tile_rows = 128 // BA
    for slot in range(4):
        mine[slot] = -1

    def find(j, count):
        row = blocks[0, j] - pos[0] * tile_rows
        col = blocks[1, j] - pos[1] * tile_rows
        inside = (row >= 0) & (row < tile_rows) & (col >= 0) & (col < tile_rows)

        @pl.when(inside)
        def _():
            mine[count] = row * tile_rows + col

        return count + inside.astype(i32)

    lax.fori_loop(0, blocks.shape[1], find, jnp.int32(0))
    loads[0].wait()
    loads[1].wait()
    lane256 = lanes((256, LANES))
    lane16 = lanes((16, LANES))

    def place(row, first, values):
        out[pl.ds(first * REC1 + row, values.shape[0], stride=REC1), :] = values

    for q in range(2):
        fields = (level[q], fuel_class[q].astype(f32))
        turned = [
            jnp.where(lane256 < 64, field[:, :LANES], field[:, LANES:]).T for field in fields
        ]
        for side in range(4):
            for number, (field, turn) in enumerate(zip(fields, turned)):
                if side == 0:
                    rows = field[0:SUB, :]
                elif side == 1:
                    rows = field[256 - SUB : 256, :]
                elif side == 2:
                    rows = turn[0:SUB, :]
                else:
                    rows = turn[LANES - SUB : LANES, :]
                strip[side, 2 * SUB * number : 2 * SUB * number + SUB, :] = rows[:, :LANES]
                strip[side, 2 * SUB * number + SUB : 2 * SUB * (number + 1), :] = rows[:, LANES:]
            place(SIDE + q * 5 + side, 0, strip[side, 0:32, :])
            place(SIDE + q * 5 + 4, 8 * side, strip[side, 32:40, :])
        for number, field in enumerate(fields):
            half = jnp.where(
                lane16 < 16,
                field[240:256, :LANES],
                jnp.where(
                    lane16 < 32,
                    rolled(field[0:16, :LANES], 16),
                    jnp.where(
                        lane16 < 48,
                        rolled(field[0:16, LANES:], 48),
                        rolled(field[240:256, LANES:], 64),
                    ),
                ),
            )
            place(CORNER + q, 16 * number, jnp.where(lane16 < 64, half, rolled(half, 64)))

    loads[2].wait()
    lane32 = lanes((32, LANES))
    for slot in range(4):
        at = jnp.maximum(mine[slot], 0)
        start = pl.multiple_of((at // tile_rows) * BA, BA)
        shift = LANES - (at % tile_rows) * BA
        u = pltpu.roll(air[0, pl.ds(start, BA), :], shift, 1)
        v = pltpu.roll(air[1, pl.ds(start, BA), :], shift, 1)
        half = jnp.where(lane32 < 32, u, rolled(v, 32))
        place(WIND + slot, 0, jnp.where(lane32 < 64, half, rolled(half, 64)))
    if out.shape[0] > PIECES * REC1:
        out[PIECES * REC1 :, :] = jnp.zeros((out.shape[0] - PIECES * REC1, LANES), f32)


WORDS = 15


def edge_kernel(air_hbm, ready, first_rows, last_rows, columns, air, sem):
    load = pltpu.make_async_copy(air_hbm, air, sem)
    load.start()
    load.wait()
    first_rows[...] = air[pl.ds(0, 48, stride=128), :]
    last_rows[...] = air[pl.ds(127, 48, stride=128), :]
    lane = lanes()

    def gather(group, carry):
        for k in range(EDGE_UNROLL):
            base = pl.multiple_of((group * EDGE_UNROLL + k) * 8, 8)
            total = jnp.zeros((8, LANES), f32)
            for plane in range(48):
                x = air[pl.ds(plane * 128 + base, 8), :]
                total = jnp.where(lane // 2 == plane, rolled(x, 1 + 2 * plane), total)
            columns[pl.ds(base, 8), :] = total
        return carry

    lax.fori_loop(0, 16 // EDGE_UNROLL, gather, 0)


def index_kernel(across, blocks, adjacency, near_own, props, out, tables, flags, padded):
    pos = position()
    total = blocks.shape[1]
    tiles = out.shape[1] // LANES
    relay = jnp.minimum(pos[0] * across + pos[1], PIECES - 1)
    padded[...] = jnp.zeros(padded.shape, i32)
    padded[0:2, 0:total] = blocks[...]
    padded[8:12, 0:total] = adjacency[...]

    def row(number):
        return [
            jnp.broadcast_to(padded[number : number + 1, LANES * u : LANES * (u + 1)], (8, LANES))
            for u in range(tiles)
        ]

    def lookup(table, index):
        found = []
        for u in range(tiles):
            value = pick(table[0], index[u] & (LANES - 1))
            for v in range(1, tiles):
                value = jnp.where(index[u] >> 7 == v, pick(table[v], index[u] & (LANES - 1)), value)
            found.append(value)
        return found

    def each(f, *rows):
        return [f(*values) for values in zip(*rows)]

    lane = lanes()
    tile_of = each(lambda r, c: (r >> 2) * across + (c >> 2), row(0), row(1))
    before = lax.broadcasted_iota(i32, (LANES, LANES), 0)
    here = lanes((LANES, LANES))
    as_rows = [jnp.broadcast_to(t[0:1, :].astype(f32), (LANES, LANES)) for t in tile_of]
    as_cols = [t.T for t in as_rows]
    wind_row = []
    placed = [jnp.zeros((8, 1), f32)] * 4
    own = (pos[0] * across + pos[1]).astype(f32)
    lane = lanes()
    for u in range(tiles):
        slot = jnp.zeros((1, LANES), f32)
        for v in range(u + 1):
            same = (as_cols[v] == as_rows[u]) & (before + LANES * v < here + LANES * u)
            slot = slot + jnp.sum(jnp.where(same, 1.0, 0.0), axis=0, keepdims=True)
        number = (lane + (LANES * u + 1)).astype(f32)
        own_tile = (jnp.broadcast_to(as_rows[u][0:1, :], (8, LANES)) == own) & (number <= total)
        for c in range(4):
            at_slot = own_tile & (jnp.broadcast_to(slot, (8, LANES)) == c)
            placed[c] = placed[c] + jnp.sum(jnp.where(at_slot, number, 0.0), axis=1, keepdims=True)
        wind_row.append(tile_of[u] * REC1 + WIND + jnp.broadcast_to(slot.astype(i32), (8, LANES)))
    near = [row(8 + s) for s in range(4)]
    safe = [each(lambda n: jnp.maximum(n, 0), near[s]) for s in range(4)]

    def diagonal(s, t):
        by_row = lookup(near[t], safe[s])
        by_col = lookup(near[s], safe[t])
        return each(
            lambda n, m, r, c: jnp.maximum(jnp.where(n >= 0, r, jnp.where(m >= 0, c, 0)), 0),
            near[s],
            near[t],
            by_row,
            by_col,
        )

    nw, ne, sw, se = diagonal(0, 2), diagonal(0, 3), diagonal(1, 2), diagonal(1, 3)
    spare_side = relay >> 3
    upper = relay >= 16

    def side_row(j, s):
        return each(lambda b: (b >> 1) * REC1 + SIDE + (b & 1) * 5 + s, j)

    def choose(flag, yes, no):
        return each(lambda a, b: jnp.where(flag, a, b), yes, no)

    words = [side_row(safe[s], opposite(s)) for s in range(4)]
    spare = choose(
        spare_side == 0,
        safe[1],
        choose(spare_side == 1, safe[0], choose(spare_side == 2, safe[3], safe[2])),
    )
    words.append(side_row(spare, 4))
    for j in (ne, se, sw, nw):
        words.append(each(lambda b: (b >> 1) * REC1 + CORNER + (b & 1), j))
    words.append(wind_row)
    for j in (
        choose(upper, safe[0], safe[1]),
        safe[3],
        safe[2],
        choose(upper, ne, se),
        choose(upper, nw, sw),
    ):
        words.append(lookup(wind_row, j))
    for number, word in enumerate(words):
        for u in range(tiles):
            out[number : number + 1, LANES * u : LANES * (u + 1)] = word[u][0:1, :]
    device = pos[0] * across + pos[1]

    def table(value):
        row = jnp.zeros((8, LANES), f32)
        for kind in range(props.shape[1]):
            row = jnp.where(lane == kind, value(kind), row)
        return row

    log2e = math.log2(math.e)
    table_base = table(lambda c: 0.125 * 0.3 * props[0, c])
    table_wind = table_base * table(lambda c: 0.3 * props[1, c])
    table_burn = (-0.5 * step_time * log2e / 4.0) / jnp.where(
        lane < props.shape[1], table(lambda c: props[2, c]), 1.0
    )
    table_heat = table(lambda c: props[3, c])
    table_emit = table(lambda c: 3.0 * props[4, c])
    for k, values in enumerate((table_base, table_wind, table_burn, table_heat, table_emit)):
        tables[k] = values

    def there(j):
        return j >= 0

    across_links = []
    groups = []
    for q in range(2):
        i = 2 * device + q
        near = [near_own[s, i] for s in range(4)]
        safe = [jnp.maximum(near[s], 0) for s in range(4)]

        def joined(s, t):
            return there(near[s]) & there(near_own[t, safe[s]])

        groups.append([(there(near[s]), joined(2, s), joined(3, s)) for s in range(2)])
        across_links.append([[joined(0, t), there(near[t]), joined(1, t)] for t in (2, 3)])

    def as_int(flag):
        return jnp.where(flag, 1, 0)

    for line in range(2):
        for q in range(2):
            mid, west, east = groups[q][line]
            row = jnp.broadcast_to(as_int(mid), (8, LANES))
            flags[12 + 5 * line + 3 * q] = row
            flags[12 + 5 * line + 3 * q + 1] = row
        w0, e0 = groups[0][line][1:]
        w1, e1 = groups[1][line][1:]
        flags[12 + 5 * line + 2] = jnp.where(
            lane < 32,
            as_int(e0),
            jnp.where(lane < 64, as_int(w0), jnp.where(lane < 96, as_int(e1), as_int(w1))),
        )

    for region in range(3):
        for k in range(4):
            flag = as_int(across_links[k // 2][k % 2][region])
            flags[4 * region + k] = jnp.broadcast_to(flag, (8, LANES))
    listed = jnp.zeros((8, LANES), f32)
    for c in range(4):
        listed = jnp.where(lane == c, placed[c], listed)
    out[WORDS : WORDS + 1, 0:LANES] = listed[0:1, :].astype(i32)
    if tiles > 1:
        out[WORDS : WORDS + 1, LANES:] = jnp.zeros((1, out.shape[1] - LANES), i32)


def select_kernel(index, received, out):
    lane1 = lanes((1, LANES))
    lane_col = lane1 % 32 < 16
    first_half = lane1 < 64
    quarter = lane1 // 16

    def one(d):
        def take(word, q):
            return received[pl.ds(index[word, 2 * d + q], 1), :]

        def put(row, value):
            out[pl.ds(d * REC2 + row, 1), :] = value

        for row in range(10):
            put(SIDE + row, take(row % 5, row // 5))
        merged = take(8, 1)
        for k in range(7):
            merged = jnp.where(quarter == k, take(5 + k % 4, k // 4), merged)
        put(CORNER2, merged)
        for q in range(2):
            own, beyond, east, west, corner_east, corner_west = [take(9 + k, q) for k in range(6)]
            put(WINDA + q, jnp.where(first_half, own, beyond))
            put(
                WINDB + q,
                jnp.where(
                    lane_col,
                    jnp.where(first_half, east, corner_east),
                    jnp.where(first_half, west, corner_west),
                ),
            )
        put(REC2 - 1, jnp.zeros((1, LANES), f32))

    def serve(pair, carry):
        one(2 * pair)
        one(2 * pair + 1)
        return carry

    lax.fori_loop(0, out.shape[0] // REC2 // 2, serve, 0)


def fire_kernel(
    across,
    down,
    tables,
    flags,
    received,
    level,
    fuel_left,
    fuel_class,
    west_side,
    east_side,
    north,
    south,
    level_hbm,
    fuel_hbm,
    heat_out,
    level_out,
    fuel_out,
    cur_a,
    cur_b,
    base_rate,
    wind_rate,
    wind,
    strips,
    turned,
    tanh_sum,
    row_heat,
    sem,
):
    cur = (cur_a, cur_b)
    pos = position()
    lane = lanes()
    sub = lax.broadcasted_iota(i32, (8, LANES), 0)
    lane32 = lanes((32, LANES))

    def got(row, first=0, size=PIECES):
        return received[pl.ds(first * REC2 + row, size, stride=REC2), :]

    table_base, table_wind, table_burn, table_heat, table_emit = [tables[k] for k in range(5)]
    log2e = math.log2(math.e)

    turned[...] = jnp.zeros(turned.shape, f32)
    for q in range(2):
        for s in range(4):
            strips[0:32, :] = got(SIDE + q * 5 + s)
            strips[32:40, :] = got(SIDE + q * 5 + 4, 8 * opposite(s), 8)
            for number in range(2):
                low = strips[2 * SUB * number : 2 * SUB * number + SUB, :]
                high = strips[2 * SUB * number + SUB : 2 * SUB * (number + 1), :]
                if s < 2:
                    at = FIRST - SUB if s == 0 else FIRST + 256
                    target = cur[number]
                    target[3 * q, at : at + SUB, :] = low
                    target[3 * q + 1, at : at + SUB, :] = high
                else:
                    at = (54, 118)[q] if s == 2 else (0, 64)[q]
                    turned[number, at : at + SUB, :LANES] = low
                    turned[number, at : at + SUB, LANES:] = high
    for number in range(2):
        cur[number][2, FIRST : FIRST + 256, :] = turned[number].T
        corner = got(CORNER2, 16 * number, 16)
        cur[number][2, TOP : TOP + 16, :] = corner
        cur[number][2, FIRST + 256 : FIRST + 272, :] = jnp.where(
            lanes((16, LANES)) % 64 < 32, rolled(corner, -16), rolled(corner, 16)
        )
    for q in range(2):
        for half in range(2):
            cur_a[3 * q + half, FIRST : FIRST + 256, :] = level[q, :, LANES * half : LANES * (half + 1)]
            cur_b[3 * q + half, FIRST : FIRST + 256, :] = fuel_class[
                q, :, LANES * half : LANES * (half + 1)
            ].astype(f32)

    def rates(group, carry):
        for k in range(RATE_UNROLL):
            at = pl.multiple_of((1 + group * RATE_UNROLL + k) * 8, 8)
            for t in range(5):
                kind = cur_b[t, pl.ds(at, 8), :].astype(i32) & 127
                base_rate[t, pl.ds(at, 8), :] = pick(table_base, kind)
                wind_rate[t, pl.ds(at, 8), :] = pick(table_wind, kind)
        return carry

    lax.fori_loop(0, 36 // RATE_UNROLL, rates, 0)

    inner = lane % 64
    side_col = jnp.where(inner < 16, inner // 8, jnp.where(inner >= 48, 30 + (inner - 48) // 8, 0))
    for k in range(2):
        for t in range(5):
            for quarter in range(4):
                for outer in (0, 64):
                    if outer and quarter in (1, 2):
                        continue
                    at = outer + k * 32
                    if t == 2:
                        west = got(WINDB, 8 * quarter, 8)
                        east = got(WINDB + 1, 8 * quarter, 8)
                        index = side_col + at
                        value = jnp.where(lane < 64, pick(west, index), pick(east, index))
                    else:
                        source = got(WINDA + t // 3, 8 * quarter, 8)
                        value = pick(source, lane // 8 + (at + 16 * (t % 3)))
                    value = value * log2e
                    if not outer:
                        wind[k, t, 3 + 8 * quarter : 11 + 8 * quarter, :] = value
                    elif quarter == 3:
                        wind[k, t, 1:3, :] = value[6:8, :]
                    else:
                        wind[k, t, 35:37, :] = value[0:2, :]

    is0 = lane == 0
    is63 = lane == 63
    is64 = lane == 64
    is127 = lane == 127
    tanh_sum[...] = jnp.zeros(tanh_sum.shape, f32)

    def make_masks(region):
        return [flags[4 * region + k] > 0 for k in range(4)]

    def update(source, target, chunk, masks, rows_edge, main):
        lw0, le0, lw1, le1 = masks
        at = chunk * 8
        x = [source[t, pl.ds(at, 8), :] for t in range(5)]
        up = [source[t, pl.ds(at - 1, 8), :] for t in range(5)]
        dn = [source[t, pl.ds(at + 1, 8), :] for t in range(5)]
        if rows_edge is not None:
            kind, line, row = rows_edge
            for t in range(5):
                broken = (sub == row) & (flags[12 + 5 * line + t] == 0)
                if kind == "up":
                    up[t] = jnp.where(broken, x[t], up[t])
                else:
                    dn[t] = jnp.where(broken, x[t], dn[t])
        right = [rolled(v, 1) for v in x]
        left = [rolled(v, -1) for v in x]
        h = x[2]
        west = [
            jnp.where(is0, jnp.where(lw0, rolled(h, 65), x[0]), right[0]),
            jnp.where(is0, right[0], right[1]),
            jnp.where(
                is0,
                jnp.where(le0, right[1], h),
                jnp.where(is64, jnp.where(le1, rolled(x[4], 65), h), right[2]),
            ),
            jnp.where(is0, jnp.where(lw1, right[2], x[3]), right[3]),
            jnp.where(is0, right[3], right[4]),
        ]
        east = [
            jnp.where(is127, left[1], left[0]),
            jnp.where(is127, jnp.where(le0, left[2], x[1]), left[1]),
            jnp.where(
                is127,
                jnp.where(lw1, left[3], h),
                jnp.where(is63, jnp.where(lw0, rolled(x[0], 63), h), left[2]),
            ),
            jnp.where(is127, left[4], left[3]),
            jnp.where(is127, jnp.where(le1, rolled(h, -65), x[4]), left[4]),
        ]
        for t in range(5):
            diff_rows = dn[t] - up[t]
            diff_cols = east[t] - west[t]
            around = (dn[t] + up[t]) + (east[t] + west[t])
            square = diff_rows * diff_rows + (diff_cols * diff_cols + 4.0 * floor_square)
            inverse = lax.rsqrt(square)
            wind_r = wind[0, t, pl.ds(chunk, 1), :]
            wind_c = wind[1, t, pl.ds(chunk, 1), :]
            along = (wind_r * diff_rows + wind_c * diff_cols) * inverse
            soft = jnp.log(1.0 + jnp.exp2(along))
            power = soft * soft * lax.rsqrt(soft)
            b = base_rate[t, pl.ds(at, 8), :]
            w = wind_rate[t, pl.ds(at, 8), :]
            new = ((1.0 - 4.0 * smoothing) * x[t] + smoothing * around) - (b + w * power) * (
                square * inverse
            )
            target[t, pl.ds(at, 8), :] = new
            if main and t != 2:
                m = t - t // 3
                tanh_sum[m, pl.ds(at - FIRST, 8), :] += jnp.tanh(new)

    above = make_masks(0)
    within = make_masks(1)
    below = make_masks(2)

    def outer(source, target):
        update(source, target, 1, above, None, False)
        update(source, target, 36, below, None, False)

    def substep(source, target):
        update(source, target, 2, above, ("down", 0, 7), False)
        update(source, target, 3, within, ("up", 0, 0), True)

        def middle(group, carry):
            for k in range(UNROLL):
                update(source, target, 4 + group * UNROLL + k, within, None, True)
            return carry

        lax.fori_loop(0, 30 // UNROLL, middle, 0)
        update(source, target, 34, within, ("down", 1, 7), True)
        update(source, target, 35, below, ("up", 1, 0), False)

    def two_substeps(pair, carry):
        substep(cur_a, cur_b)
        substep(cur_b, cur_a)
        return carry

    outer(cur_a, cur_b)
    lax.fori_loop(0, SUB // 2, two_substeps, 0)

    last = SUB % 2

    def finish(chunk, burn, emit):
        at = pl.multiple_of(chunk * 8, 8)
        for q in range(2):
            for half in range(2):
                t = 3 * q + half
                cols = slice(LANES * half, LANES * (half + 1))
                final = cur[last][t, pl.ds(FIRST + at, 8), :]
                level_out[q, pl.ds(at, 8), cols] = final
                burn = burn + (0.5 - 0.5 * jnp.tanh(final))
                kind = fuel_class[q, pl.ds(at, 8), cols]
                fuel = fuel_left[q, pl.ds(at, 8), cols]
                power = pick(table_burn, kind) * (float(SUB) - tanh_sum[2 * q + half, pl.ds(at, 8), :])
                new_fuel = fuel * jnp.exp2(power)
                fuel_out[q, pl.ds(at, 8), cols] = new_fuel
                spent = fuel - new_fuel
                emit = emit + pick(table_emit, kind) * spent
                released = pick(table_heat, kind) * spent
                row_heat[2 * q + half, pl.ds(chunk, 1), :] = jnp.sum(released, axis=0, keepdims=True)
        return burn, emit

    blank = jnp.zeros((8, LANES), f32)
    sums = [blank] * 4

    def stores(group):
        rows = pl.ds(group * (8 * FINISH_UNROLL), 8 * FINISH_UNROLL)
        return [
            pltpu.make_async_copy(level_out.at[:, rows, :], level_hbm.at[:, rows, :], sem.at[0, group]),
            pltpu.make_async_copy(fuel_out.at[:, rows, :], fuel_hbm.at[:, rows, :], sem.at[1, group]),
        ]

    def finish_group(group, totals):
        totals = list(totals)
        for k in range(FINISH_UNROLL):
            pair = 2 * (k % 2)
            totals[pair], totals[pair + 1] = finish(
                group * FINISH_UNROLL + k, totals[pair], totals[pair + 1]
            )
        for copy in stores(group):
            copy.start()
        return tuple(totals)

    sums = lax.fori_loop(0, 32 // FINISH_UNROLL, finish_group, tuple(sums))
    burn = sums[0] + sums[2]
    emit = sums[1] + sums[3]
    devices = across * down

    def spread(row, value):
        heat_out[pl.ds(row, devices, stride=HEAT_ROWS), :] = jnp.broadcast_to(value, (devices, LANES))

    source_lane = lax.broadcasted_iota(i32, (LANES, LANES), 0) // REF
    target_lane = lanes((LANES, LANES))
    for q in range(2):
        packed = blank
        for g in range(4):
            for half in range(2):
                gather = jnp.where(
                    target_lane == 32 * g + 16 * half + source_lane, heating / (REF * REF), 0.0
                ).astype(f32)
                packed = packed + jnp.dot(
                    row_heat[2 * q + half, 8 * g : 8 * g + 8, :],
                    gather,
                    precision=lax.Precision.HIGHEST,
                    preferred_element_type=f32,
                )
        for row in range(8):
            spread(8 * q + row, packed[row : row + 1, :])
    burn_sum = jnp.sum(jnp.sum(burn, axis=0, keepdims=True), axis=1, keepdims=True)
    emit_sum = jnp.sum(jnp.sum(emit, axis=0, keepdims=True), axis=1, keepdims=True)
    lane1 = lanes((1, LANES))
    spread(16, jnp.where(lane1 == 0, burn_sum, jnp.where(lane1 == 1, emit_sum, 0.0)))
    for group in range(32 // FINISH_UNROLL):
        for copy in stores(group):
            copy.wait()


def air_kernel(north, south, west_side, east_side, air_hbm, air_out, surface, air, fresh, sides, sem_in, sem_out):
    def load(number):
        return pltpu.make_async_copy(
            air_hbm.at[:, number], air.at[:, number + 1, 8:136, :], sem_in.at[number]
        )

    def store(number):
        return pltpu.make_async_copy(fresh.at[:, number], air_out.at[:, number], sem_out.at[number])

    levels = 16
    for number in range(levels):
        load(number).start()
    lane = lanes()
    is0 = lane == 0
    is127 = lane == 127
    zero = jnp.zeros((128, LANES), f32)
    for f in range(3):
        air[f, 0, 8:136, :] = zero
        air[f, levels + 1, 8:136, :] = zero
    for plane in range(48):
        at = (plane // 16, plane % 16 + 1)
        air[at[0], at[1], 7:8, :] = north[plane : plane + 1, :]
        air[at[0], at[1], 136:137, :] = south[plane : plane + 1, :]
    sides[...] = jnp.where(lanes((128, LANES)) % 2 == 1, east_side[...], west_side[...])

    load(0).wait()

    def air_level(number, carry):
        @pl.when(number < levels - 1)
        def _():
            load(number + 1).wait()

        def air_rows(group, inner_carry):
            for k in range(AIR_UNROLL):
                row = group * (8 * AIR_UNROLL) + k * 8
                at = 8 + row
                halo = sides[pl.ds(row, 8), :]
                x = [air[f, number + 1, pl.ds(at, 8), :] for f in range(3)]
                for f in range(3):
                    up = air[f, number + 1, pl.ds(at - 1, 8), :]
                    dn = air[f, number + 1, pl.ds(at + 1, 8), :]
                    over = air[f, number + 2, pl.ds(at, 8), :]
                    under = air[f, number, pl.ds(at, 8), :]
                    mine = pltpu.roll(halo, LANES - 1 - 2 * (f * 16 + number), 1)
                    west = rolled(jnp.where(is127, mine, x[f]), 1)
                    east = rolled(jnp.where(is0, mine, x[f]), -1)
                    around = (up + dn) + (west + east)
                    advect = x[0] * (dn - up) + x[1] * (east - west)
                    fresh[f, number, pl.ds(row, 8), :] = (
                        (1.0 - 4.0 * viscosity - 2.0 * mixing) * x[f]
                        + viscosity * around
                        - (0.5 * courant) * advect
                        + mixing * (over + under)
                    )
            return inner_carry

        lax.fori_loop(0, 16 // AIR_UNROLL, air_rows, 0)
        store(number).start()
        return carry

    lax.fori_loop(0, levels, air_level, 0)

    surface[...] = fresh[2, 0]

    def drain(number, carry):
        store(number).wait()
        return carry

    lax.fori_loop(0, levels, drain, 0)


def heat_kernel(cells, blocks, index, gathered, plane, air_in, air_out, totals, warm, sem):
    pos = position()
    tile_rows = 128 // BA
    lane = lanes()
    warm[...] = plane[...]
    for slot in range(4):
        j = index[WORDS, slot] - 1

        @pl.when(j >= 0)
        def _():
            row = blocks[0, j] - pos[0] * tile_rows
            col = blocks[1, j] - pos[1] * tile_rows
            heat = gathered[pl.ds((j // 2) * HEAT_ROWS + 8 * (j % 2), 8), :]
            for g in range(4):
                moved = pltpu.roll(heat, (col - g + 4) * BA % LANES, 1)
                at = pl.multiple_of(row * BA + 8 * g, 8)
                warm[pl.ds(at, 8), :] += jnp.where(lane // BA == col, moved, 0.0)

    store = pltpu.make_async_copy(warm, air_out.at[2, 0], sem)
    store.start()
    devices = gathered.shape[0] // HEAT_ROWS
    sums = jnp.sum(gathered[pl.ds(16, devices, stride=HEAT_ROWS), :], axis=0, keepdims=True)
    lane1 = lanes((1, LANES))
    for k in range(2):
        totals[k] = jnp.sum(jnp.where(lane1 == k, sums, 0.0)) * (1.0 / cells)
    store.wait()


def local(air_state, level_set, fuel_left, fuel_class, fuel_props, blocks, adjacency):
    down = lax.axis_size("gx")
    across = lax.axis_size("gy")
    devices = down * across
    both = ("gx", "gy")
    smem = pl.BlockSpec(memory_space=pltpu.SMEM)
    vmem = pl.BlockSpec(memory_space=pltpu.VMEM)
    anywhere = pl.BlockSpec(memory_space=pl.ANY)
    blocks = blocks.T
    adjacency = adjacency.T
    packed = pl.pallas_call(
        pack_kernel,
        out_shape=pltpu.VMEM((devices * REC1, LANES), f32),
        in_specs=[smem, anywhere, anywhere, anywhere],
        out_specs=vmem,
        scratch_shapes=[
            pltpu.VMEM(level_set.shape, f32),
            pltpu.VMEM(level_set.shape, i32),
            pltpu.VMEM((2, 128, LANES), f32),
            pltpu.VMEM((4, 40, LANES), f32),
            pltpu.SMEM((8,), i32),
            pltpu.SemaphoreType.DMA((3,)),
        ],
        name="pack",
    )(blocks, level_set, fuel_class, air_state)
    relayed = lax.all_to_all(packed.reshape(devices, REC1, LANES), both, 0, 0)
    lanes_used = -(-blocks.shape[1] // LANES) * LANES
    index, tables, flags = pl.pallas_call(
        lambda *refs: index_kernel(across, *refs),
        out_shape=(
            jax.ShapeDtypeStruct((WORDS + 1, lanes_used), i32),
            pltpu.VMEM((5, 8, LANES), f32),
            pltpu.VMEM((22, 8, LANES), i32),
        ),
        in_specs=[vmem, vmem, smem, smem],
        out_specs=(vmem, vmem, vmem),
        scratch_shapes=[pltpu.VMEM((16, lanes_used), i32)],
        cost_estimate=pl.CostEstimate(flops=20_000_000, transcendentals=0, bytes_accessed=10_000),
        name="index",
    )(blocks, adjacency, adjacency, fuel_props)
    first_rows, last_rows, columns = pl.pallas_call(
        edge_kernel,
        out_shape=(
            pltpu.VMEM((48, LANES), f32),
            pltpu.VMEM((48, LANES), f32),
            pltpu.VMEM((128, LANES), f32),
        ),
        in_specs=[anywhere, anywhere],
        out_specs=(vmem, vmem, vmem),
        scratch_shapes=[pltpu.VMEM((48 * 128, LANES), f32), pltpu.SemaphoreType.DMA(())],
        cost_estimate=pl.CostEstimate(flops=30_000_000, transcendentals=0, bytes_accessed=3_200_000),
        name="edge",
    )(air_state.reshape(48 * 128, LANES), index)
    north = near(lax.ppermute(last_rows, "gx", [(k, k + 1) for k in range(down - 1)]))
    south = near(lax.ppermute(first_rows, "gx", [(k + 1, k) for k in range(down - 1)]))
    chosen = pl.pallas_call(
        select_kernel,
        out_shape=pltpu.VMEM((devices * REC2, LANES), f32),
        in_specs=[smem, vmem],
        out_specs=vmem,
        name="select",
    )(index, near(relayed.reshape(devices * REC1, LANES)))
    columns, chosen = lax.optimization_barrier((columns, chosen))
    west_side = near(lax.ppermute(columns, "gy", [(k, k + 1) for k in range(across - 1)]))
    east_side = near(lax.ppermute(columns, "gy", [(k + 1, k) for k in range(across - 1)]))
    received = lax.all_to_all(chosen.reshape(devices, REC2, LANES), both, 0, 0)
    received = received.reshape(devices * REC2, LANES)[: PIECES * REC2]
    received = near(received)
    level_next, fuel_next, heat = pl.pallas_call(
        lambda *refs: fire_kernel(across, down, *refs),
        out_shape=(
            jax.ShapeDtypeStruct(level_set.shape, f32),
            jax.ShapeDtypeStruct(level_set.shape, f32),
            pltpu.VMEM((devices * HEAT_ROWS, LANES), f32),
        ),
        in_specs=[vmem] * 10,
        out_specs=(anywhere, anywhere, vmem),
        scratch_shapes=[
            pltpu.VMEM(level_set.shape, f32),
            pltpu.VMEM(level_set.shape, f32),
            pltpu.VMEM((5, EXT, LANES), f32),
            pltpu.VMEM((5, EXT, LANES), f32),
            pltpu.VMEM((5, EXT, LANES), f32),
            pltpu.VMEM((5, EXT, LANES), f32),
            pltpu.VMEM((2, 5, 40, LANES), f32),
            pltpu.VMEM((40, LANES), f32),
            pltpu.VMEM((2, LANES, 256), f32),
            pltpu.VMEM((4, 256, LANES), f32),
            pltpu.VMEM((4, 32, LANES), f32),
            pltpu.SemaphoreType.DMA((2, 32 // FINISH_UNROLL)),
        ],
        name="fire",
    )(
        near(tables),
        near(flags),
        received,
        near(level_set),
        near(fuel_left),
        near(fuel_class),
        west_side,
        east_side,
        north,
        south,
    )
    gathered = lax.all_to_all(heat.reshape(devices, 1, HEAT_ROWS * LANES), both, 0, 0)
    gathered = near(gathered.reshape(devices * HEAT_ROWS, LANES))
    air_next, plane = pl.pallas_call(
        air_kernel,
        out_shape=(jax.ShapeDtypeStruct(air_state.shape, f32), pltpu.VMEM((128, LANES), f32)),
        in_specs=[vmem, vmem, vmem, vmem, anywhere],
        out_specs=(anywhere, vmem),
        scratch_shapes=[
            pltpu.VMEM((3, 18, 144, LANES), f32),
            pltpu.VMEM((3, 16, 128, LANES), f32),
            pltpu.VMEM((128, LANES), f32),
            pltpu.SemaphoreType.DMA((16,)),
            pltpu.SemaphoreType.DMA((16,)),
        ],
        cost_estimate=pl.CostEstimate(flops=80_000_000, transcendentals=0, bytes_accessed=6_300_000),
        name="air",
    )(north, south, west_side, east_side, air_state)
    cells = blocks.shape[1] * level_set.shape[1] * level_set.shape[2]
    air_next, totals = pl.pallas_call(
        lambda *refs: heat_kernel(cells, *refs),
        out_shape=(jax.ShapeDtypeStruct(air_state.shape, f32), jax.ShapeDtypeStruct((2,), f32)),
        in_specs=[smem, smem, vmem, vmem, anywhere],
        out_specs=(anywhere, smem),
        scratch_shapes=[pltpu.VMEM((128, LANES), f32), pltpu.SemaphoreType.DMA(())],
        input_output_aliases={4: 0},
        name="heat",
    )(blocks, index, gathered, near(plane), air_next)
    return (air_next, level_next, fuel_next, totals)


def near(x):
    return pltpu.with_memory_space_constraint(x, pltpu.VMEM)


def solution(mesh):
    in_specs = (
        P(None, None, "gx", "gy"),
        P(("gx", "gy"), None, None),
        P(("gx", "gy"), None, None),
        P(("gx", "gy"), None, None),
        P(),
        P(),
        P(),
    )
    out_specs = (
        P(None, None, "gx", "gy"),
        P(("gx", "gy"), None, None),
        P(("gx", "gy"), None, None),
        P(),
    )
    return jax.shard_map(local, mesh=mesh, in_specs=in_specs, out_specs=out_specs, check_vma=False)
```

```python
import math

import jax
import jax.numpy as jnp
from jax import lax
from jax.experimental import pallas as pl
from jax.experimental.pallas import tpu as pltpu
from jax.sharding import PartitionSpec as P


REF = 8
BA = 32
SUB = 10
PIECES = 32
LANES = 128
UNROLL = 30
RATE_UNROLL = 12
FINISH_UNROLL = 16
AIR_UNROLL = 16
EDGE_UNROLL = 2

step_time = 0.25
smoothing = 0.15
floor_square = 0.25
viscosity = 0.1
courant = 0.25
mixing = 0.1
heating = 2.0

SIDE = 0
CORNER = 10
WIND = 12
REC1 = 16
CORNER2 = 10
WINDA = 11
WINDB = 13
REC2 = 16
HEAT_ROWS = 17

TOP = 8
EXT = 304
FIRST = 24

f32 = jnp.float32
i32 = jnp.int32


def lanes(shape=(8, LANES)):
    return lax.broadcasted_iota(i32, shape, len(shape) - 1)


def rolled(x, shift):
    return pltpu.roll(x, shift % LANES, x.ndim - 1)


def opposite(side):
    return (1, 0, 3, 2)[side]


def pick(table, index):
    return jnp.take_along_axis(table, index, axis=1, mode="promise_in_bounds")


def position():
    return lax.axis_index("gx"), lax.axis_index("gy")


def pack_kernel(blocks, level_hbm, class_hbm, air_hbm, out, level, fuel_class, air, strip, mine, sem):
    loads = [
        pltpu.make_async_copy(level_hbm, level, sem.at[0]),
        pltpu.make_async_copy(class_hbm, fuel_class, sem.at[1]),
        pltpu.make_async_copy(air_hbm.at[0:2, 0], air, sem.at[2]),
    ]
    for load in loads:
        load.start()
    pos = position()
    tile_rows = 128 // BA
    for slot in range(4):
        mine[slot] = -1

    def find(j, count):
        row = blocks[0, j] - pos[0] * tile_rows
        col = blocks[1, j] - pos[1] * tile_rows
        inside = (row >= 0) & (row < tile_rows) & (col >= 0) & (col < tile_rows)

        @pl.when(inside)
        def _():
            mine[count] = row * tile_rows + col

        return count + inside.astype(i32)

    lax.fori_loop(0, blocks.shape[1], find, jnp.int32(0))
    loads[0].wait()
    loads[1].wait()
    lane256 = lanes((256, LANES))
    lane16 = lanes((16, LANES))

    def place(row, first, values):
        out[pl.ds(first * REC1 + row, values.shape[0], stride=REC1), :] = values

    for q in range(2):
        fields = (level[q], fuel_class[q].astype(f32))
        turned = [
            jnp.where(lane256 < 64, field[:, :LANES], field[:, LANES:]).T for field in fields
        ]
        for side in range(4):
            for number, (field, turn) in enumerate(zip(fields, turned)):
                if side == 0:
                    rows = field[0:SUB, :]
                elif side == 1:
                    rows = field[256 - SUB : 256, :]
                elif side == 2:
                    rows = turn[0:SUB, :]
                else:
                    rows = turn[LANES - SUB : LANES, :]
                strip[side, 2 * SUB * number : 2 * SUB * number + SUB, :] = rows[:, :LANES]
                strip[side, 2 * SUB * number + SUB : 2 * SUB * (number + 1), :] = rows[:, LANES:]
            place(SIDE + q * 5 + side, 0, strip[side, 0:32, :])
            place(SIDE + q * 5 + 4, 8 * side, strip[side, 32:40, :])
        for number, field in enumerate(fields):
            half = jnp.where(
                lane16 < 16,
                field[240:256, :LANES],
                jnp.where(
                    lane16 < 32,
                    rolled(field[0:16, :LANES], 16),
                    jnp.where(
                        lane16 < 48,
                        rolled(field[0:16, LANES:], 48),
                        rolled(field[240:256, LANES:], 64),
                    ),
                ),
            )
            place(CORNER + q, 16 * number, jnp.where(lane16 < 64, half, rolled(half, 64)))

    loads[2].wait()
    lane32 = lanes((32, LANES))
    for slot in range(4):
        at = jnp.maximum(mine[slot], 0)
        start = pl.multiple_of((at // tile_rows) * BA, BA)
        shift = LANES - (at % tile_rows) * BA
        u = pltpu.roll(air[0, pl.ds(start, BA), :], shift, 1)
        v = pltpu.roll(air[1, pl.ds(start, BA), :], shift, 1)
        half = jnp.where(lane32 < 32, u, rolled(v, 32))
        place(WIND + slot, 0, jnp.where(lane32 < 64, half, rolled(half, 64)))
    if out.shape[0] > PIECES * REC1:
        out[PIECES * REC1 :, :] = jnp.zeros((out.shape[0] - PIECES * REC1, LANES), f32)


WORDS = 15


def edge_kernel(air_hbm, ready, first_rows, last_rows, columns, air, sem):
    load = pltpu.make_async_copy(air_hbm, air, sem)
    load.start()
    load.wait()
    first_rows[...] = air[pl.ds(0, 48, stride=128), :]
    last_rows[...] = air[pl.ds(127, 48, stride=128), :]
    lane = lanes()

    def gather(group, carry):
        for k in range(EDGE_UNROLL):
            base = pl.multiple_of((group * EDGE_UNROLL + k) * 8, 8)
            total = jnp.zeros((8, LANES), f32)
            for plane in range(48):
                x = air[pl.ds(plane * 128 + base, 8), :]
                total = jnp.where(lane // 2 == plane, rolled(x, 1 + 2 * plane), total)
            columns[pl.ds(base, 8), :] = total
        return carry

    lax.fori_loop(0, 16 // EDGE_UNROLL, gather, 0)


def index_kernel(across, blocks, adjacency, near_own, props, out, tables, flags, padded):
    pos = position()
    total = blocks.shape[1]
    tiles = out.shape[1] // LANES
    relay = jnp.minimum(pos[0] * across + pos[1], PIECES - 1)
    padded[...] = jnp.zeros(padded.shape, i32)
    padded[0:2, 0:total] = blocks[...]
    padded[8:12, 0:total] = adjacency[...]

    def row(number):
        return [
            jnp.broadcast_to(padded[number : number + 1, LANES * u : LANES * (u + 1)], (8, LANES))
            for u in range(tiles)
        ]

    def lookup(table, index):
        found = []
        for u in range(tiles):
            value = pick(table[0], index[u] & (LANES - 1))
            for v in range(1, tiles):
                value = jnp.where(index[u] >> 7 == v, pick(table[v], index[u] & (LANES - 1)), value)
            found.append(value)
        return found

    def each(f, *rows):
        return [f(*values) for values in zip(*rows)]

    lane = lanes()
    tile_of = each(lambda r, c: (r >> 2) * across + (c >> 2), row(0), row(1))
    before = lax.broadcasted_iota(i32, (LANES, LANES), 0)
    here = lanes((LANES, LANES))
    as_rows = [jnp.broadcast_to(t[0:1, :].astype(f32), (LANES, LANES)) for t in tile_of]
    as_cols = [t.T for t in as_rows]
    wind_row = []
    placed = [jnp.zeros((8, 1), f32)] * 4
    own = (pos[0] * across + pos[1]).astype(f32)
    lane = lanes()
    for u in range(tiles):
        slot = jnp.zeros((1, LANES), f32)
        for v in range(u + 1):
            same = (as_cols[v] == as_rows[u]) & (before + LANES * v < here + LANES * u)
            slot = slot + jnp.sum(jnp.where(same, 1.0, 0.0), axis=0, keepdims=True)
        number = (lane + (LANES * u + 1)).astype(f32)
        own_tile = (jnp.broadcast_to(as_rows[u][0:1, :], (8, LANES)) == own) & (number <= total)
        for c in range(4):
            at_slot = own_tile & (jnp.broadcast_to(slot, (8, LANES)) == c)
            placed[c] = placed[c] + jnp.sum(jnp.where(at_slot, number, 0.0), axis=1, keepdims=True)
        wind_row.append(tile_of[u] * REC1 + WIND + jnp.broadcast_to(slot.astype(i32), (8, LANES)))
    near = [row(8 + s) for s in range(4)]
    safe = [each(lambda n: jnp.maximum(n, 0), near[s]) for s in range(4)]

    def diagonal(s, t):
        by_row = lookup(near[t], safe[s])
        by_col = lookup(near[s], safe[t])
        return each(
            lambda n, m, r, c: jnp.maximum(jnp.where(n >= 0, r, jnp.where(m >= 0, c, 0)), 0),
            near[s],
            near[t],
            by_row,
            by_col,
        )

    nw, ne, sw, se = diagonal(0, 2), diagonal(0, 3), diagonal(1, 2), diagonal(1, 3)
    spare_side = relay >> 3
    upper = relay >= 16

    def side_row(j, s):
        return each(lambda b: (b >> 1) * REC1 + SIDE + (b & 1) * 5 + s, j)

    def choose(flag, yes, no):
        return each(lambda a, b: jnp.where(flag, a, b), yes, no)

    words = [side_row(safe[s], opposite(s)) for s in range(4)]
    spare = choose(
        spare_side == 0,
        safe[1],
        choose(spare_side == 1, safe[0], choose(spare_side == 2, safe[3], safe[2])),
    )
    words.append(side_row(spare, 4))
    for j in (ne, se, sw, nw):
        words.append(each(lambda b: (b >> 1) * REC1 + CORNER + (b & 1), j))
    words.append(wind_row)
    for j in (
        choose(upper, safe[0], safe[1]),
        safe[3],
        safe[2],
        choose(upper, ne, se),
        choose(upper, nw, sw),
    ):
        words.append(lookup(wind_row, j))
    for number, word in enumerate(words):
        for u in range(tiles):
            out[number : number + 1, LANES * u : LANES * (u + 1)] = word[u][0:1, :]
    device = pos[0] * across + pos[1]

    def table(value):
        row = jnp.zeros((8, LANES), f32)
        for kind in range(props.shape[1]):
            row = jnp.where(lane == kind, value(kind), row)
        return row

    log2e = math.log2(math.e)
    table_base = table(lambda c: 0.125 * 0.3 * props[0, c])
    table_wind = table_base * table(lambda c: 0.3 * props[1, c])
    table_burn = (-0.5 * step_time * log2e / 4.0) / jnp.where(
        lane < props.shape[1], table(lambda c: props[2, c]), 1.0
    )
    table_heat = table(lambda c: props[3, c])
    table_emit = table(lambda c: 3.0 * props[4, c])
    for k, values in enumerate((table_base, table_wind, table_burn, table_heat, table_emit)):
        tables[k] = values

    def there(j):
        return j >= 0

    across_links = []
    groups = []
    for q in range(2):
        i = 2 * device + q
        near = [near_own[s, i] for s in range(4)]
        safe = [jnp.maximum(near[s], 0) for s in range(4)]

        def joined(s, t):
            return there(near[s]) & there(near_own[t, safe[s]])

        groups.append([(there(near[s]), joined(2, s), joined(3, s)) for s in range(2)])
        across_links.append([[joined(0, t), there(near[t]), joined(1, t)] for t in (2, 3)])

    def as_int(flag):
        return jnp.where(flag, 1, 0)

    for line in range(2):
        for q in range(2):
            mid, _, _ = groups[q][line]
            row = jnp.broadcast_to(as_int(mid), (8, LANES))
            flags[12 + 5 * line + 3 * q] = row
            flags[12 + 5 * line + 3 * q + 1] = row
        w0, e0 = groups[0][line][1:]
        w1, e1 = groups[1][line][1:]
        flags[12 + 5 * line + 2] = jnp.where(
            lane < 32,
            as_int(e0),
            jnp.where(lane < 64, as_int(w0), jnp.where(lane < 96, as_int(e1), as_int(w1))),
        )

    for region in range(3):
        for k in range(4):
            flag = as_int(across_links[k // 2][k % 2][region])
            flags[4 * region + k] = jnp.broadcast_to(flag, (8, LANES))
    listed = jnp.zeros((8, LANES), f32)
    for c in range(4):
        listed = jnp.where(lane == c, placed[c], listed)
    out[WORDS : WORDS + 1, 0:LANES] = listed[0:1, :].astype(i32)
    if tiles > 1:
        out[WORDS : WORDS + 1, LANES:] = jnp.zeros((1, out.shape[1] - LANES), i32)


def select_kernel(index, received, out):
    lane1 = lanes((1, LANES))
    lane_col = lane1 % 32 < 16
    first_half = lane1 < 64
    quarter = lane1 // 16

    def one(d):
        def take(word, q):
            return received[pl.ds(index[word, 2 * d + q], 1), :]

        def put(row, value):
            out[pl.ds(d * REC2 + row, 1), :] = value

        for row in range(10):
            put(SIDE + row, take(row % 5, row // 5))
        merged = take(8, 1)
        for k in range(7):
            merged = jnp.where(quarter == k, take(5 + k % 4, k // 4), merged)
        put(CORNER2, merged)
        for q in range(2):
            own, beyond, east, west, corner_east, corner_west = [take(9 + k, q) for k in range(6)]
            put(WINDA + q, jnp.where(first_half, own, beyond))
            put(
                WINDB + q,
                jnp.where(
                    lane_col,
                    jnp.where(first_half, east, corner_east),
                    jnp.where(first_half, west, corner_west),
                ),
            )
        put(REC2 - 1, jnp.zeros((1, LANES), f32))

    def serve(pair, carry):
        one(2 * pair)
        one(2 * pair + 1)
        return carry

    lax.fori_loop(0, out.shape[0] // REC2 // 2, serve, 0)


def fire_kernel(
    across,
    down,
    tables,
    flags,
    received,
    level,
    fuel_left,
    fuel_class,
    west_side,
    east_side,
    north,
    south,
    level_hbm,
    fuel_hbm,
    heat_out,
    level_out,
    fuel_out,
    cur_a,
    cur_b,
    base_rate,
    wind_rate,
    wind,
    strips,
    turned,
    tanh_sum,
    row_heat,
    sem,
):
    cur = (cur_a, cur_b)
    lane = lanes()
    sub = lax.broadcasted_iota(i32, (8, LANES), 0)
    lane32 = lanes((32, LANES))

    def got(row, first=0, size=PIECES):
        return received[pl.ds(first * REC2 + row, size, stride=REC2), :]

    table_base, table_wind, table_burn, table_heat, table_emit = [tables[k] for k in range(5)]
    log2e = math.log2(math.e)

    turned[...] = jnp.zeros(turned.shape, f32)
    for q in range(2):
        for s in range(4):
            strips[0:32, :] = got(SIDE + q * 5 + s)
            strips[32:40, :] = got(SIDE + q * 5 + 4, 8 * opposite(s), 8)
            for number in range(2):
                low = strips[2 * SUB * number : 2 * SUB * number + SUB, :]
                high = strips[2 * SUB * number + SUB : 2 * SUB * (number + 1), :]
                if s < 2:
                    at = FIRST - SUB if s == 0 else FIRST + 256
                    target = cur[number]
                    target[3 * q, at : at + SUB, :] = low
                    target[3 * q + 1, at : at + SUB, :] = high
                else:
                    at = (54, 118)[q] if s == 2 else (0, 64)[q]
                    turned[number, at : at + SUB, :LANES] = low
                    turned[number, at : at + SUB, LANES:] = high
    for number in range(2):
        cur[number][2, FIRST : FIRST + 256, :] = turned[number].T
        corner = got(CORNER2, 16 * number, 16)
        cur[number][2, TOP : TOP + 16, :] = corner
        cur[number][2, FIRST + 256 : FIRST + 272, :] = jnp.where(
            lanes((16, LANES)) % 64 < 32, rolled(corner, -16), rolled(corner, 16)
        )
    for q in range(2):
        for half in range(2):
            cur_a[3 * q + half, FIRST : FIRST + 256, :] = level[q, :, LANES * half : LANES * (half + 1)]
            cur_b[3 * q + half, FIRST : FIRST + 256, :] = fuel_class[
                q, :, LANES * half : LANES * (half + 1)
            ].astype(f32)

    def rates(group, carry):
        for k in range(RATE_UNROLL):
            at = pl.multiple_of((1 + group * RATE_UNROLL + k) * 8, 8)
            for t in range(5):
                kind = cur_b[t, pl.ds(at, 8), :].astype(i32) & 127
                base_rate[t, pl.ds(at, 8), :] = pick(table_base, kind)
                wind_rate[t, pl.ds(at, 8), :] = pick(table_wind, kind)
        return carry

    lax.fori_loop(0, 36 // RATE_UNROLL, rates, 0)

    inner = lane % 64
    side_col = jnp.where(inner < 16, inner // 8, jnp.where(inner >= 48, 30 + (inner - 48) // 8, 0))
    for k in range(2):
        for t in range(5):
            for quarter in range(4):
                for outer in (0, 64):
                    if outer and quarter in (1, 2):
                        continue
                    at = outer + k * 32
                    if t == 2:
                        west = got(WINDB, 8 * quarter, 8)
                        east = got(WINDB + 1, 8 * quarter, 8)
                        index = side_col + at
                        value = jnp.where(lane < 64, pick(west, index), pick(east, index))
                    else:
                        source = got(WINDA + t // 3, 8 * quarter, 8)
                        value = pick(source, lane // 8 + (at + 16 * (t % 3)))
                    value = value * log2e
                    if not outer:
                        wind[k, t, 3 + 8 * quarter : 11 + 8 * quarter, :] = value
                    elif quarter == 3:
                        wind[k, t, 1:3, :] = value[6:8, :]
                    else:
                        wind[k, t, 35:37, :] = value[0:2, :]

    is0 = lane == 0
    is63 = lane == 63
    is64 = lane == 64
    is127 = lane == 127
    tanh_sum[...] = jnp.zeros(tanh_sum.shape, f32)

    def make_masks(region):
        return [flags[4 * region + k] > 0 for k in range(4)]

    def update(source, target, chunk, masks, rows_edge, main):
        lw0, le0, lw1, le1 = masks
        at = chunk * 8
        x = [source[t, pl.ds(at, 8), :] for t in range(5)]
        up = [source[t, pl.ds(at - 1, 8), :] for t in range(5)]
        dn = [source[t, pl.ds(at + 1, 8), :] for t in range(5)]
        if rows_edge is not None:
            kind, line, row = rows_edge
            for t in range(5):
                broken = (sub == row) & (flags[12 + 5 * line + t] == 0)
                if kind == "up":
                    up[t] = jnp.where(broken, x[t], up[t])
                else:
                    dn[t] = jnp.where(broken, x[t], dn[t])
        right = [rolled(v, 1) for v in x]
        left = [rolled(v, -1) for v in x]
        h = x[2]
        west = [
            jnp.where(is0, jnp.where(lw0, rolled(h, 65), x[0]), right[0]),
            jnp.where(is0, right[0], right[1]),
            jnp.where(
                is0,
                jnp.where(le0, right[1], h),
                jnp.where(is64, jnp.where(le1, rolled(x[4], 65), h), right[2]),
            ),
            jnp.where(is0, jnp.where(lw1, right[2], x[3]), right[3]),
            jnp.where(is0, right[3], right[4]),
        ]
        east = [
            jnp.where(is127, left[1], left[0]),
            jnp.where(is127, jnp.where(le0, left[2], x[1]), left[1]),
            jnp.where(
                is127,
                jnp.where(lw1, left[3], h),
                jnp.where(is63, jnp.where(lw0, rolled(x[0], 63), h), left[2]),
            ),
            jnp.where(is127, left[4], left[3]),
            jnp.where(is127, jnp.where(le1, rolled(h, -65), x[4]), left[4]),
        ]
        for t in range(5):
            diff_rows = dn[t] - up[t]
            diff_cols = east[t] - west[t]
            around = (dn[t] + up[t]) + (east[t] + west[t])
            square = diff_rows * diff_rows + (diff_cols * diff_cols + 4.0 * floor_square)
            inverse = lax.rsqrt(square)
            wind_r = wind[0, t, pl.ds(chunk, 1), :]
            wind_c = wind[1, t, pl.ds(chunk, 1), :]
            along = (wind_r * diff_rows + wind_c * diff_cols) * inverse
            soft = jnp.log(1.0 + jnp.exp2(along))
            power = soft * soft * lax.rsqrt(soft)
            b = base_rate[t, pl.ds(at, 8), :]
            w = wind_rate[t, pl.ds(at, 8), :]
            new = ((1.0 - 4.0 * smoothing) * x[t] + smoothing * around) - (b + w * power) * (
                square * inverse
            )
            target[t, pl.ds(at, 8), :] = new
            if main and t != 2:
                m = t - t // 3
                tanh_sum[m, pl.ds(at - FIRST, 8), :] += jnp.tanh(new)

    above = make_masks(0)
    within = make_masks(1)
    below = make_masks(2)

    def outer(source, target):
        update(source, target, 1, above, None, False)
        update(source, target, 36, below, None, False)

    def substep(source, target):
        update(source, target, 2, above, ("down", 0, 7), False)
        update(source, target, 3, within, ("up", 0, 0), True)

        def middle(group, carry):
            for k in range(UNROLL):
                update(source, target, 4 + group * UNROLL + k, within, None, True)
            return carry

        lax.fori_loop(0, 30 // UNROLL, middle, 0)
        update(source, target, 34, within, ("down", 1, 7), True)
        update(source, target, 35, below, ("up", 1, 0), False)

    def two_substeps(pair, carry):
        substep(cur_a, cur_b)
        substep(cur_b, cur_a)
        return carry

    outer(cur_a, cur_b)
    lax.fori_loop(0, SUB // 2, two_substeps, 0)

    last = SUB % 2

    def finish(chunk, burn, emit):
        at = pl.multiple_of(chunk * 8, 8)
        for q in range(2):
            for half in range(2):
                t = 3 * q + half
                cols = slice(LANES * half, LANES * (half + 1))
                final = cur[last][t, pl.ds(FIRST + at, 8), :]
                level_out[q, pl.ds(at, 8), cols] = final
                burn = burn + (0.5 - 0.5 * jnp.tanh(final))
                kind = fuel_class[q, pl.ds(at, 8), cols]
                fuel = fuel_left[q, pl.ds(at, 8), cols]
                power = pick(table_burn, kind) * (float(SUB) - tanh_sum[2 * q + half, pl.ds(at, 8), :])
                new_fuel = fuel * jnp.exp2(power)
                fuel_out[q, pl.ds(at, 8), cols] = new_fuel
                spent = fuel - new_fuel
                emit = emit + pick(table_emit, kind) * spent
                released = pick(table_heat, kind) * spent
                row_heat[2 * q + half, pl.ds(chunk, 1), :] = jnp.sum(released, axis=0, keepdims=True)
        return burn, emit

    blank = jnp.zeros((8, LANES), f32)
    sums = [blank] * 4

    def stores(group):
        rows = pl.ds(group * (8 * FINISH_UNROLL), 8 * FINISH_UNROLL)
        return [
            pltpu.make_async_copy(level_out.at[:, rows, :], level_hbm.at[:, rows, :], sem.at[0, group]),
            pltpu.make_async_copy(fuel_out.at[:, rows, :], fuel_hbm.at[:, rows, :], sem.at[1, group]),
        ]

    def finish_group(group, totals):
        totals = list(totals)
        for k in range(FINISH_UNROLL):
            pair = 2 * (k % 2)
            totals[pair], totals[pair + 1] = finish(
                group * FINISH_UNROLL + k, totals[pair], totals[pair + 1]
            )
        for copy in stores(group):
            copy.start()
        return tuple(totals)

    sums = lax.fori_loop(0, 32 // FINISH_UNROLL, finish_group, tuple(sums))
    burn = sums[0] + sums[2]
    emit = sums[1] + sums[3]
    devices = across * down

    def spread(row, value):
        heat_out[pl.ds(row, devices, stride=HEAT_ROWS), :] = jnp.broadcast_to(value, (devices, LANES))

    source_lane = lax.broadcasted_iota(i32, (LANES, LANES), 0) // REF
    target_lane = lanes((LANES, LANES))
    for q in range(2):
        packed = blank
        for g in range(4):
            for half in range(2):
                gather = jnp.where(
                    target_lane == 32 * g + 16 * half + source_lane, heating / (REF * REF), 0.0
                ).astype(f32)
                packed = packed + jnp.dot(
                    row_heat[2 * q + half, 8 * g : 8 * g + 8, :],
                    gather,
                    precision=lax.Precision.HIGHEST,
                    preferred_element_type=f32,
                )
        for row in range(8):
            spread(8 * q + row, packed[row : row + 1, :])
    burn_sum = jnp.sum(jnp.sum(burn, axis=0, keepdims=True), axis=1, keepdims=True)
    emit_sum = jnp.sum(jnp.sum(emit, axis=0, keepdims=True), axis=1, keepdims=True)
    lane1 = lanes((1, LANES))
    spread(16, jnp.where(lane1 == 0, burn_sum, jnp.where(lane1 == 1, emit_sum, 0.0)))
    for group in range(32 // FINISH_UNROLL):
        for copy in stores(group):
            copy.wait()


def air_kernel(north, south, west_side, east_side, air_hbm, air_out, surface, air, fresh, sides, sem_in, sem_out):
    def load(number):
        return pltpu.make_async_copy(
            air_hbm.at[:, number], air.at[:, number + 1, 8:136, :], sem_in.at[number]
        )

    def store(number):
        return pltpu.make_async_copy(fresh.at[:, number], air_out.at[:, number], sem_out.at[number])

    levels = 16
    for number in range(levels):
        load(number).start()
    lane = lanes()
    is0 = lane == 0
    is127 = lane == 127
    zero = jnp.zeros((128, LANES), f32)
    for f in range(3):
        air[f, 0, 8:136, :] = zero
        air[f, levels + 1, 8:136, :] = zero
    for plane in range(48):
        at = (plane // 16, plane % 16 + 1)
        air[at[0], at[1], 7:8, :] = north[plane : plane + 1, :]
        air[at[0], at[1], 136:137, :] = south[plane : plane + 1, :]
    sides[...] = jnp.where(lanes((128, LANES)) % 2 == 1, east_side[...], west_side[...])

    load(0).wait()

    def air_level(number, carry):
        @pl.when(number < levels - 1)
        def _():
            load(number + 1).wait()

        def air_rows(group, inner_carry):
            for k in range(AIR_UNROLL):
                row = group * (8 * AIR_UNROLL) + k * 8
                at = 8 + row
                halo = sides[pl.ds(row, 8), :]
                x = [air[f, number + 1, pl.ds(at, 8), :] for f in range(3)]
                for f in range(3):
                    up = air[f, number + 1, pl.ds(at - 1, 8), :]
                    dn = air[f, number + 1, pl.ds(at + 1, 8), :]
                    over = air[f, number + 2, pl.ds(at, 8), :]
                    under = air[f, number, pl.ds(at, 8), :]
                    mine = pltpu.roll(halo, LANES - 1 - 2 * (f * 16 + number), 1)
                    west = rolled(jnp.where(is127, mine, x[f]), 1)
                    east = rolled(jnp.where(is0, mine, x[f]), -1)
                    around = (up + dn) + (west + east)
                    advect = x[0] * (dn - up) + x[1] * (east - west)
                    fresh[f, number, pl.ds(row, 8), :] = (
                        (1.0 - 4.0 * viscosity - 2.0 * mixing) * x[f]
                        + viscosity * around
                        - (0.5 * courant) * advect
                        + mixing * (over + under)
                    )
            return inner_carry

        lax.fori_loop(0, 16 // AIR_UNROLL, air_rows, 0)
        store(number).start()
        return carry

    lax.fori_loop(0, levels, air_level, 0)

    surface[...] = fresh[2, 0]

    def drain(number, carry):
        store(number).wait()
        return carry

    lax.fori_loop(0, levels, drain, 0)


def heat_kernel(cells, blocks, index, gathered, plane, air_in, air_out, totals, warm, sem):
    pos = position()
    tile_rows = 128 // BA
    lane = lanes()
    warm[...] = plane[...]
    for slot in range(4):
        j = index[WORDS, slot] - 1

        @pl.when(j >= 0)
        def _():
            row = blocks[0, j] - pos[0] * tile_rows
            col = blocks[1, j] - pos[1] * tile_rows
            heat = gathered[pl.ds((j // 2) * HEAT_ROWS + 8 * (j % 2), 8), :]
            for g in range(4):
                moved = pltpu.roll(heat, (col - g + 4) * BA % LANES, 1)
                at = pl.multiple_of(row * BA + 8 * g, 8)
                warm[pl.ds(at, 8), :] += jnp.where(lane // BA == col, moved, 0.0)

    store = pltpu.make_async_copy(warm, air_out.at[2, 0], sem)
    store.start()
    devices = gathered.shape[0] // HEAT_ROWS
    sums = jnp.sum(gathered[pl.ds(16, devices, stride=HEAT_ROWS), :], axis=0, keepdims=True)
    lane1 = lanes((1, LANES))
    for k in range(2):
        totals[k] = jnp.sum(jnp.where(lane1 == k, sums, 0.0)) * (1.0 / cells)
    store.wait()


def step(air_state, level_set, fuel_left, fuel_class, fuel_props, blocks, adjacency):
    down = lax.axis_size("gx")
    across = lax.axis_size("gy")
    devices = down * across
    both = ("gx", "gy")
    smem = pl.BlockSpec(memory_space=pltpu.SMEM)
    vmem = pl.BlockSpec(memory_space=pltpu.VMEM)
    anywhere = pl.BlockSpec(memory_space=pl.ANY)
    blocks = blocks.T
    adjacency = adjacency.T
    packed = pl.pallas_call(
        pack_kernel,
        out_shape=pltpu.VMEM((devices * REC1, LANES), f32),
        in_specs=[smem, anywhere, anywhere, anywhere],
        out_specs=vmem,
        scratch_shapes=[
            pltpu.VMEM(level_set.shape, f32),
            pltpu.VMEM(level_set.shape, i32),
            pltpu.VMEM((2, 128, LANES), f32),
            pltpu.VMEM((4, 40, LANES), f32),
            pltpu.SMEM((8,), i32),
            pltpu.SemaphoreType.DMA((3,)),
        ],
        name="pack",
    )(blocks, level_set, fuel_class, air_state)
    relayed = lax.all_to_all(packed.reshape(devices, REC1, LANES), both, 0, 0)
    lanes_used = -(-blocks.shape[1] // LANES) * LANES
    index, tables, flags = pl.pallas_call(
        lambda *refs: index_kernel(across, *refs),
        out_shape=(
            jax.ShapeDtypeStruct((WORDS + 1, lanes_used), i32),
            pltpu.VMEM((5, 8, LANES), f32),
            pltpu.VMEM((22, 8, LANES), i32),
        ),
        in_specs=[vmem, vmem, smem, smem],
        out_specs=(vmem, vmem, vmem),
        scratch_shapes=[pltpu.VMEM((16, lanes_used), i32)],
        cost_estimate=pl.CostEstimate(flops=20_000_000, transcendentals=0, bytes_accessed=10_000),
        name="index",
    )(blocks, adjacency, adjacency, fuel_props)
    first_rows, last_rows, columns = pl.pallas_call(
        edge_kernel,
        out_shape=(
            pltpu.VMEM((48, LANES), f32),
            pltpu.VMEM((48, LANES), f32),
            pltpu.VMEM((128, LANES), f32),
        ),
        in_specs=[anywhere, anywhere],
        out_specs=(vmem, vmem, vmem),
        scratch_shapes=[pltpu.VMEM((48 * 128, LANES), f32), pltpu.SemaphoreType.DMA(())],
        cost_estimate=pl.CostEstimate(flops=30_000_000, transcendentals=0, bytes_accessed=3_200_000),
        name="edge",
    )(air_state.reshape(48 * 128, LANES), index)
    north = lax.ppermute(last_rows, "gx", [(k, k + 1) for k in range(down - 1)])
    south = lax.ppermute(first_rows, "gx", [(k + 1, k) for k in range(down - 1)])
    north = near(north)
    south = near(south)
    chosen = pl.pallas_call(
        select_kernel,
        out_shape=pltpu.VMEM((devices * REC2, LANES), f32),
        in_specs=[smem, vmem],
        out_specs=vmem,
        name="select",
    )(index, near(relayed.reshape(devices * REC1, LANES)))
    west_side = lax.ppermute(columns, "gy", [(k, k + 1) for k in range(across - 1)])
    east_side = lax.ppermute(columns, "gy", [(k + 1, k) for k in range(across - 1)])
    west_side = near(west_side)
    east_side = near(east_side)
    received = lax.all_to_all(chosen.reshape(devices, REC2, LANES), both, 0, 0)
    received = received.reshape(devices * REC2, LANES)[: PIECES * REC2]
    received = near(received)
    level_next, fuel_next, heat = pl.pallas_call(
        lambda *refs: fire_kernel(across, down, *refs),
        out_shape=(
            jax.ShapeDtypeStruct(level_set.shape, f32),
            jax.ShapeDtypeStruct(level_set.shape, f32),
            pltpu.VMEM((devices * HEAT_ROWS, LANES), f32),
        ),
        in_specs=[vmem] * 10,
        out_specs=(anywhere, anywhere, vmem),
        scratch_shapes=[
            pltpu.VMEM(level_set.shape, f32),
            pltpu.VMEM(level_set.shape, f32),
            pltpu.VMEM((5, EXT, LANES), f32),
            pltpu.VMEM((5, EXT, LANES), f32),
            pltpu.VMEM((5, EXT, LANES), f32),
            pltpu.VMEM((5, EXT, LANES), f32),
            pltpu.VMEM((2, 5, 40, LANES), f32),
            pltpu.VMEM((40, LANES), f32),
            pltpu.VMEM((2, LANES, 256), f32),
            pltpu.VMEM((4, 256, LANES), f32),
            pltpu.VMEM((4, 32, LANES), f32),
            pltpu.SemaphoreType.DMA((2, 32 // FINISH_UNROLL)),
        ],
        name="fire",
    )(
        near(tables),
        near(flags),
        received,
        near(level_set),
        near(fuel_left),
        near(fuel_class),
        west_side,
        east_side,
        north,
        south,
    )
    gathered = lax.all_to_all(heat.reshape(devices, 1, HEAT_ROWS * LANES), both, 0, 0)
    gathered = near(gathered.reshape(devices * HEAT_ROWS, LANES))
    air_next, plane = pl.pallas_call(
        air_kernel,
        out_shape=(jax.ShapeDtypeStruct(air_state.shape, f32), pltpu.VMEM((128, LANES), f32)),
        in_specs=[vmem, vmem, vmem, vmem, anywhere],
        out_specs=(anywhere, vmem),
        scratch_shapes=[
            pltpu.VMEM((3, 18, 144, LANES), f32),
            pltpu.VMEM((3, 16, 128, LANES), f32),
            pltpu.VMEM((128, LANES), f32),
            pltpu.SemaphoreType.DMA((16,)),
            pltpu.SemaphoreType.DMA((16,)),
        ],
        cost_estimate=pl.CostEstimate(flops=80_000_000, transcendentals=0, bytes_accessed=6_300_000),
        name="air",
    )(north, south, west_side, east_side, air_state)
    cells = blocks.shape[1] * level_set.shape[1] * level_set.shape[2]
    air_next, totals = pl.pallas_call(
        lambda *refs: heat_kernel(cells, *refs),
        out_shape=(jax.ShapeDtypeStruct(air_state.shape, f32), jax.ShapeDtypeStruct((2,), f32)),
        in_specs=[smem, smem, vmem, vmem, anywhere],
        out_specs=(anywhere, smem),
        scratch_shapes=[pltpu.VMEM((128, LANES), f32), pltpu.SemaphoreType.DMA(())],
        input_output_aliases={4: 0},
        name="heat",
    )(blocks, index, gathered, near(plane), air_next)
    return (air_next, level_next, fuel_next, totals)


def near(x):
    return pltpu.with_memory_space_constraint(x, pltpu.VMEM)


def solution(mesh):
    in_specs = (
        P(None, None, "gx", "gy"),
        P(("gx", "gy"), None, None),
        P(("gx", "gy"), None, None),
        P(("gx", "gy"), None, None),
        P(),
        P(),
        P(),
    )
    out_specs = (
        P(None, None, "gx", "gy"),
        P(("gx", "gy"), None, None),
        P(("gx", "gy"), None, None),
        P(),
    )
    return jax.shard_map(step, mesh=mesh, in_specs=in_specs, out_specs=out_specs, check_vma=False)
```
